32 devices in a mesh: rep: 2 (over y), grp: 16 (over z, x, core).
Axes of the slice: x: 2, y: 2, z: 4, core: 2. Of those that a mesh axis runs over, the one named last changes fastest.
Arguments:
- tokens: bfloat16 [16, 512, 2048], P('grp', 'rep'), may hold values from -6 to 6
- w_qkv: bfloat16 [2048, 6144], P('grp'), may hold values from -0.125 to 0.125
- w_out: bfloat16 [2048, 2048], P('grp'), may hold values from -1 to 1
- gains: bfloat16 [4352], P('grp'), may hold values from 0.25 to 1.75
- w_gate: bfloat16 [16, 2048, 1024], P('grp'), may hold values from -0.125 to 0.125
- w_up: bfloat16 [16, 2048, 1024], P('grp'), may hold values from -0.125 to 0.125
- w_down: bfloat16 [16, 1024, 2048], P('grp'), may hold values from -0.1875 to 0.1875
- segment_ids: int32 [16, 512], P('grp'), may hold values from 0 to 7, never falling along the last dimension, each value on 1 to 256 neighbouring positions
- routes: int32 [16, 512, 8], P('grp', 'rep'), may hold values from 0 to 15, all different within a row; in each aligned block of 256 rows (0 to 255, 256 to 511, ..., all dimensions but the last counted through in order) at most 144 rows name the same one
- gate_weights: float32 [16, 512, 8], P('grp', 'rep'), may hold values from 0.1 to 1
- cotangent: bfloat16 [16, 512, 2048], P('grp', 'rep'), may hold values from -6 to 6
Outputs:
- output: float32 [16, 512, 2048], P('grp', 'rep')
- d_tokens: float32 [16, 512, 2048], P('grp', 'rep')
- d_w_qkv: float32 [2048, 6144], P('grp')
- d_w_out: float32 [2048, 2048], P('grp')
- d_gains: float32 [4352], P('grp')
- d_w_gate: float32 [16, 2048, 1024], P('grp')
- d_w_up: float32 [16, 2048, 1024], P('grp')
- d_w_down: float32 [16, 1024, 2048], P('grp')
The draws below stay inside these ranges and needn't reach their ends.
Inputs may be any that keep to these rules, and one draw needn't show every extreme that they name: `routes`: each token names 8 different experts. Among the tokens of one device (aligned blocks of 256 tokens of a sequence) no expert is named by more than 144 of them, and some expert reaches 144 on some device. `segment_ids`: document numbers never fall along a sequence; a document has 1 to 256 tokens, and one has exactly that many.
All inputs are finite; a program needn't handle non-finite values.
Results may differ from the reference program's by a relative error of at most 0.02.
Values may be sent and summed in bfloat16 or wider, within the bound.
A program may use at most 320 MiB of HBM per device.

```python
import math
import jax
import jax.numpy as jnp
import numpy as np
from jax import lax

D = 2048
HEADS = 16
HD = 128
FF = 1024
TOP = 8
TOK_DEV = 256
LEN = 512
SEQS = 16
EXPERTS = 16
CAP = 144
DOCS = 8
GAINS = 4352


def block_levels(rng, extent, split, least, high):
    factor_of = 1.0
    for dim, blocks in split:
        draws = jax.random.uniform(jax.random.fold_in(jax.random.fold_in(rng, 6), dim), (blocks,), jnp.float32, least / len(split), high / len(split))
        factor_of = factor_of * jnp.repeat(jnp.exp(draws), extent[dim] // blocks).reshape((-1,) + (1,) * (len(extent) - 1 - dim))
    return factor_of


def profile(number_of, total, most, slope):
    portions = [(1 << 20) // math.isqrt(rank ** slope) + 1 for rank in range(2, number_of + 1)]
    spare, holding = total - most - (number_of - 1), [1] * (number_of - 1)
    while spare > 0:
        free = [i for i in range(number_of - 1) if holding[i] < most]
        whole, budget = sum([portions[i] for i in free]), spare
        for i in free:
            addition = min(most - holding[i], max(1, budget * portions[i] // whole), spare)
            holding[i] = holding[i] + addition
            spare = spare - addition
    return np.array([most] + holding)


def ragged_sizes(key, amount, total, limit, slope):
    if amount == 2:
        one = jax.random.randint(key, (), max(1, total - limit), min(limit, total - 1) + 1)
        return jnp.stack([one, total - one])
    lengths = jnp.asarray(profile(amount, total, limit, slope), jnp.int32)
    couples = (amount - 1) // 2
    giver, receiver = lengths[1:1 + 2 * couples:2], lengths[2:2 + 2 * couples:2]
    room = jnp.minimum(giver - 1, limit - receiver)
    shifted = jax.random.randint(jax.random.fold_in(key, 1), (couples,), 0, 1 << 20) % (room + 1)
    lengths = lengths.at[1:1 + 2 * couples:2].set(giver - shifted).at[2:2 + 2 * couples:2].set(receiver + shifted)
    return lengths[jax.random.permutation(jax.random.fold_in(key, 2), amount)]


def assign_block(stream_key, own, number, rows, number_of, top, bound, slope):
    sequence = jax.random.permutation(stream_key, number_of)
    crowded, usual = load_shares(number_of, rows * top, bound, slope, True), load_shares(number_of, rows * top, bound, slope, False)
    places = jnp.arange(number_of)

    def named(lengths, turn):
        used = int((lengths > 0).sum())
        fixed = max(1, used // 4)
        moved = fixed + (places - fixed + turn * (used - fixed)) % max(1, number_of - fixed)
        return jnp.zeros((number_of,), jnp.int32).at[sequence[jnp.where(places < fixed, places, moved)]].set(jnp.asarray(lengths, jnp.int32))

    lengths = jnp.where(number % 4 == 0, named(crowded, number // 4), named(usual, number - number // 4 - 1))
    mixed = jax.random.permutation(jax.random.fold_in(own, 3), number_of)
    donor, receiver = mixed[0:number_of // 2 * 2:2], mixed[1:number_of // 2 * 2:2]
    margin = jnp.minimum(lengths[donor] - 1, bound - lengths[receiver]) // 2
    margin = jnp.where((donor == sequence[0]) | (receiver == sequence[0]) | (lengths[receiver] == 0), 0, jnp.maximum(margin, 0))
    moved = jax.random.randint(jax.random.fold_in(own, 4), (number_of // 2,), 0, 1 << 20) % (margin + 1)
    lengths = lengths.at[donor].add(-moved).at[receiver].add(moved)
    items = jnp.searchsorted(jnp.cumsum(lengths), jnp.arange(rows * top), side="right").astype(jnp.int32)
    listing = items.reshape(top, rows).T
    listing = listing[jax.random.permutation(jax.random.fold_in(own, 1), rows)]
    turn = jax.random.randint(jax.random.fold_in(own, 2), (rows, 1), 0, top)
    return jnp.take_along_axis(listing, (jnp.arange(top)[None, :] + turn) % top, axis=1)


def load_shares(count, total, most, slope, full):
    weights = [(1 << 20) // math.isqrt(grade ** slope) + 1 for grade in range(1, count + 1)]
    largest = most if full else min(most, max(-(-total // count), total * weights[0] // sum(weights)))
    least = 1 if total - largest >= count - 1 else 0
    counts, spare = [largest] + [least] * (count - 1), total - largest - least * (count - 1)
    while spare > 0:
        free = [i for i in range(1, count) if counts[i] < largest] or [i for i in range(1, count) if counts[i] < most]
        mass, remaining = sum([weights[i] for i in free]), spare
        for i in free:
            extra = min(most - counts[i], max(1, remaining * weights[i] // mass), spare)
            counts[i] = counts[i] + extra
            spare = spare - extra
    return np.array(counts)


def noise(rng, shape, width, reach, shards=(), kind=jnp.bfloat16):
    values = width * jax.random.normal(rng, shape, jnp.float32)
    if shards:
        values = values * block_levels(rng, shape, shards, -0.22, 0.18)
    return jnp.clip(values, -reach, reach).astype(kind)


def setup_inputs(seed: int = 0) -> dict:
    key_of = jax.random.split(jax.random.key(seed), 12)
    tokens = noise(key_of[0], (SEQS, LEN, D), 1.0, 6.0, ((0, 16), (1, 2)))
    w_qkv = noise(key_of[1], (D, 3 * D), D ** -0.5, 0.125, ((0, 16),))
    w_out = noise(key_of[2], (D, D), (D // 64) ** -0.5, 1.0, ((0, 16),))
    gains = jnp.clip(1.0 + 0.15 * jax.random.normal(key_of[3], (GAINS,), jnp.float32), 0.25, 1.75).astype(jnp.bfloat16)
    w_gate = noise(key_of[4], (EXPERTS, D, FF), D ** -0.5, 0.125, ((0, 16),))
    w_up = noise(key_of[5], (EXPERTS, D, FF), D ** -0.5, 0.125, ((0, 16),))
    w_down = noise(key_of[6], (EXPERTS, FF, D), FF ** -0.5, 0.1875, ((0, 16),))
    segment_ids = jax.vmap(lambda own: jnp.searchsorted(jnp.cumsum(ragged_sizes(own, DOCS, LEN, LEN // 2, 2)), jnp.arange(LEN), side="right"))(jax.random.split(key_of[7], SEQS)).reshape((SEQS, LEN)).astype(jnp.int32)
    routes_keys = jax.random.split(jax.random.fold_in(key_of[8], 1), SEQS * LEN // TOK_DEV)
    routes_turns = jax.random.permutation(jax.random.fold_in(key_of[8], 3), SEQS * LEN // TOK_DEV)
    routes = jax.vmap(lambda own, number: assign_block(jax.random.fold_in(key_of[8], 2), own, number, TOK_DEV, EXPERTS, TOP, CAP, 1))(routes_keys, routes_turns).reshape((SEQS, LEN, TOP))
    gate_weights = jnp.clip(0.1 + 0.9 * jax.random.uniform(key_of[9], (SEQS, LEN, TOP), jnp.float32) ** block_levels(key_of[9], (SEQS, LEN, TOP), ((0, 16), (1, 2)), -0.2, 0.2), 0.1, 1.0)
    cotangent = noise(key_of[10], (SEQS, LEN, D), 1.0, 6.0, ((0, 16), (1, 2)))
    return {"tokens": tokens, "w_qkv": w_qkv, "w_out": w_out, "gains": gains, "w_gate": w_gate, "w_up": w_up, "w_down": w_down, "segment_ids": segment_ids, "routes": routes, "gate_weights": gate_weights, "cotangent": cotangent}


epsilon = 1e-06
rope_base = 10000.0
precise = lax.Precision.HIGHEST

@jax.custom_vjp
def low(v):
    return lax.optimization_barrier(v.astype(jnp.bfloat16)).astype(jnp.float32)

@jax.custom_vjp
def low_back(v):
    return v

def low_keep(v):
    return (low(v), None)

def low_pass(kept, grad):
    return (grad,)

def back_keep(v):
    return (v, None)

def back_low(kept, grad):
    return (low(grad),)
low.defvjp(low_keep, low_pass)
low_back.defvjp(back_keep, back_low)

def rms_norm(values, gain_vec):
    return values * lax.rsqrt(lax.optimization_barrier(jnp.mean(values * values, axis=-1, keepdims=True)) + epsilon) * gain_vec

def rotate(values, positions):
    half_size = values.shape[-1] // 2
    frequency = rope_base ** (-2.0 * jnp.arange(half_size, dtype=jnp.float32) / values.shape[-1])
    angles = positions[:, None] * frequency[None, :]
    cosine_table = jnp.cos(angles)[:, None, :]
    sine_table = jnp.sin(angles)[:, None, :]
    first_half = values[..., :half_size]
    second_half = values[..., half_size:]
    return jnp.concatenate([first_half * cosine_table - second_half * sine_table, second_half * cosine_table + first_half * sine_table], axis=-1)

def reference(tokens, w_qkv, w_out, gains, w_gate, w_up, w_down, segment_ids, routes, gate_weights, cotangent):
    score_scale = HD ** (-0.5)
    flat_routes = routes.reshape(SEQS * LEN, TOP)
    flat_gates = gate_weights.reshape(SEQS * LEN, TOP).astype(jnp.float32)

    def attend(operands):
        queries, keys, vals, segments = operands
        scores = jnp.einsum('qhd,khd->hqk', queries, keys, precision=precise) * score_scale
        scores = low_back(scores)
        same_doc = segments[:, None] == segments[None, :]
        scores = jnp.where(same_doc[None], scores, -1e+30)
        probs = jax.nn.softmax(scores, axis=-1)
        return jnp.einsum('hqk,khd->qhd', low(probs), vals, precision=precise)

    def forward(inputs, qkv_weights, out_weights, gain_all, gate_all, up_all, down_all):
        g_attn = gain_all[:D]
        g_ffn = gain_all[D:2 * D]
        g_query = gain_all[2 * D:2 * D + HD]
        g_key = gain_all[2 * D + HD:]
        flat_rows = inputs.reshape(SEQS * LEN, D)
        normed_b = low(rms_norm(flat_rows, g_attn))
        projected = low_back(jnp.dot(normed_b, qkv_weights, precision=precise))
        queries = projected[:, :D].reshape(SEQS, LEN, HEADS, HD)
        keys = projected[:, D:2 * D].reshape(SEQS, LEN, HEADS, HD)
        vals = projected[:, 2 * D:].reshape(SEQS, LEN, HEADS, HD)
        positions = jnp.arange(LEN, dtype=jnp.float32)
        queries = low(rotate(rms_norm(queries, g_query), positions))
        keys = low(rotate(rms_norm(keys, g_key), positions))
        vals = low(vals)
        attended = lax.map(jax.checkpoint(attend), (queries, keys, vals, segment_ids))
        attended = low_back(low(attended.reshape(SEQS * LEN, D)))
        mid_rows = flat_rows + low_back(jnp.dot(attended, out_weights, precision=precise))
        moe_in = low(rms_norm(mid_rows, g_ffn))

        def expert_step(running, operands):
            expert_id, gate_e, up_e, down_e = operands
            route_share = lax.optimization_barrier(jnp.sum(jnp.where(flat_routes == expert_id, flat_gates, 0.0), axis=1))
            expert_in = low_back(moe_in)
            gate_pre = low_back(jnp.dot(expert_in, gate_e, precision=precise))
            up_pre = low_back(jnp.dot(expert_in, up_e, precision=precise))
            activated = low(jax.nn.silu(gate_pre) * up_pre)
            expert_out = low(low_back(jnp.dot(activated, down_e, precision=precise)))
            return (running + route_share[:, None] * expert_out, None)
        moe_out, _ = lax.scan(jax.checkpoint(expert_step), jnp.zeros((SEQS * LEN, D), jnp.float32), (jnp.arange(EXPERTS, dtype=jnp.int32), gate_all, up_all, down_all))
        return (mid_rows + moe_out).reshape(SEQS, LEN, D)
    operands = (tokens.astype(jnp.float32), w_qkv.astype(jnp.float32), w_out.astype(jnp.float32), gains.astype(jnp.float32), w_gate.astype(jnp.float32), w_up.astype(jnp.float32), w_down.astype(jnp.float32))
    result, pullback = jax.vjp(forward, *operands)
    gradients = pullback(cotangent.astype(jnp.float32))
    return (result, gradients[0], gradients[1], gradients[2], gradients[3], gradients[4], gradients[5], gradients[6])
```

```python
import jax
import jax.numpy as jnp
import numpy as np
from jax import lax
from jax.sharding import PartitionSpec as P

D = 2048
HEADS = 16
HD = 128
TOP = 8
BF = jnp.bfloat16
F32 = jnp.float32

epsilon = 1e-06
rope_base = 10000.0


def rms_forward(values, gain_vec):
    inverse = lax.rsqrt(jnp.mean(values * values, axis=-1, keepdims=True) + epsilon)
    normed = values * inverse
    return (normed * gain_vec, normed, inverse)


def rms_backward(grad_out, normed, inverse, gain_vec):
    scaled = grad_out * gain_vec
    grad_in = inverse * (scaled - normed * jnp.mean(scaled * normed, axis=-1, keepdims=True))
    return (grad_in, grad_out * normed)


def rotate(values, positions, direction):
    half_size = values.shape[-1] // 2
    frequency = rope_base ** (-2.0 * jnp.arange(half_size, dtype=jnp.float32) / values.shape[-1])
    angles = positions[:, None] * frequency[None, :]
    cosine_table = jnp.cos(angles)[:, None, :]
    sine_table = direction * jnp.sin(angles)[:, None, :]
    first_half = values[..., :half_size]
    second_half = values[..., half_size:]
    return jnp.concatenate(
        [
            first_half * cosine_table - second_half * sine_table,
            second_half * cosine_table + first_half * sine_table,
        ],
        axis=-1,
    )


def dot32(a, b):
    return jnp.dot(a, b, preferred_element_type=F32)


class Ring:
    def __init__(self, devices):
        self.devices = devices
        self.chips = devices // 2
        outer = 4 if self.chips % 4 == 0 else 2
        inner = self.chips // outer
        cycle = [(a, 0) for a in range(outer)]
        for step, a in enumerate(reversed(range(outer))):
            columns = range(1, inner)
            cycle += [(a, b) for b in (columns if step % 2 == 0 else reversed(columns))]
        self.cycle = [a * inner + b for a, b in cycle]
        self.place = {chip: i for i, chip in enumerate(self.cycle)}
        self.half = self.chips // 2

    def perm(self, shift):
        pairs = []
        for chip in range(self.chips):
            other = self.cycle[(self.place[chip] + shift) % self.chips]
            pairs += [(2 * chip + core, 2 * other + core) for core in range(2)]
        return pairs

    def table(self):
        out = np.zeros((self.devices, self.chips, 2), np.int32)
        for dev in range(self.devices):
            chip, core = dev // 2, dev % 2
            for d in range(self.chips):
                other = self.cycle[(self.place[chip] + d) % self.chips]
                out[dev, d, 0] = 2 * other + core
                out[dev, d, 1] = 2 * other + (1 - core)
        return out

    def ahead(self, v):
        return lax.ppermute(v, "grp", self.perm(1))

    def back(self, v):
        return lax.ppermute(v, "grp", self.perm(-1))

    def flip(self, v):
        return lax.ppermute(v, "grp", [(i, i ^ 1) for i in range(self.devices)])

    def gather(self, own):
        rows = own.shape[0] // 2
        blocks = {0: (own, self.flip(own))}
        up = down = own
        for step in range(1, self.half):
            up, down = self.ahead(up), self.back(down)
            blocks[-step % self.chips] = (up, self.flip(up))
            blocks[step] = (down, self.flip(down))
        first, last = self.ahead(up[:rows]), self.back(down[rows:])
        far = jnp.concatenate([first, last], axis=0)
        blocks[self.half] = (far, self.flip(far))
        return blocks

    def scatter_sum(self, blocks):
        def joined(d):
            same, other = blocks[d]
            return same.astype(F32) + self.flip(other.astype(BF)).astype(F32)

        far = joined(self.half).astype(BF)
        rows = far.shape[0] // 2
        up, down = self.ahead(far[:rows]), self.back(far[rows:])
        zero = jnp.zeros_like(up)
        up = jnp.concatenate([up, zero], axis=0)
        down = jnp.concatenate([zero, down], axis=0)
        for step in range(self.half - 1, 0, -1):
            up = self.ahead((joined(step) + up.astype(F32)).astype(BF))
            down = self.back((joined(-step % self.chips) + down.astype(F32)).astype(BF))
        return joined(0) + up.astype(F32) + down.astype(F32)


def per_device(
    tokens, w_qkv, w_out, gains, w_gate, w_up, w_down, segment_ids, routes, gate_weights, cotangent
):
    groups = lax.axis_size("grp")
    reps = lax.axis_size("rep")
    ring = Ring(groups)
    rep, grp = lax.axis_index("rep"), lax.axis_index("grp")
    rel = jnp.asarray(ring.table())[grp]
    rel_flat = rel.reshape(-1)
    tok_rows = tokens.shape[1]
    seq_len = segment_ids.shape[1]
    heads = HEADS // reps
    wide = heads * HD
    score_scale = HD ** (-0.5)

    def from_rep(v, k):
        return lax.ppermute(v, "rep", [((s + k) % reps, s) for s in range(reps)])

    def to_rep(v, k):
        return lax.ppermute(v, "rep", [(s, (s + k) % reps) for s in range(reps)])

    def rep_gather(v):
        return jnp.concatenate([v] + [from_rep(v, k) for k in range(1, reps)], axis=0)

    def rep_scatter(v):
        parts = v.reshape(reps, tok_rows, v.shape[-1])
        out = parts[0].astype(F32)
        for k in range(1, reps):
            out = out + to_rep(parts[k].astype(BF), k).astype(F32)
        return out

    own_b = tokens[0]
    seq_b = rep_gather(own_b)
    gates_f = gate_weights[0]
    experts = jnp.arange(groups, dtype=jnp.int32)
    weight_of = jnp.sum(
        jnp.where(routes[0][None] == experts[:, None, None], gates_f[None], 0.0), axis=-1
    )
    small = jnp.concatenate(
        [
            weight_of,
            jnp.broadcast_to(gains.astype(F32)[None], (groups, gains.shape[0])),
        ],
        axis=1,
    )
    small = lax.all_to_all(small, "grp", split_axis=0, concat_axis=0, tiled=True)
    gains_f = small[:, tok_rows:].reshape(-1)
    weight_in = small[:, :tok_rows][rel_flat]
    g_attn = gains_f[:D]
    g_ffn = gains_f[D : 2 * D]
    g_query = gains_f[2 * D : 2 * D + HD]
    g_key = gains_f[2 * D + HD :]

    my_qkv = lax.dynamic_index_in_dim(
        w_qkv.reshape(w_qkv.shape[0], 3, heads, reps, HD), rep, axis=3, keepdims=False
    ).reshape(w_qkv.shape[0], 3 * wide)
    shard = my_qkv.shape[0]
    full_qkv = jnp.zeros((D, 3 * wide), BF)
    for d, pair in ring.gather(my_qkv).items():
        for k in range(2):
            full_qkv = lax.dynamic_update_slice(full_qkv, pair[k], (rel[d, k] * shard, 0))
    full_out = lax.all_gather(w_out, "grp", axis=0, tiled=True)
    my_out = lax.dynamic_index_in_dim(
        full_out.reshape(heads, reps, HD, D), rep, axis=1, keepdims=False
    ).reshape(wide, D)

    seq_f = seq_b.astype(F32)
    normed_one, hat_one, inv_one = rms_forward(seq_f, g_attn)
    h1_b = normed_one.astype(BF)
    projected = dot32(h1_b, full_qkv)
    q_pre = projected[:, :wide].reshape(seq_len, heads, HD)
    k_pre = projected[:, wide : 2 * wide].reshape(seq_len, heads, HD)
    v_pre = projected[:, 2 * wide :]
    q_normed, q_hat, q_inv = rms_forward(q_pre, g_query)
    k_normed, k_hat, k_inv = rms_forward(k_pre, g_key)
    order = jnp.concatenate(
        [((rep + k) % reps) * tok_rows + jnp.arange(tok_rows, dtype=jnp.int32) for k in range(reps)]
    )
    positions = order.astype(F32)
    q_b = rotate(q_normed, positions, 1.0).astype(BF)
    k_b = rotate(k_normed, positions, 1.0).astype(BF)
    v_b = v_pre.astype(BF).reshape(seq_len, heads, HD)
    docs = segment_ids[0][order]
    same_doc = (docs[:, None] == docs[None, :])[None]
    scores = jnp.where(
        same_doc,
        jnp.einsum("qhd,khd->hqk", q_b, k_b, preferred_element_type=F32) * score_scale,
        -1e30,
    )
    row_max = jnp.max(scores, axis=-1, keepdims=True)
    log_total = row_max + jnp.log(jnp.sum(jnp.exp(scores - row_max), axis=-1, keepdims=True))
    probs_f = jnp.exp(scores - log_total)
    probs_b = probs_f.astype(BF)
    attended = jnp.einsum("hqk,khd->qhd", probs_b, v_b, preferred_element_type=F32)
    attended_b = attended.reshape(seq_len, wide).astype(BF)
    mid_rows = own_b.astype(F32) + rep_scatter(dot32(attended_b, my_out))
    normed_two, hat_two, inv_two = rms_forward(mid_rows, g_ffn)
    h2_b = normed_two.astype(BF)

    entries = tok_rows * TOP
    capacity = min(tok_rows, (9 * entries + 8 * groups - 1) // (8 * groups))
    named = weight_in > 0
    before = dot32(
        named.astype(BF), jnp.tri(tok_rows, dtype=BF).T
    )
    slot = jnp.where(named, before - 1.0, -1.0).astype(jnp.int32)
    pick = (slot[:, None, :] == jnp.arange(capacity, dtype=jnp.int32)[None, :, None]).astype(BF)
    row_weight = jnp.sum(pick.astype(F32) * weight_in[:, None, :], axis=-1)

    chips, half = ring.chips, ring.half
    batches = [(0,)] + [(d, chips - d) for d in range(1, half)] + [(half,)]

    def select(blocks, batch):
        return jnp.concatenate(
            [dot32(pick[2 * d + k], blocks[d][k]).astype(BF) for d in batch for k in range(2)], axis=0
        )

    def spread(rows, batch):
        out, at = {}, 0
        for d in batch:
            pair = []
            for k in range(2):
                part = rows[at : at + capacity]
                pair.append(
                    lax.dot_general(
                        pick[2 * d + k], part, (((0,), (0,)), ((), ())), preferred_element_type=F32
                    ).astype(BF)
                )
                at += capacity
            out[d] = tuple(pair)
        return out

    def weights_of(batch):
        return jnp.concatenate([row_weight[2 * d + k] for d in batch for k in range(2)])[:, None]

    dy_blocks = ring.gather(cotangent[0])
    h2_blocks = ring.gather(h2_b)
    acts, upres, gpres, rows_in, grads_in, grad_acts = [], [], [], [], [], []
    for batch in batches:
        picked = select(h2_blocks, batch)
        grads = (weights_of(batch) * select(dy_blocks, batch).astype(F32)).astype(BF)
        rows_in.append(picked)
        grads_in.append(grads)
        gpres.append(dot32(picked, w_gate[0]))
        upres.append(dot32(picked, w_up[0]))
        acts.append((jax.nn.silu(gpres[-1]) * upres[-1]).astype(BF))
        grad_acts.append(
            jnp.einsum("rd,fd->rf", grads, w_down[0], preferred_element_type=F32)
        )
    grad_gates, grad_ups = [], []
    back_blocks = {}
    for i in reversed(range(len(batches))):
        sig = jax.nn.sigmoid(gpres[i])
        grad_gates.insert(
            0, (grad_acts[i] * upres[i] * sig * (1.0 + gpres[i] * (1.0 - sig))).astype(BF)
        )
        grad_ups.insert(0, (grad_acts[i] * gpres[i] * sig).astype(BF))
        drow = (
            jnp.einsum("rf,df->rd", grad_gates[0], w_gate[0], preferred_element_type=F32)
            + jnp.einsum("rf,df->rd", grad_ups[0], w_up[0], preferred_element_type=F32)
        ).astype(BF)
        back_blocks.update(spread(drow, batches[i]))
    grad_h2 = ring.scatter_sum(back_blocks)

    acts_late, _ = lax.optimization_barrier((acts, grad_h2))
    out_blocks = {}
    for i in reversed(range(len(batches))):
        eout = dot32(acts_late[i], w_down[0]).astype(BF).astype(F32)
        out_blocks.update(spread((weights_of(batches[i]) * eout).astype(BF), batches[i]))
    result = mid_rows + ring.scatter_sum(out_blocks)

    all_rows = jnp.concatenate(rows_in, axis=0)
    all_grads = jnp.concatenate(grads_in, axis=0)
    all_acts = jnp.concatenate(acts, axis=0)
    all_gates = jnp.concatenate(grad_gates, axis=0)
    all_ups = jnp.concatenate(grad_ups, axis=0)

    def rep_sum(v):
        v = v.astype(BF)
        out = v.astype(F32)
        for k in range(1, reps):
            out = out + from_rep(v, k).astype(F32)
        return out

    grad_wdown = rep_sum(jnp.einsum("rf,rd->fd", all_acts, all_grads, preferred_element_type=F32))
    grad_wgate = rep_sum(jnp.einsum("rd,rf->df", all_rows, all_gates, preferred_element_type=F32))
    grad_wup = rep_sum(jnp.einsum("rd,rf->df", all_rows, all_ups, preferred_element_type=F32))

    grad_out = cotangent[0].astype(F32)
    grad_mid_norm, ffn_terms = rms_backward(grad_h2, hat_two, inv_two, g_ffn)
    grad_mid = grad_out + grad_mid_norm
    grad_branch_b = rep_gather(grad_mid.astype(BF))
    grad_wout = jnp.einsum("td,te->de", attended_b, grad_branch_b, preferred_element_type=F32)
    grad_attn_b = (
        jnp.einsum("te,de->td", grad_branch_b, my_out, preferred_element_type=F32)
        .astype(BF)
        .reshape(seq_len, heads, HD)
    )
    grad_probs = jnp.einsum("qhd,khd->hqk", grad_attn_b, v_b, preferred_element_type=F32)
    grad_vals = jnp.einsum("hqk,qhd->khd", probs_b, grad_attn_b, preferred_element_type=F32)
    grad_scores = (
        probs_f * (grad_probs - jnp.sum(probs_f * grad_probs, axis=-1, keepdims=True))
    ).astype(BF)
    grad_q = jnp.einsum("hqk,khd->qhd", grad_scores, k_b, preferred_element_type=F32) * score_scale
    grad_k = jnp.einsum("hqk,qhd->khd", grad_scores, q_b, preferred_element_type=F32) * score_scale
    grad_qn = rotate(grad_q, positions, -1.0)
    grad_kn = rotate(grad_k, positions, -1.0)
    grad_q_pre, query_terms = rms_backward(grad_qn, q_hat, q_inv, g_query)
    grad_k_pre, key_terms = rms_backward(grad_kn, k_hat, k_inv, g_key)
    grad_proj = jnp.concatenate(
        [
            grad_q_pre.reshape(seq_len, wide),
            grad_k_pre.reshape(seq_len, wide),
            grad_vals.reshape(seq_len, wide),
        ],
        axis=1,
    ).astype(BF)
    grad_wqkv = jnp.einsum("td,te->de", h1_b, grad_proj, preferred_element_type=F32).astype(BF)
    grad_h1 = rep_scatter(
        jnp.einsum("te,de->td", grad_proj, full_qkv, preferred_element_type=F32)
    )
    grad_rows_one, attn_terms = rms_backward(
        grad_h1, hat_one[:tok_rows], inv_one[:tok_rows], g_attn
    )
    grad_tokens = grad_mid + grad_rows_one

    qkv_blocks = {
        d: tuple(
            lax.dynamic_slice(grad_wqkv, (rel[d, k] * shard, 0), (shard, 3 * wide))
            for k in range(2)
        )
        for d in range(chips)
    }
    shard_qkv = ring.scatter_sum(qkv_blocks).astype(BF)
    qkv_all = [shard_qkv] + [from_rep(shard_qkv, k) for k in range(1, reps)]
    columns = jnp.stack(qkv_all, axis=0).reshape(reps, shard, 3, heads, HD)
    columns = columns[(jnp.arange(reps) - rep) % reps]
    shard_qkv = columns.transpose(1, 2, 3, 0, 4).reshape(shard, 3 * D).astype(F32)

    zero_out = jnp.zeros((heads, reps, HD, D), BF)
    whole_out = lax.dynamic_update_slice(
        zero_out, grad_wout.astype(BF).reshape(heads, 1, HD, D), (0, rep, 0, 0)
    ).reshape(D, D)
    shard_out = lax.psum(
        lax.psum_scatter(whole_out, "grp", scatter_dimension=0, tiled=True), "rep"
    ).astype(F32)

    grad_gains = jnp.concatenate(
        [
            jnp.sum(attn_terms, axis=0),
            jnp.sum(ffn_terms, axis=0),
            jnp.sum(query_terms, axis=(0, 1)),
            jnp.sum(key_terms, axis=(0, 1)),
        ]
    )
    pieces = lax.all_to_all(
        grad_gains.reshape(groups, -1), "grp", split_axis=0, concat_axis=0, tiled=True
    )
    shard_gains = jnp.sum(pieces, axis=0)
    total = shard_gains
    for k in range(1, reps):
        total = total + from_rep(shard_gains, k)
    return (
        result[None],
        grad_tokens[None],
        shard_qkv,
        shard_out,
        total,
        grad_wgate[None],
        grad_wup[None],
        grad_wdown[None],
    )


def solution(mesh):
    in_specs = (
        P("grp", "rep", None),
        P("grp", None),
        P("grp", None),
        P("grp"),
        P("grp", None, None),
        P("grp", None, None),
        P("grp", None, None),
        P("grp", None),
        P("grp", "rep", None),
        P("grp", "rep", None),
        P("grp", "rep", None),
    )
    out_specs = (
        P("grp", "rep", None),
        P("grp", "rep", None),
        P("grp", None),
        P("grp", None),
        P("grp"),
        P("grp", None, None),
        P("grp", None, None),
        P("grp", None, None),
    )
    return jax.shard_map(
        per_device, mesh=mesh, in_specs=in_specs, out_specs=out_specs, check_vma=False
    )
```

```python
import functools

import jax
import jax.numpy as jnp
import numpy as np
from jax import lax
from jax.experimental import pallas as pl
from jax.experimental.pallas import tpu as pltpu
from jax.sharding import PartitionSpec as P

D = 2048
HEADS = 16
HD = 128
TOP = 8
BF = jnp.bfloat16
F32 = jnp.float32

epsilon = 1e-06
rope_base = 10000.0


def rms_forward(values, gain_vec):
    inverse = lax.rsqrt(jnp.mean(values * values, axis=-1, keepdims=True) + epsilon)
    normed = values * inverse
    return (normed * gain_vec, normed, inverse)


def rms_backward(grad_out, normed, inverse, gain_vec):
    scaled = grad_out * gain_vec
    grad_in = inverse * (scaled - normed * jnp.mean(scaled * normed, axis=-1, keepdims=True))
    return (grad_in, grad_out * normed)


def rotate(values, positions, direction):
    half_size = values.shape[-1] // 2
    frequency = rope_base ** (-2.0 * jnp.arange(half_size, dtype=jnp.float32) / values.shape[-1])
    angles = positions[:, None] * frequency[None, :]
    cosine_table = jnp.cos(angles)[:, None, :]
    sine_table = direction * jnp.sin(angles)[:, None, :]
    first_half = values[..., :half_size]
    second_half = values[..., half_size:]
    return jnp.concatenate(
        [
            first_half * cosine_table - second_half * sine_table,
            second_half * cosine_table + first_half * sine_table,
        ],
        axis=-1,
    )


def dot32(a, b):
    return jnp.dot(a, b, preferred_element_type=F32)


class Ring:
    def __init__(self, devices):
        self.devices = devices
        self.chips = devices // 2
        outer = 4 if self.chips % 4 == 0 else 2
        inner = self.chips // outer
        cycle = [(a, 0) for a in range(outer)]
        for step, a in enumerate(reversed(range(outer))):
            columns = range(1, inner)
            cycle += [(a, b) for b in (columns if step % 2 == 0 else reversed(columns))]
        self.cycle = [a * inner + b for a, b in cycle]
        self.place = {chip: i for i, chip in enumerate(self.cycle)}
        self.half = self.chips // 2

    def perm(self, shift):
        pairs = []
        for chip in range(self.chips):
            other = self.cycle[(self.place[chip] + shift) % self.chips]
            pairs += [(2 * chip + core, 2 * other + core) for core in range(2)]
        return pairs

    def table(self):
        out = np.zeros((self.devices, self.chips, 2), np.int32)
        for dev in range(self.devices):
            chip, core = dev // 2, dev % 2
            for d in range(self.chips):
                other = self.cycle[(self.place[chip] + d) % self.chips]
                out[dev, d, 0] = 2 * other + core
                out[dev, d, 1] = 2 * other + (1 - core)
        return out

    def ahead(self, v):
        return lax.ppermute(v, "grp", self.perm(1))

    def back(self, v):
        return lax.ppermute(v, "grp", self.perm(-1))

    def flip(self, v):
        return lax.ppermute(v, "grp", [(i, i ^ 1) for i in range(self.devices)])

    def gather(self, own):
        rows = own.shape[0] // 2
        blocks = {0: (own, self.flip(own))}
        up = down = own
        for step in range(1, self.half):
            up, down = self.ahead(up), self.back(down)
            blocks[-step % self.chips] = (up, self.flip(up))
            blocks[step] = (down, self.flip(down))
        first, last = self.ahead(up[:rows]), self.back(down[rows:])
        far = jnp.concatenate([first, last], axis=0)
        blocks[self.half] = (far, self.flip(far))
        return blocks

    def scatter_sum(self, blocks):
        def joined(d):
            same, other = blocks[d]
            return same.astype(F32) + self.flip(other.astype(BF)).astype(F32)

        far = joined(self.half).astype(BF)
        rows = far.shape[0] // 2
        up, down = self.ahead(far[:rows]), self.back(far[rows:])
        zero = jnp.zeros_like(up)
        up = jnp.concatenate([up, zero], axis=0)
        down = jnp.concatenate([zero, down], axis=0)
        for step in range(self.half - 1, 0, -1):
            up = self.ahead((joined(step) + up.astype(F32)).astype(BF))
            down = self.back((joined(-step % self.chips) + down.astype(F32)).astype(BF))
        return joined(0) + up.astype(F32) + down.astype(F32)


MESH = pl.DeviceIdType.MESH
DMA = pltpu.SemaphoreType.DMA
VMEM_LIMIT = 60 << 20


class Hops:
    def __init__(self, chips):
        self.chips, self.half = chips, chips // 2
        self.outer = 4 if chips % 4 == 0 else 2
        self.inner = chips // self.outer
        self.me = lax.axis_index("grp")
        chip, self.core = self.me // 2, self.me % 2
        a, b = chip // self.inner, chip % self.inner
        row = self.outer - 1 - a
        along = jnp.where(row % 2 == 0, b - 1, self.inner - 1 - b)
        self.place = jnp.where(b == 0, a, self.outer + row * (self.inner - 1) + along)
        self.ahead, self.back = self.device(1), self.device(-1)
        self.flip = self.me + 1 - 2 * self.core
        self.started = []

    def chip(self, d):
        p = (self.place + (d % self.chips)) % self.chips
        q = jnp.maximum(p - self.outer, 0)
        k, m = q // (self.inner - 1), q % (self.inner - 1)
        b = jnp.where(k % 2 == 0, m + 1, self.inner - 1 - m)
        return jnp.where(
            p < self.outer, p * self.inner, (self.outer - 1 - k) * self.inner + b
        )

    def device(self, d):
        return 2 * self.chip(d) + self.core

    def meet(self):
        barrier = pltpu.get_barrier_semaphore()
        for dev in (self.ahead, self.back, self.flip):
            pl.semaphore_signal(barrier, inc=1, device_id={"grp": dev}, device_id_type=MESH)
        pl.semaphore_wait(barrier, 3)

    def copy(self, src, dst, send_sem, recv_sem, dev):
        return pltpu.make_async_remote_copy(
            src_ref=src,
            dst_ref=dst,
            send_sem=send_sem,
            recv_sem=recv_sem,
            device_id={"grp": dev},
            device_id_type=MESH,
        )

    def send(self, src, dst, sems, at, dev):
        c = self.copy(src, dst, sems.at[0, at], sems.at[1, at], dev)
        c.start()
        self.started.append(c)

    def wait(self, dst, sems, at):
        self.copy(dst, dst, sems.at[0, at], sems.at[1, at], self.flip).wait_recv()

    def drain(self):
        for c in self.started:
            c.wait_send()

    def gather(self, own, slot, up, down, side, use):
        half, rows = self.half, own.shape[0]
        cut = rows // 2
        self.send(own, slot(self.me), up, 0, self.ahead)
        self.send(own, slot(self.me), down, 0, self.back)
        self.send(own, slot(self.me), side, 0, self.flip)

        def ready(d):
            dev = self.device(d)
            self.wait(slot(dev + 1 - 2 * self.core), side, d % self.chips)
            use(d)

        for s in range(1, half):
            last = s == half - 1
            a, b = slot(self.device(-s)), slot(self.device(s))
            self.wait(a, up, s - 1)
            part = a.at[pl.ds(0, cut)] if last else a
            self.send(part, part, up, s, self.ahead)
            self.send(a, a, side, -s % self.chips, self.flip)
            self.wait(b, down, s - 1)
            part = b.at[pl.ds(cut, rows - cut)] if last else b
            self.send(part, part, down, s, self.back)
            self.send(b, b, side, s, self.flip)
            for d in sorted({1 - s, s - 1}):
                ready(d)
        far = slot(self.device(half))
        self.wait(far.at[pl.ds(0, cut)], up, half - 1)
        self.wait(far.at[pl.ds(cut, rows - cut)], down, half - 1)
        self.send(far, far, side, half, self.flip)
        for d in sorted({1 - half, half - 1}):
            ready(d)
        ready(half)
        self.drain()


    def scatter(self, rows, produce, mine, out, came, far, up_in, down_in, up, down, side, finish):
        half, chips = self.half, self.chips
        cut = rows // 2
        strip = 16
        made = {}

        def make(d):
            made[d] = len(made) % mine.shape[0]
            produce(d, mine.at[made[d]], out.at[d % chips])
            self.send(out.at[d % chips], came.at[d % chips], side, d % chips, self.flip)

        def joined(d, at):
            return mine[made[d], at, :] + came[d % chips, at, :].astype(F32)

        def strips(first, last, body):
            def step(i, carry):
                body(pl.ds(pl.multiple_of(first + i * strip, strip), strip))
                return carry

            lax.fori_loop(0, (last - first) // strip, step, 0)

        for d in (half, half - 1, 1 - half):
            make(d)
        self.wait(came.at[half], side, half)

        def far_sum(at):
            far[at, :] = joined(half, at).astype(BF)

        strips(0, rows, far_sum)
        low, high = pl.ds(0, cut), pl.ds(cut, rows - cut)
        self.send(far.at[low], up_in.at[0, low], up, 0, self.ahead)
        self.send(far.at[high], down_in.at[0, high], down, 0, self.back)
        for s in range(half - 1, 0, -1):
            i = half - s
            for d in sorted({s - 1, 1 - s}):
                make(d)
            for d, buf, sems, target in (
                (s, up_in, up, self.ahead),
                (-s, down_in, down, self.back),
            ):
                self.wait(came.at[d % chips], side, d % chips)

                def fresh(at, d=d, buf=buf, i=i):
                    buf[i - 1, at, :] = joined(d, at).astype(BF)

                def onto(at, d=d, buf=buf, i=i):
                    buf[i - 1, at, :] = (joined(d, at) + buf[i - 1, at, :].astype(F32)).astype(BF)

                if i > 1:
                    self.wait(buf.at[i - 1], sems, i - 1)
                    strips(0, rows, onto)
                elif d > 0:
                    self.wait(buf.at[0, low], sems, 0)
                    strips(0, cut, onto)
                    strips(cut, rows, fresh)
                else:
                    self.wait(buf.at[0, high], sems, 0)
                    strips(0, cut, fresh)
                    strips(cut, rows, onto)
                self.send(buf.at[i - 1], buf.at[i], sems, i, target)
        self.wait(came.at[0], side, 0)
        self.wait(up_in.at[half - 1], up, half - 1)
        self.wait(down_in.at[half - 1], down, half - 1)

        def total(at):
            finish(
                joined(0, at)
                + up_in[half - 1, at, :].astype(F32)
                + down_in[half - 1, at, :].astype(F32),
                at,
            )

        strips(0, rows, total)
        self.drain()


def scatter_scratch(chips, rows, width):
    half = chips // 2
    return [
        pltpu.VMEM((4, rows, width), F32),
        pltpu.VMEM((chips, rows, width), BF),
        pltpu.VMEM((chips, rows, width), BF),
        pltpu.VMEM((rows, width), BF),
        pltpu.VMEM((half, rows, width), BF),
        pltpu.VMEM((half, rows, width), BF),
    ]


def dot_nt(a, b):
    return lax.dot_general(a, b, (((1,), (1,)), ((), ())), preferred_element_type=F32)


def tiles(count, width, body):
    def step(i, carry):
        body(pl.ds(pl.multiple_of(i * width, width), width))
        return carry

    lax.fori_loop(0, count, step, 0)


def experts_kernel(
    chips, cap,
    h2_ref, dy_ref, slot_ref, weight_ref, wg_hbm, wu_hbm, wd_hbm,
    xs_ref, de_ref, act_ref, dg_ref, du_ref,
    held, dy, wg, wu, wd, xs_b, de_b, act_b, dg_b, du_b,
    up, down, side, w_sem, dy_sem, own_sem, out_sem,
):
    hops = Hops(chips)
    half = chips // 2
    tok, width = h2_ref.shape
    ff = wg.shape[1]
    order = [0]
    for s in range(1, half):
        order += [-s, s]
    order += [half]
    number = {d: i for i, d in enumerate(order)}

    loads = [
        pltpu.make_async_copy(a, b, w_sem.at[i])
        for i, (a, b) in enumerate(((wg_hbm, wg), (wu_hbm, wu), (wd_hbm, wd)))
    ]

    def dy_copy(i):
        chip = hops.chip(order[i])
        return pltpu.make_async_copy(dy_ref.at[pl.ds(2 * chip, 2)], dy.at[i % 2], dy_sem.at[i % 2])

    def out_copies(i):
        chip = hops.chip(order[i])
        pairs = ((xs_b, xs_ref), (de_b, de_ref), (act_b, act_ref), (dg_b, dg_ref), (du_b, du_ref))
        return [
            pltpu.make_async_copy(b.at[i % 2], r.at[chip], out_sem.at[i % 2, j])
            for j, (b, r) in enumerate(pairs)
        ]

    hops.meet()
    own = pltpu.make_async_copy(h2_ref, held.at[hops.me], own_sem)
    own.start()

    def use(d):
        i = number[d]
        p = i % 2
        if i == 0:
            own.wait()
            for c in loads:
                c.start()
            dy_copy(0).start()
            for c in loads:
                c.wait()
        dy_copy(i).wait()
        if i + 1 < chips:
            dy_copy(i + 1).start()
        if i >= 2:
            for c in out_copies(i - 2):
                c.wait()
        chip = hops.chip(d)
        for k in range(2):
            dev = 2 * chip + k
            hit = slot_ref[pl.ds(dev, 1), :] == lax.broadcasted_iota(jnp.int32, (cap, tok), 0)
            pick = hit.astype(F32).astype(BF)
            scale = jnp.sum(
                jnp.where(hit, weight_ref[pl.ds(dev, 1), :], 0.0), axis=1, keepdims=True
            )
            rows = pl.ds(k * cap, cap)

            def choose(at, k=k, dev=dev, pick=pick, scale=scale, rows=rows):
                xs_b[p, rows, at] = dot32(pick, held[dev, :, at]).astype(BF)
                de_b[p, rows, at] = (scale * dot32(pick, dy[p, k, :, at])).astype(BF)

            tiles(width // 512, 512, choose)

        def hidden(at):
            gpre = dot32(xs_b[p], wg[:, at])
            upre = dot32(xs_b[p], wu[:, at])
            dact = dot_nt(de_b[p], wd[at, :])
            sig = 1.0 / (1.0 + jnp.exp(-gpre))
            act_b[p, :, at] = (gpre * sig * upre).astype(BF)
            dg_b[p, :, at] = (dact * upre * sig * (1.0 + gpre * (1.0 - sig))).astype(BF)
            du_b[p, :, at] = (dact * gpre * sig).astype(BF)

        tiles(ff // 256, 256, hidden)
        for c in out_copies(i):
            c.start()

    hops.gather(h2_ref, lambda dev: held.at[dev], up, down, side, use)
    for i in (chips - 2, chips - 1):
        for c in out_copies(i):
            c.wait()


def expert_rows(chips, cap, h2, dy_all, slot, weight, wg, wu, wd, collective_id):
    tok, width = h2.shape
    ff = wg.shape[1]
    anywhere = pl.BlockSpec(memory_space=pl.ANY)
    vmem = pl.BlockSpec(memory_space=pltpu.VMEM)
    wide = jax.ShapeDtypeStruct((chips, 2 * cap, width), BF)
    thin = jax.ShapeDtypeStruct((chips, 2 * cap, ff), BF)
    return pl.pallas_call(
        functools.partial(experts_kernel, chips, cap),
        out_shape=(wide, wide, thin, thin, thin),
        in_specs=[anywhere, anywhere, vmem, vmem, anywhere, anywhere, anywhere],
        out_specs=(anywhere,) * 5,
        scratch_shapes=[
            pltpu.VMEM((2 * chips, tok, width), BF),
            pltpu.VMEM((2, 2, tok, width), BF),
            pltpu.VMEM((width, ff), BF),
            pltpu.VMEM((width, ff), BF),
            pltpu.VMEM((ff, width), BF),
            pltpu.VMEM((2, 2 * cap, width), BF),
            pltpu.VMEM((2, 2 * cap, width), BF),
            pltpu.VMEM((2, 2 * cap, ff), BF),
            pltpu.VMEM((2, 2 * cap, ff), BF),
            pltpu.VMEM((2, 2 * cap, ff), BF),
            *ring_sems(chips),
            DMA((3,)),
            DMA((2,)),
            DMA,
            DMA((2, 5)),
        ],
        compiler_params=pltpu.CompilerParams(
            collective_id=collective_id, has_side_effects=True, vmem_limit_bytes=VMEM_LIMIT
        ),
        cost_estimate=pl.CostEstimate(
            flops=2 * chips * cap * width * ff * 6, transcendentals=0, bytes_accessed=200 << 20
        ),
        name="experts",
    )(h2, dy_all, slot, weight, wg, wu, wd)


def rows_back_kernel(
    chips, cap,
    dg_ref, du_ref, slot_ref, wg_hbm, wu_hbm, total_ref,
    wg, wu, dg, du, drow, mine, out, came, far, up_in, down_in,
    up, down, side, w_sem, in_sem,
):
    hops = Hops(chips)
    half = chips // 2
    tok, width = total_ref.shape
    order = [half]
    for s in range(half - 1, 0, -1):
        order += [s, -s] if s == half - 1 else [-s, s]
    order += [0]
    number = {d: i for i, d in enumerate(order)}
    loads = [
        pltpu.make_async_copy(a, b, w_sem.at[i])
        for i, (a, b) in enumerate(((wg_hbm, wg), (wu_hbm, wu)))
    ]

    def in_copies(i):
        chip = hops.chip(order[i])
        return [
            pltpu.make_async_copy(r.at[chip], b.at[i % 2], in_sem.at[i % 2, j])
            for j, (r, b) in enumerate(((dg_ref, dg), (du_ref, du)))
        ]

    for c in loads + in_copies(0):
        c.start()
    hops.meet()
    for c in loads:
        c.wait()

    def produce(d, same_ref, other_ref):
        i = number[d]
        p = i % 2
        for c in in_copies(i):
            c.wait()
        if i + 1 < chips:
            for c in in_copies(i + 1):
                c.start()

        def back(at):
            drow[:, at] = (dot_nt(dg[p], wg[at, :]) + dot_nt(du[p], wu[at, :])).astype(BF)

        tiles(width // 256, 256, back)
        chip = hops.chip(d)
        lanes = lax.broadcasted_iota(jnp.int32, (tok, cap), 1)

        def pick(k):
            return (slot_ref[2 * chip + k] == lanes).astype(F32).astype(BF)

        same, other = hops.core, 1 - hops.core
        same_pick, other_pick = pick(same), pick(other)
        same_rows = pl.ds(pl.multiple_of(same * cap, 16), cap)
        other_rows = pl.ds(pl.multiple_of(other * cap, 16), cap)

        def spread(at):
            same_ref[:, at] = dot32(same_pick, drow[same_rows, at])
            other_ref[:, at] = dot32(other_pick, drow[other_rows, at]).astype(BF)

        tiles(width // 512, 512, spread)

    def finish(value, at):
        total_ref[at, :] = value

    hops.scatter(
        tok, produce, mine, out, came, far, up_in, down_in, up, down, side, finish
    )


def rows_back(chips, cap, dg, du, slot, wg, wu, collective_id):
    tok = slot.shape[1]
    width, ff = wg.shape
    anywhere = pl.BlockSpec(memory_space=pl.ANY)
    vmem = pl.BlockSpec(memory_space=pltpu.VMEM)
    return pl.pallas_call(
        functools.partial(rows_back_kernel, chips, cap),
        out_shape=jax.ShapeDtypeStruct((tok, width), F32),
        in_specs=[anywhere, anywhere, vmem, anywhere, anywhere],
        out_specs=vmem,
        scratch_shapes=[
            pltpu.VMEM((width, ff), BF),
            pltpu.VMEM((width, ff), BF),
            pltpu.VMEM((2, 2 * cap, ff), BF),
            pltpu.VMEM((2, 2 * cap, ff), BF),
            pltpu.VMEM((2 * cap, width), BF),
            *scatter_scratch(chips, tok, width),
            *ring_sems(chips),
            DMA((2,)),
            DMA((2, 2)),
        ],
        compiler_params=pltpu.CompilerParams(
            collective_id=collective_id, has_side_effects=True, vmem_limit_bytes=VMEM_LIMIT
        ),
        cost_estimate=pl.CostEstimate(
            flops=2 * chips * cap * width * ff * 6, transcendentals=0, bytes_accessed=200 << 20
        ),
        name="rows_back",
    )(dg, du, slot, wg, wu)


def qkv_gradient_kernel(
    chips, h1_ref, grad_ref, total_ref, mine, out, came, far, up_in, down_in, up, down, side
):
    hops = Hops(chips)
    shard, width = total_ref.shape
    hops.meet()

    def produce(d, same_ref, other_ref):
        first = 2 * hops.chip(d) * shard
        rows = pl.ds(pl.multiple_of(first, 2 * shard), 2 * shard)

        def block(at):
            value = dot32(h1_ref[rows, :], grad_ref[:, at])
            same_ref[:, at] = value[:shard]
            other_ref[:, at] = value[shard:].astype(BF)

        tiles(width // 512, 512, block)

    def finish(value, at):
        total_ref[at, :] = value.astype(BF)

    hops.scatter(
        shard, produce, mine, out, came, far, up_in, down_in, up, down, side, finish
    )


def qkv_gradient(chips, h1_t, grad, collective_id):
    shard = h1_t.shape[0] // (2 * chips)
    width = grad.shape[1]
    vmem = pl.BlockSpec(memory_space=pltpu.VMEM)
    return pl.pallas_call(
        functools.partial(qkv_gradient_kernel, chips),
        out_shape=jax.ShapeDtypeStruct((shard, width), BF),
        in_specs=[vmem, vmem],
        out_specs=vmem,
        scratch_shapes=[*scatter_scratch(chips, shard, width), *ring_sems(chips)],
        compiler_params=pltpu.CompilerParams(
            collective_id=collective_id, has_side_effects=True, vmem_limit_bytes=VMEM_LIMIT
        ),
        cost_estimate=pl.CostEstimate(
            flops=2 * h1_t.size * width, transcendentals=0, bytes_accessed=200 << 20
        ),
        name="qkv_gradient",
    )(h1_t, grad)


def gather_kernel(chips, own_ref, all_ref, up, down, side, local):
    hops = Hops(chips)
    hops.meet()
    mine = pltpu.make_async_copy(own_ref, all_ref.at[hops.me], local)
    mine.start()
    hops.gather(own_ref, lambda dev: all_ref.at[dev], up, down, side, lambda d: None)
    mine.wait()


def ring_sems(chips):
    return [DMA((2, chips // 2)), DMA((2, chips // 2)), DMA((2, chips))]


def ring_gather(chips, own, collective_id, name):
    anywhere = pl.BlockSpec(memory_space=pl.ANY)
    return pl.pallas_call(
        functools.partial(gather_kernel, chips),
        out_shape=jax.ShapeDtypeStruct((2 * chips, *own.shape), own.dtype),
        in_specs=[anywhere],
        out_specs=anywhere,
        scratch_shapes=[*ring_sems(chips), DMA],
        compiler_params=pltpu.CompilerParams(collective_id=collective_id, has_side_effects=True),
        cost_estimate=pl.CostEstimate(
            flops=0, transcendentals=0, bytes_accessed=4 * chips * own.size * own.dtype.itemsize
        ),
        name=name,
    )(own)


def out_gradient(ring, grad, reps, heads, rel, rep, grp):
    if reps != 2 or heads != ring.chips:
        whole = lax.dynamic_update_slice(
            jnp.zeros((heads, reps, HD, D), BF), grad.reshape(heads, 1, HD, D), (0, rep, 0, 0)
        ).reshape(D, D)
        part = lax.psum_scatter(whole, "grp", scatter_dimension=0, tiled=True)
        return lax.psum(part, "rep").astype(F32)
    n = ring.devices
    owners = [(r, 2 * chip + r) for r in range(2) for chip in range(ring.chips)]

    def send(v, where):
        pairs = []
        for r, dev in owners:
            src, dst = where(r, dev)
            pairs.append((src[0] * n + src[1], dst[0] * n + dst[1]))
        return lax.ppermute(v, ("rep", "grp"), pairs)

    def hop(v, shift):
        def to(r, dev):
            chip = ring.cycle[(ring.place[dev // 2] + shift) % ring.chips]
            return (r, dev), (r, 2 * chip + r)

        return send(v, to)

    other = send(grad, lambda r, dev: ((r, dev ^ 1), (r, dev)))
    both = (grad.astype(F32) + other.astype(F32)).reshape(heads, HD, D)

    def block(d):
        return lax.dynamic_index_in_dim(both, rel[d, 0] // 2, 0, False)

    far = block(ring.half).astype(BF)
    rows = HD // 2
    up, down = hop(far[:rows], 1), hop(far[rows:], -1)
    zero = jnp.zeros_like(up)
    up = jnp.concatenate([up, zero], axis=0)
    down = jnp.concatenate([zero, down], axis=0)
    for step in range(ring.half - 1, 0, -1):
        up = hop((block(step) + up.astype(F32)).astype(BF), 1)
        down = hop((block(-step % ring.chips) + down.astype(F32)).astype(BF), -1)
    total = (block(0) + up.astype(F32) + down.astype(F32)).astype(BF)
    mine = send(total, lambda r, dev: ((r, dev), (1 - r, dev)))
    return jnp.where(grp % 2 == rep, total, mine).astype(F32)


def per_device(
    tokens, w_qkv, w_out, gains, w_gate, w_up, w_down, segment_ids, routes, gate_weights, cotangent
):
    groups = lax.axis_size("grp")
    reps = lax.axis_size("rep")
    ring = Ring(groups)
    rep, grp = lax.axis_index("rep"), lax.axis_index("grp")
    rel = jnp.asarray(ring.table())[grp]
    tok_rows = tokens.shape[1]
    seq_len = segment_ids.shape[1]
    heads = HEADS // reps
    wide = heads * HD
    score_scale = HD ** (-0.5)

    def from_rep(v, k):
        return lax.ppermute(v, "rep", [((s + k) % reps, s) for s in range(reps)])

    def to_rep(v, k):
        return lax.ppermute(v, "rep", [(s, (s + k) % reps) for s in range(reps)])

    def rep_gather(v):
        return jnp.concatenate([v] + [from_rep(v, k) for k in range(1, reps)], axis=0)

    def rep_scatter(v):
        parts = v.reshape(reps, tok_rows, v.shape[-1])
        out = parts[0].astype(F32)
        for k in range(1, reps):
            out = out + to_rep(parts[k].astype(BF), k).astype(F32)
        return out

    own_b = tokens[0]
    seq_b = rep_gather(own_b)
    gates_f = gate_weights[0]
    experts = jnp.arange(groups, dtype=jnp.int32)
    weight_of = jnp.sum(
        jnp.where(routes[0][None] == experts[:, None, None], gates_f[None], 0.0), axis=-1
    )
    small = jnp.concatenate(
        [
            weight_of,
            jnp.broadcast_to(gains.astype(F32)[None], (groups, gains.shape[0])),
        ],
        axis=1,
    )
    small = lax.all_to_all(small, "grp", split_axis=0, concat_axis=0, tiled=True)
    gains_f = small[:, tok_rows:].reshape(-1)
    weight_in = small[:, :tok_rows]
    g_attn = gains_f[:D]
    g_ffn = gains_f[D : 2 * D]
    g_query = gains_f[2 * D : 2 * D + HD]
    g_key = gains_f[2 * D + HD :]

    my_qkv = lax.dynamic_index_in_dim(
        w_qkv.reshape(w_qkv.shape[0], 3, heads, reps, HD), rep, axis=3, keepdims=False
    ).reshape(w_qkv.shape[0], 3 * wide)
    shard = my_qkv.shape[0]
    full_qkv = ring_gather(ring.chips, my_qkv, 1, "gather_qkv").reshape(D, 3 * wide)
    full_out = lax.all_gather(w_out, "grp", axis=0, tiled=True)
    my_out = lax.dynamic_index_in_dim(
        full_out.reshape(heads, reps, HD, D), rep, axis=1, keepdims=False
    ).reshape(wide, D)

    cot_late, full_qkv = lax.optimization_barrier((cotangent[0], full_qkv))
    dy_all = lax.all_gather(cot_late, "grp", axis=0, tiled=False)

    seq_f = seq_b.astype(F32)
    normed_one, hat_one, inv_one = rms_forward(seq_f, g_attn)
    h1_b = normed_one.astype(BF)
    projected = dot32(h1_b, full_qkv)
    q_pre = projected[:, :wide].reshape(seq_len, heads, HD)
    k_pre = projected[:, wide : 2 * wide].reshape(seq_len, heads, HD)
    v_pre = projected[:, 2 * wide :]
    q_normed, q_hat, q_inv = rms_forward(q_pre, g_query)
    k_normed, k_hat, k_inv = rms_forward(k_pre, g_key)
    order = jnp.concatenate(
        [((rep + k) % reps) * tok_rows + jnp.arange(tok_rows, dtype=jnp.int32) for k in range(reps)]
    )
    positions = order.astype(F32)
    q_b = rotate(q_normed, positions, 1.0).astype(BF)
    k_b = rotate(k_normed, positions, 1.0).astype(BF)
    v_b = v_pre.astype(BF).reshape(seq_len, heads, HD)
    docs = segment_ids[0][order]
    same_doc = (docs[:, None] == docs[None, :])[None]
    scores = jnp.where(
        same_doc,
        jnp.einsum("qhd,khd->hqk", q_b, k_b, preferred_element_type=F32) * score_scale,
        -1e30,
    )
    row_max = jnp.max(scores, axis=-1, keepdims=True)
    log_total = row_max + jnp.log(jnp.sum(jnp.exp(scores - row_max), axis=-1, keepdims=True))
    probs_f = jnp.exp(scores - log_total)
    probs_b = probs_f.astype(BF)
    attended = jnp.einsum("hqk,khd->qhd", probs_b, v_b, preferred_element_type=F32)
    attended_b = attended.reshape(seq_len, wide).astype(BF)
    mid_rows = own_b.astype(F32) + rep_scatter(dot32(attended_b, my_out))
    normed_two, hat_two, inv_two = rms_forward(mid_rows, g_ffn)
    h2_b = normed_two.astype(BF)

    chips = ring.chips
    entries = tok_rows * TOP
    capacity = min(tok_rows, (9 * entries + 8 * groups - 1) // (8 * groups))
    capacity = -(-capacity // 16) * 16
    named = weight_in > 0
    before = dot32(
        named.astype(BF), jnp.tri(tok_rows, dtype=BF).T
    )
    slot = jnp.where(named, before - 1.0, -1.0).astype(jnp.int32)
    rows_in, grads_in, acts, grad_gates, grad_ups = expert_rows(
        chips, capacity, h2_b, dy_all, slot, weight_in, w_gate[0], w_up[0], w_down[0], 2
    )
    cuts = 1 if chips <= 8 else chips // 8
    grad_h2 = jnp.concatenate(
        [
            rows_back(chips, capacity, grad_gates, grad_ups, slot[:, :, None], wg, wu, 8 + i)
            for i, (wg, wu) in enumerate(
                zip(jnp.split(w_gate[0], cuts), jnp.split(w_up[0], cuts), strict=True)
            )
        ],
        axis=1,
    )

    pick = (slot[:, None, :] == jnp.arange(capacity, dtype=jnp.int32)[None, :, None]).astype(BF)
    row_weight = jnp.sum(pick.astype(F32) * weight_in[:, None, :], axis=-1)
    all_rows = rows_in.reshape(-1, D)
    all_grads = grads_in.reshape(-1, D)
    all_acts = acts.reshape(groups * capacity, -1)
    all_gates = grad_gates.reshape(groups * capacity, -1)
    all_ups = grad_ups.reshape(groups * capacity, -1)
    eout = dot32(all_acts, w_down[0]).astype(BF).astype(F32)
    eout = (row_weight.reshape(-1, 1) * eout).astype(BF).reshape(groups, capacity, D)
    out_all = jnp.einsum("gct,gcd->gtd", pick, eout, preferred_element_type=F32).astype(BF)
    out_sum = lax.psum_scatter(
        out_all.reshape(groups * tok_rows, D), "grp", scatter_dimension=0, tiled=True
    )

    def rep_send(v):
        v = v.astype(BF)
        return [v] + [from_rep(v, k) for k in range(1, reps)]

    def rep_sum(parts, after):
        parts, _ = lax.optimization_barrier((parts, after))
        out = parts[0].astype(F32)
        for part in parts[1:]:
            out = out + part.astype(F32)
        return out

    grad_wdown = rep_send(jnp.einsum("rf,rd->fd", all_acts, all_grads, preferred_element_type=F32))
    grad_wgate = rep_send(jnp.einsum("rd,rf->df", all_rows, all_gates, preferred_element_type=F32))
    grad_wup = rep_send(jnp.einsum("rd,rf->df", all_rows, all_ups, preferred_element_type=F32))

    grad_out = cotangent[0].astype(F32)
    grad_mid_norm, ffn_terms = rms_backward(grad_h2, hat_two, inv_two, g_ffn)
    grad_mid = grad_out + grad_mid_norm
    grad_branch_b = rep_gather(grad_mid.astype(BF))
    grad_wout = jnp.einsum("td,te->de", attended_b, grad_branch_b, preferred_element_type=F32)
    grad_attn_b = (
        jnp.einsum("te,de->td", grad_branch_b, my_out, preferred_element_type=F32)
        .astype(BF)
        .reshape(seq_len, heads, HD)
    )
    grad_probs = jnp.einsum("qhd,khd->hqk", grad_attn_b, v_b, preferred_element_type=F32)
    grad_vals = jnp.einsum("hqk,qhd->khd", probs_b, grad_attn_b, preferred_element_type=F32)
    grad_scores = (
        probs_f * (grad_probs - jnp.sum(probs_f * grad_probs, axis=-1, keepdims=True))
    ).astype(BF)
    grad_q = jnp.einsum("hqk,khd->qhd", grad_scores, k_b, preferred_element_type=F32) * score_scale
    grad_k = jnp.einsum("hqk,qhd->khd", grad_scores, q_b, preferred_element_type=F32) * score_scale
    grad_qn = rotate(grad_q, positions, -1.0)
    grad_kn = rotate(grad_k, positions, -1.0)
    grad_q_pre, query_terms = rms_backward(grad_qn, q_hat, q_inv, g_query)
    grad_k_pre, key_terms = rms_backward(grad_kn, k_hat, k_inv, g_key)
    grad_proj = jnp.concatenate(
        [
            grad_q_pre.reshape(seq_len, wide),
            grad_k_pre.reshape(seq_len, wide),
            grad_vals.reshape(seq_len, wide),
        ],
        axis=1,
    ).astype(BF)
    grad_h1 = rep_scatter(
        jnp.einsum("te,de->td", grad_proj, full_qkv, preferred_element_type=F32)
    )
    grad_rows_one, attn_terms = rms_backward(
        grad_h1, hat_one[:tok_rows], inv_one[:tok_rows], g_attn
    )
    grad_tokens = grad_mid + grad_rows_one

    h1_t = h1_b.T.reshape(chips, 2, shard, seq_len)
    h1_t = jnp.where(grp % 2 == 0, h1_t, h1_t[:, ::-1]).reshape(D, seq_len)
    shard_qkv = qkv_gradient(chips, h1_t, grad_proj, 4)
    grad_wdown = rep_sum(grad_wdown, grad_proj)
    qkv_all = [shard_qkv] + [from_rep(shard_qkv, k) for k in range(1, reps)]
    columns = jnp.stack(qkv_all, axis=0).reshape(reps, shard, 3, heads, HD)
    columns = columns[(jnp.arange(reps) - rep) % reps]
    shard_qkv = columns.transpose(1, 2, 3, 0, 4).reshape(shard, 3 * D).astype(F32)

    grad_wgate = rep_sum(grad_wgate, shard_qkv)
    grad_wup = rep_sum(grad_wup, shard_qkv)
    result = mid_rows + lax.optimization_barrier((out_sum, shard_qkv))[0].astype(F32)

    shard_out = out_gradient(ring, grad_wout.astype(BF), reps, heads, rel, rep, grp)

    grad_gains = jnp.concatenate(
        [
            jnp.sum(attn_terms, axis=0),
            jnp.sum(ffn_terms, axis=0),
            jnp.sum(query_terms, axis=(0, 1)),
            jnp.sum(key_terms, axis=(0, 1)),
        ]
    )
    pieces = lax.all_to_all(
        grad_gains.reshape(groups, -1), "grp", split_axis=0, concat_axis=0, tiled=True
    )
    shard_gains = jnp.sum(pieces, axis=0)
    total = shard_gains
    for k in range(1, reps):
        total = total + from_rep(shard_gains, k)
    return (
        result[None],
        grad_tokens[None],
        shard_qkv,
        shard_out,
        total,
        grad_wgate[None],
        grad_wup[None],
        grad_wdown[None],
    )


def solution(mesh):
    in_specs = (
        P("grp", "rep", None),
        P("grp", None),
        P("grp", None),
        P("grp"),
        P("grp", None, None),
        P("grp", None, None),
        P("grp", None, None),
        P("grp", None),
        P("grp", "rep", None),
        P("grp", "rep", None),
        P("grp", "rep", None),
    )
    out_specs = (
        P("grp", "rep", None),
        P("grp", "rep", None),
        P("grp", None),
        P("grp", None),
        P("grp"),
        P("grp", None, None),
        P("grp", None, None),
        P("grp", None, None),
    )
    return jax.shard_map(
        per_device, mesh=mesh, in_specs=in_specs, out_specs=out_specs, check_vma=False
    )
```

```python
import functools

import jax
import jax.numpy as jnp
import numpy as np
from jax import lax
from jax.experimental import pallas as pl
from jax.experimental.pallas import tpu as pltpu
from jax.sharding import PartitionSpec as P

D = 2048
HEADS = 16
HD = 128
TOP = 8
BF = jnp.bfloat16
F32 = jnp.float32

epsilon = 1e-06
rope_base = 10000.0


def rms_forward(values, gain_vec):
    inverse = lax.rsqrt(jnp.mean(values * values, axis=-1, keepdims=True) + epsilon)
    normed = values * inverse
    return (normed * gain_vec, normed, inverse)


def rms_backward(grad_out, normed, inverse, gain_vec):
    scaled = grad_out * gain_vec
    grad_in = inverse * (scaled - normed * jnp.mean(scaled * normed, axis=-1, keepdims=True))
    return (grad_in, grad_out * normed)


def dot32(a, b):
    return jnp.dot(a, b, preferred_element_type=F32)


class Ring:
    def __init__(self, devices):
        self.devices = devices
        self.chips = devices // 2
        outer = 4 if self.chips % 4 == 0 else 2
        inner = self.chips // outer
        cycle = [(a, 0) for a in range(outer)]
        for step, a in enumerate(reversed(range(outer))):
            columns = range(1, inner)
            cycle += [(a, b) for b in (columns if step % 2 == 0 else reversed(columns))]
        self.cycle = [a * inner + b for a, b in cycle]
        self.place = {chip: i for i, chip in enumerate(self.cycle)}
        self.half = self.chips // 2

    def perm(self, shift):
        pairs = []
        for chip in range(self.chips):
            other = self.cycle[(self.place[chip] + shift) % self.chips]
            pairs += [(2 * chip + core, 2 * other + core) for core in range(2)]
        return pairs

    def table(self):
        out = np.zeros((self.devices, self.chips, 2), np.int32)
        for dev in range(self.devices):
            chip, core = dev // 2, dev % 2
            for d in range(self.chips):
                other = self.cycle[(self.place[chip] + d) % self.chips]
                out[dev, d, 0] = 2 * other + core
                out[dev, d, 1] = 2 * other + (1 - core)
        return out

    def ahead(self, v):
        return lax.ppermute(v, "grp", self.perm(1))

    def back(self, v):
        return lax.ppermute(v, "grp", self.perm(-1))

    def flip(self, v):
        return lax.ppermute(v, "grp", [(i, i ^ 1) for i in range(self.devices)])

    def gather(self, own):
        rows = own.shape[0] // 2
        blocks = {0: (own, self.flip(own))}
        up = down = own
        for step in range(1, self.half):
            up, down = self.ahead(up), self.back(down)
            blocks[-step % self.chips] = (up, self.flip(up))
            blocks[step] = (down, self.flip(down))
        first, last = self.ahead(up[:rows]), self.back(down[rows:])
        far = jnp.concatenate([first, last], axis=0)
        blocks[self.half] = (far, self.flip(far))
        return blocks

    def scatter_sum(self, blocks):
        def joined(d):
            same, other = blocks[d]
            return same.astype(F32) + self.flip(other.astype(BF)).astype(F32)

        far = joined(self.half).astype(BF)
        rows = far.shape[0] // 2
        up, down = self.ahead(far[:rows]), self.back(far[rows:])
        zero = jnp.zeros_like(up)
        up = jnp.concatenate([up, zero], axis=0)
        down = jnp.concatenate([zero, down], axis=0)
        for step in range(self.half - 1, 0, -1):
            up = self.ahead((joined(step) + up.astype(F32)).astype(BF))
            down = self.back((joined(-step % self.chips) + down.astype(F32)).astype(BF))
        return joined(0) + up.astype(F32) + down.astype(F32)


MESH = pl.DeviceIdType.MESH
DMA = pltpu.SemaphoreType.DMA
VMEM_LIMIT = 60 << 20


class Hops:
    def __init__(self, chips):
        self.chips, self.half = chips, chips // 2
        self.outer = 4 if chips % 4 == 0 else 2
        self.inner = chips // self.outer
        self.me = lax.axis_index("grp")
        chip, self.core = self.me // 2, self.me % 2
        a, b = chip // self.inner, chip % self.inner
        row = self.outer - 1 - a
        along = jnp.where(row % 2 == 0, b - 1, self.inner - 1 - b)
        self.place = jnp.where(b == 0, a, self.outer + row * (self.inner - 1) + along)
        self.ahead, self.back = self.device(1), self.device(-1)
        self.flip = self.me + 1 - 2 * self.core
        self.started = []

    def chip(self, d):
        p = (self.place + (d % self.chips)) % self.chips
        q = jnp.maximum(p - self.outer, 0)
        k, m = q // (self.inner - 1), q % (self.inner - 1)
        b = jnp.where(k % 2 == 0, m + 1, self.inner - 1 - m)
        return jnp.where(
            p < self.outer, p * self.inner, (self.outer - 1 - k) * self.inner + b
        )

    def device(self, d):
        return 2 * self.chip(d) + self.core

    def meet(self, reps=1):
        barrier = pltpu.get_barrier_semaphore()
        for dev in (self.ahead, self.back, self.flip):
            pl.semaphore_signal(barrier, inc=1, device_id={"grp": dev}, device_id_type=MESH)
        rep = lax.axis_index("rep")
        for k in range(1, reps):
            pl.semaphore_signal(
                barrier, inc=1, device_id={"rep": (rep + k) % reps}, device_id_type=MESH
            )
        pl.semaphore_wait(barrier, 2 + reps)

    def copy(self, src, dst, send_sem, recv_sem, dev):
        return pltpu.make_async_remote_copy(
            src_ref=src,
            dst_ref=dst,
            send_sem=send_sem,
            recv_sem=recv_sem,
            device_id={"grp": dev},
            device_id_type=MESH,
        )

    def send(self, src, dst, sems, at, dev):
        c = self.copy(src, dst, sems.at[0, at], sems.at[1, at], dev)
        c.start()
        self.started.append(c)

    def wait(self, dst, sems, at):
        self.copy(dst, dst, sems.at[0, at], sems.at[1, at], self.flip).wait_recv()

    def drain(self):
        for c in self.started:
            c.wait_send()

    def gather(self, items, use):
        half = self.half

        def parts(ref):
            cut = ref.shape[0] // 2
            return ref.at[pl.ds(0, cut)], ref.at[pl.ds(cut, ref.shape[0] - cut)]

        for own, slot, up, down, side in items:
            self.send(own, slot(self.me), up, 0, self.ahead)
            self.send(own, slot(self.me), down, 0, self.back)
            self.send(own, slot(self.me), side, 0, self.flip)
        yield

        def ready(d):
            dev = self.device(d)
            for _, slot, _, _, side in items:
                self.wait(slot(dev + 1 - 2 * self.core), side, d % self.chips)
            use(d)

        ready(0)
        for s in range(1, half):
            last = s == half - 1
            for _, slot, up, down, side in items:
                a, b = slot(self.device(-s)), slot(self.device(s))
                self.wait(a, up, s - 1)
                part = parts(a)[0] if last else a
                self.send(part, part, up, s, self.ahead)
                self.send(a, a, side, -s % self.chips, self.flip)
                self.wait(b, down, s - 1)
                part = parts(b)[1] if last else b
                self.send(part, part, down, s, self.back)
                self.send(b, b, side, s, self.flip)
            for d in (-s, s):
                ready(d)
            yield
        for _, slot, up, down, side in items:
            far = slot(self.device(half))
            low, high = parts(far)
            self.wait(low, up, half - 1)
            self.wait(high, down, half - 1)
            self.send(far, far, side, half, self.flip)
        ready(half)

    def scatter(self, rows, produce, mine, out, came, far, up_in, down_in, up, down, side, finish):
        half, chips = self.half, self.chips
        cut = rows // 2
        strip = 16
        made = {}

        def make(d):
            made[d] = len(made) % mine.shape[0]
            produce(d, mine.at[made[d]], out.at[d % chips])
            self.send(out.at[d % chips], came.at[d % chips], side, d % chips, self.flip)

        def joined(d, at):
            return mine[made[d], at, :] + came[d % chips, at, :].astype(F32)

        def strips(first, last, body):
            def step(i, carry):
                body(pl.ds(pl.multiple_of(first + i * strip, strip), strip))
                return carry

            lax.fori_loop(0, (last - first) // strip, step, 0)

        for d in (half, half - 1):
            make(d)
        self.wait(came.at[half], side, half)

        def far_sum(at):
            far[at, :] = joined(half, at).astype(BF)

        strips(0, rows, far_sum)
        low, high = pl.ds(0, cut), pl.ds(cut, rows - cut)
        self.send(far.at[low], up_in.at[0, low], up, 0, self.ahead)
        self.send(far.at[high], down_in.at[0, high], down, 0, self.back)
        make(1 - half)
        yield
        for s in range(half - 1, 0, -1):
            i = half - s
            for d in sorted({s - 1, 1 - s}):
                make(d)
            for d, buf, sems, target in (
                (s, up_in, up, self.ahead),
                (-s, down_in, down, self.back),
            ):
                self.wait(came.at[d % chips], side, d % chips)

                def fresh(at, d=d, buf=buf, i=i):
                    buf[i - 1, at, :] = joined(d, at).astype(BF)

                def onto(at, d=d, buf=buf, i=i):
                    buf[i - 1, at, :] = (joined(d, at) + buf[i - 1, at, :].astype(F32)).astype(BF)

                if i > 1:
                    self.wait(buf.at[i - 1], sems, i - 1)
                    strips(0, rows, onto)
                elif d > 0:
                    self.wait(buf.at[0, low], sems, 0)
                    strips(0, cut, onto)
                    strips(cut, rows, fresh)
                else:
                    self.wait(buf.at[0, high], sems, 0)
                    strips(0, cut, fresh)
                    strips(cut, rows, onto)
                self.send(buf.at[i - 1], buf.at[i], sems, i, target)
            yield
        self.wait(came.at[0], side, 0)
        self.wait(up_in.at[half - 1], up, half - 1)
        self.wait(down_in.at[half - 1], down, half - 1)

        def total(at):
            finish(
                joined(0, at)
                + up_in[half - 1, at, :].astype(F32)
                + down_in[half - 1, at, :].astype(F32),
                at,
            )

        strips(0, rows, total)

    def turn(self, *rings):
        rings = list(rings)
        while rings:
            rings = [r for r in rings if next(r, self) is not self]
        self.drain()


def scatter_scratch(chips, rows, width):
    half = chips // 2
    return [
        pltpu.VMEM((4, rows, width), F32),
        pltpu.VMEM((chips, rows, width), BF),
        pltpu.VMEM((chips, rows, width), BF),
        pltpu.VMEM((rows, width), BF),
        pltpu.VMEM((half, rows, width), BF),
        pltpu.VMEM((half, rows, width), BF),
    ]


def dot_nt(a, b):
    return lax.dot_general(a, b, (((1,), (1,)), ((), ())), preferred_element_type=F32)


def dot_tn(a, b):
    return lax.dot_general(a, b, (((0,), (0,)), ((), ())), preferred_element_type=F32)


def tiles(count, width, body):
    for i in range(count):
        body(pl.ds(i * width, width))


def experts_kernel(
    chips, cap,
    h2_ref, dy_ref, slot_ref, weight_ref, wg_hbm, wu_hbm, wd_hbm,
    xs_ref, de_ref, act_ref, dg_ref, du_ref,
    held, dy, wg, wu, wd, xs_b, de_b, act_b, dg_b, du_b,
    up, down, side, w_sem, dy_sem, own_sem, out_sem,
):
    hops = Hops(chips)
    half = chips // 2
    tok, width = h2_ref.shape
    ff = wg.shape[1]
    order = [0]
    for s in range(1, half):
        order += [-s, s]
    order += [half]
    number = {d: i for i, d in enumerate(order)}

    loads = [
        pltpu.make_async_copy(a, b, w_sem.at[i])
        for i, (a, b) in enumerate(((wg_hbm, wg), (wu_hbm, wu), (wd_hbm, wd)))
    ]

    def dy_copy(i):
        chip = hops.chip(order[i])
        return pltpu.make_async_copy(dy_ref.at[pl.ds(2 * chip, 2)], dy.at[i % 2], dy_sem.at[i % 2])

    def out_copies(i):
        chip = hops.chip(order[i])
        pairs = ((xs_b, xs_ref), (de_b, de_ref), (act_b, act_ref), (dg_b, dg_ref), (du_b, du_ref))
        return [
            pltpu.make_async_copy(b.at[i % 2], r.at[chip], out_sem.at[i % 2, j])
            for j, (b, r) in enumerate(pairs)
        ]

    hops.meet()
    own = pltpu.make_async_copy(h2_ref, held.at[hops.me], own_sem)
    own.start()

    def use(d):
        i = number[d]
        p = i % 2
        if i == 0:
            own.wait()
            for c in loads:
                c.start()
            dy_copy(0).start()
            for c in loads:
                c.wait()
        dy_copy(i).wait()
        if i + 1 < chips:
            dy_copy(i + 1).start()
        if i >= 2:
            for c in out_copies(i - 2):
                c.wait()
        chip = hops.chip(d)
        for k in range(2):
            dev = 2 * chip + k
            hit = slot_ref[pl.ds(dev, 1), :] == lax.broadcasted_iota(jnp.int32, (cap, tok), 0)
            pick = hit.astype(F32).astype(BF)
            scale = jnp.sum(
                jnp.where(hit, weight_ref[pl.ds(dev, 1), :], 0.0), axis=1, keepdims=True
            )
            rows = pl.ds(k * cap, cap)

            def choose(at, k=k, dev=dev, pick=pick, scale=scale, rows=rows):
                xs_b[p, rows, at] = dot32(pick, held[dev, :, at]).astype(BF)
                de_b[p, rows, at] = (scale * dot32(pick, dy[p, k, :, at])).astype(BF)

            tiles(width // 1024, 1024, choose)

        def hidden(at):
            gpre = dot32(xs_b[p], wg[:, at])
            upre = dot32(xs_b[p], wu[:, at])
            dact = dot_nt(de_b[p], wd[at, :])
            sig = 1.0 / (1.0 + jnp.exp(-gpre))
            act_b[p, :, at] = (gpre * sig * upre).astype(BF)
            dg_b[p, :, at] = (dact * upre * sig * (1.0 + gpre * (1.0 - sig))).astype(BF)
            du_b[p, :, at] = (dact * gpre * sig).astype(BF)

        tiles(ff // 512, 512, hidden)
        for c in out_copies(i):
            c.start()

    hops.turn(hops.gather([(h2_ref, lambda dev: held.at[dev], up, down, side)], use))
    for i in (chips - 2, chips - 1):
        for c in out_copies(i):
            c.wait()


def expert_rows(chips, cap, h2, dy_all, slot, weight, wg, wu, wd, collective_id):
    tok, width = h2.shape
    ff = wg.shape[1]
    anywhere = pl.BlockSpec(memory_space=pl.ANY)
    vmem = pl.BlockSpec(memory_space=pltpu.VMEM)
    wide = jax.ShapeDtypeStruct((chips, 2 * cap, width), BF)
    thin = jax.ShapeDtypeStruct((chips, 2 * cap, ff), BF)
    return pl.pallas_call(
        functools.partial(experts_kernel, chips, cap),
        out_shape=(wide, wide, thin, thin, thin),
        in_specs=[anywhere, anywhere, vmem, vmem, anywhere, anywhere, anywhere],
        out_specs=(anywhere,) * 5,
        scratch_shapes=[
            pltpu.VMEM((2 * chips, tok, width), BF),
            pltpu.VMEM((2, 2, tok, width), BF),
            pltpu.VMEM((width, ff), BF),
            pltpu.VMEM((width, ff), BF),
            pltpu.VMEM((ff, width), BF),
            pltpu.VMEM((2, 2 * cap, width), BF),
            pltpu.VMEM((2, 2 * cap, width), BF),
            pltpu.VMEM((2, 2 * cap, ff), BF),
            pltpu.VMEM((2, 2 * cap, ff), BF),
            pltpu.VMEM((2, 2 * cap, ff), BF),
            *ring_sems(chips),
            DMA((3,)),
            DMA((2,)),
            DMA,
            DMA((2, 5)),
        ],
        compiler_params=pltpu.CompilerParams(
            collective_id=collective_id, has_side_effects=True, vmem_limit_bytes=VMEM_LIMIT
        ),
        cost_estimate=pl.CostEstimate(
            flops=2 * chips * cap * width * ff * 6, transcendentals=0, bytes_accessed=200 << 20
        ),
        name="experts",
    )(h2, dy_all, slot, weight, wg, wu, wd)


def rows_back_kernel(
    chips, cap,
    dg_ref, du_ref, slot_ref, wg_hbm, wu_hbm, total_ref,
    wg, wu, dg, du, drow, mine, out, came, far, up_in, down_in,
    up, down, side, w_sem, in_sem,
):
    hops = Hops(chips)
    half = chips // 2
    tok, width = total_ref.shape
    order = [half]
    for s in range(half - 1, 0, -1):
        order += [s, -s] if s == half - 1 else [-s, s]
    order += [0]
    number = {d: i for i, d in enumerate(order)}
    loads = [
        pltpu.make_async_copy(a, b, w_sem.at[i])
        for i, (a, b) in enumerate(((wg_hbm, wg), (wu_hbm, wu)))
    ]

    def in_copies(i):
        chip = hops.chip(order[i])
        return [
            pltpu.make_async_copy(r.at[chip], b.at[i % 2], in_sem.at[i % 2, j])
            for j, (r, b) in enumerate(((dg_ref, dg), (du_ref, du)))
        ]

    for c in loads + in_copies(0):
        c.start()
    hops.meet()
    for c in loads:
        c.wait()

    def produce(d, same_ref, other_ref):
        i = number[d]
        p = i % 2
        for c in in_copies(i):
            c.wait()
        if i + 1 < chips:
            for c in in_copies(i + 1):
                c.start()

        def back(at):
            drow[:, at] = (dot_nt(dg[p], wg[at, :]) + dot_nt(du[p], wu[at, :])).astype(BF)

        tiles(width // 512, 512, back)
        chip = hops.chip(d)
        lanes = lax.broadcasted_iota(jnp.int32, (tok, cap), 1)

        def pick(k):
            return (slot_ref[2 * chip + k] == lanes).astype(F32).astype(BF)

        same, other = hops.core, 1 - hops.core
        same_pick, other_pick = pick(same), pick(other)
        same_rows = pl.ds(pl.multiple_of(same * cap, 16), cap)
        other_rows = pl.ds(pl.multiple_of(other * cap, 16), cap)

        def spread(at):
            same_ref[:, at] = dot32(same_pick, drow[same_rows, at])
            other_ref[:, at] = dot32(other_pick, drow[other_rows, at]).astype(BF)

        tiles(width // 1024, 1024, spread)

    def finish(value, at):
        total_ref[at, :] = value

    hops.turn(
        hops.scatter(tok, produce, mine, out, came, far, up_in, down_in, up, down, side, finish)
    )


def rows_back(chips, cap, dg, du, slot, wg, wu, collective_id):
    tok = slot.shape[1]
    width, ff = wg.shape
    anywhere = pl.BlockSpec(memory_space=pl.ANY)
    vmem = pl.BlockSpec(memory_space=pltpu.VMEM)
    return pl.pallas_call(
        functools.partial(rows_back_kernel, chips, cap),
        out_shape=jax.ShapeDtypeStruct((tok, width), F32),
        in_specs=[anywhere, anywhere, vmem, anywhere, anywhere],
        out_specs=vmem,
        scratch_shapes=[
            pltpu.VMEM((width, ff), BF),
            pltpu.VMEM((width, ff), BF),
            pltpu.VMEM((2, 2 * cap, ff), BF),
            pltpu.VMEM((2, 2 * cap, ff), BF),
            pltpu.VMEM((2 * cap, width), BF),
            *scatter_scratch(chips, tok, width),
            *ring_sems(chips),
            DMA((2,)),
            DMA((2, 2)),
        ],
        compiler_params=pltpu.CompilerParams(
            collective_id=collective_id, has_side_effects=True, vmem_limit_bytes=VMEM_LIMIT
        ),
        cost_estimate=pl.CostEstimate(
            flops=2 * chips * cap * width * ff * 6, transcendentals=0, bytes_accessed=200 << 20
        ),
        name="rows_back",
    )(dg, du, slot, wg, wu)


def turned(v, cosine, sine):
    return v * cosine + pltpu.roll(v, HD // 2, 1) * sine


def head_of(proj, at, gain, cosine, sine):
    value = proj[:, at]
    inverse = lax.rsqrt(jnp.mean(value * value, axis=-1, keepdims=True) + epsilon)
    hat = value * inverse
    return hat, inverse, turned(hat * gain, cosine, sine).astype(BF)


def softmax_rows(queries, keys, docs_q, docs_k):
    raw = dot_nt(queries, keys) * HD ** (-0.5)
    raw = jnp.where(docs_q == docs_k, raw, -1e30)
    grown = jnp.exp(raw - jnp.max(raw, axis=-1, keepdims=True))
    return grown * (1.0 / jnp.sum(grown, axis=-1, keepdims=True))


def columns_of(block, head, heads):
    return pl.ds(pl.multiple_of((block * heads + head) * HD, HD), HD)


def attention_kernel(
    chips, reps, heads,
    cot_ref, seq_ref, ga_ref, gf_ref, gq_ref, gk_ref, cos_ref, sin_ref, dc_ref, dr_ref, wq_hbm, wo_hbm,
    dy_ref, h1_ref, proj_ref, ob_ref, mid_ref, h2_ref,
    wq, wo, give, came, up, down, side, rep_sem, own_sem,
):
    hops = Hops(chips)
    rep = lax.axis_index("rep")
    seq_len, width = seq_ref.shape
    tok = mid_ref.shape[0]
    block = min(256, seq_len)
    loads = [
        pltpu.make_async_copy(a, b, own_sem.at[i])
        for i, (a, b) in enumerate(((wq_hbm, wq), (wo_hbm, wo), (cot_ref, dy_ref.at[hops.me])))
    ]
    hops.meet(reps)
    ring = hops.gather([(cot_ref, lambda dev: dy_ref.at[dev], up, down, side)], lambda d: None)
    next(ring)
    for c in loads:
        c.start()

    def normed(i, carry):
        rows = pl.ds(pl.multiple_of(i * 64, 64), 64)
        v = seq_ref[rows, :].astype(F32)
        v = v * lax.rsqrt(jnp.mean(v * v, axis=-1, keepdims=True) + epsilon)
        h1_ref[rows, :] = (v * ga_ref[...]).astype(BF)
        return carry

    lax.fori_loop(0, seq_len // 64, normed, 0)
    loads[0].wait()
    total = 3 * heads * HD
    step = 512 if total % 512 == 0 else HD
    for i in range(total // step):
        at = pl.ds(i * step, step)
        proj_ref[:, at] = dot32(h1_ref[...], wq[:, at])

    def one(head, carry):
        _, _, q_b = head_of(
            proj_ref, columns_of(0, head, heads), gq_ref[...], cos_ref[...], sin_ref[...]
        )
        _, _, k_b = head_of(
            proj_ref, columns_of(1, head, heads), gk_ref[...], cos_ref[...], sin_ref[...]
        )
        v_b = proj_ref[:, columns_of(2, head, heads)].astype(BF)
        for i in range(seq_len // block):
            rows = slice(i * block, (i + 1) * block)
            probs = softmax_rows(q_b[rows], k_b, dc_ref[rows, :], dr_ref[...])
            ob_ref[rows, columns_of(0, head, heads)] = dot32(probs.astype(BF), v_b).astype(BF)
        return carry

    lax.fori_loop(0, heads // 2, one, 0)
    next(ring)
    lax.fori_loop(heads // 2, heads, one, 0)
    loads[1].wait()
    swaps = []
    for k in range(1, reps):
        for i in range(width // 512):
            at = pl.ds(i * 512, 512)
            give[k - 1, :, at] = dot32(ob_ref[pl.ds(k * tok, tok), :], wo[:, at]).astype(BF)
        c = pltpu.make_async_remote_copy(
            src_ref=give.at[k - 1],
            dst_ref=came.at[k - 1],
            send_sem=rep_sem.at[0, k - 1],
            recv_sem=rep_sem.at[1, k - 1],
            device_id={"rep": (rep + k) % reps},
            device_id_type=MESH,
        )
        c.start()
        swaps.append(c)
    for i in range(width // 512):
        at = pl.ds(i * 512, 512)
        mid_ref[:, at] = dot32(ob_ref[pl.ds(0, tok), :], wo[:, at])
    next(ring)
    for c in swaps:
        c.wait()

    def second(i, carry):
        rows = pl.ds(pl.multiple_of(i * 64, 64), 64)
        v = seq_ref[rows, :].astype(F32) + mid_ref[rows, :]
        for k in range(1, reps):
            v = v + came[k - 1, rows, :].astype(F32)
        mid_ref[rows, :] = v
        v = v * lax.rsqrt(jnp.mean(v * v, axis=-1, keepdims=True) + epsilon)
        h2_ref[rows, :] = (v * gf_ref[...]).astype(BF)
        return carry

    lax.fori_loop(0, tok // 64, second, 0)
    loads[2].wait()
    hops.turn(ring)


def attention(chips, reps, cot, seq, ga, gf, gq, gk, cosine, sine, docs, w_qkv, w_out, collective_id):
    seq_len, width = seq.shape
    tok = cot.shape[0]
    heads = w_out.shape[0] // HD
    anywhere = pl.BlockSpec(memory_space=pl.ANY)
    vmem = pl.BlockSpec(memory_space=pltpu.VMEM)
    return pl.pallas_call(
        functools.partial(attention_kernel, chips, reps, heads),
        out_shape=(
            jax.ShapeDtypeStruct((2 * chips, tok, width), BF),
            jax.ShapeDtypeStruct((seq_len, width), BF),
            jax.ShapeDtypeStruct((seq_len, 3 * heads * HD), F32),
            jax.ShapeDtypeStruct((seq_len, heads * HD), BF),
            jax.ShapeDtypeStruct((tok, width), F32),
            jax.ShapeDtypeStruct((tok, width), BF),
        ),
        in_specs=[anywhere] + [vmem] * 9 + [anywhere] * 2,
        out_specs=(anywhere,) + (vmem,) * 5,
        scratch_shapes=[
            pltpu.VMEM(w_qkv.shape, BF),
            pltpu.VMEM(w_out.shape, BF),
            pltpu.VMEM((reps - 1, tok, width), BF),
            pltpu.VMEM((reps - 1, tok, width), BF),
            *ring_sems(chips),
            DMA((2, reps - 1)),
            DMA((3,)),
        ],
        compiler_params=pltpu.CompilerParams(
            collective_id=collective_id, has_side_effects=True, vmem_limit_bytes=VMEM_LIMIT
        ),
        cost_estimate=pl.CostEstimate(
            flops=2 * seq_len * w_qkv.size, transcendentals=0, bytes_accessed=100 << 20
        ),
        name="attention",
    )(cot, seq, ga, gf, gq, gk, cosine, sine, docs[:, None], docs[None, :], w_qkv, w_out)


def attention_back_kernel(
    heads,
    proj_ref, mid_ref, wo_ref, gq_ref, gk_ref, cos_ref, sin_ref, dc_ref, dr_ref,
    grad_ref, qt_ref, kt_ref,
    dob, dk, dv,
):
    seq_len = proj_ref.shape[0]
    block = min(256, seq_len)
    scale = HD ** (-0.5)
    for i in range(heads * HD // 512):
        at = pl.ds(i * 512, 512)
        dob[:, at] = dot_nt(mid_ref[...], wo_ref[at, :]).astype(BF)
    qt_ref[...] = jnp.zeros_like(qt_ref)
    kt_ref[...] = jnp.zeros_like(kt_ref)

    def unturned(grad, hat, inverse, gain, rows):
        grad = turned(grad, cos_ref[rows, :], -sin_ref[rows, :])
        scaled = grad * gain
        pre = inverse * (scaled - hat * jnp.mean(scaled * hat, axis=-1, keepdims=True))
        return pre.astype(BF), jnp.sum(grad * hat, axis=0, keepdims=True)

    def one(head, carry):
        q_at, k_at, v_at = (columns_of(b, head, heads) for b in range(3))
        q_hat, q_inv, q_b = head_of(proj_ref, q_at, gq_ref[...], cos_ref[...], sin_ref[...])
        k_hat, k_inv, k_b = head_of(proj_ref, k_at, gk_ref[...], cos_ref[...], sin_ref[...])
        v_b = proj_ref[:, v_at].astype(BF)
        for i in range(seq_len // block):
            rows = slice(i * block, (i + 1) * block)
            probs = softmax_rows(q_b[rows], k_b, dc_ref[rows, :], dr_ref[...])
            grad_o = dob[rows, columns_of(0, head, heads)]
            grad_p = dot_nt(grad_o, v_b)
            grad_s = (
                probs * (grad_p - jnp.sum(probs * grad_p, axis=-1, keepdims=True))
            ).astype(BF)
            dv_part = dot_tn(probs.astype(BF), grad_o)
            dk_part = dot_tn(grad_s, q_b[rows])
            if i == 0:
                dv[...] = dv_part
                dk[...] = dk_part
            else:
                dv[...] += dv_part
                dk[...] += dk_part
            pre, terms = unturned(
                dot32(grad_s, k_b) * scale, q_hat[rows], q_inv[rows], gq_ref[...], rows
            )
            grad_ref[rows, q_at] = pre
            qt_ref[...] += terms
        pre, terms = unturned(dk[...] * scale, k_hat, k_inv, gk_ref[...], slice(0, seq_len))
        grad_ref[:, k_at] = pre
        kt_ref[...] += terms
        grad_ref[:, v_at] = dv[...].astype(BF)
        return carry

    lax.fori_loop(0, heads, one, 0)


def attention_back(proj, mid, w_out, gq, gk, cosine, sine, docs):
    seq_len = proj.shape[0]
    heads = w_out.shape[0] // HD
    vmem = pl.BlockSpec(memory_space=pltpu.VMEM)
    return pl.pallas_call(
        functools.partial(attention_back_kernel, heads),
        out_shape=(
            jax.ShapeDtypeStruct(proj.shape, BF),
            jax.ShapeDtypeStruct((1, HD), F32),
            jax.ShapeDtypeStruct((1, HD), F32),
        ),
        in_specs=[vmem] * 9,
        out_specs=(vmem,) * 3,
        scratch_shapes=[
            pltpu.VMEM((seq_len, heads * HD), BF),
            pltpu.VMEM((seq_len, HD), F32),
            pltpu.VMEM((seq_len, HD), F32),
        ],
        compiler_params=pltpu.CompilerParams(vmem_limit_bytes=VMEM_LIMIT),
        cost_estimate=pl.CostEstimate(
            flops=20 * heads * seq_len * seq_len * HD, transcendentals=0, bytes_accessed=20 << 20
        ),
        name="attention_back",
    )(proj, mid, w_out, gq, gk, cosine, sine, docs[:, None], docs[None, :])


def ring_sems(chips):
    return [DMA((2, chips // 2)), DMA((2, chips // 2)), DMA((2, chips))]


def dense_gradients_kernel(
    chips, split_out, h1_ref, grad_ref, ob_ref, mid_ref, gains_ref, qkv_ref, out_ref, gain_ref, *scratch
):
    hops = Hops(chips)
    scratches = [scratch[9 * i : 9 * i + 9] for i in range(3)]
    hops.meet()

    first = hops.core == 0

    def product(left_ref, right_ref, rows, width):
        def produce(d, same_ref, other_ref):
            columns = pl.ds(pl.multiple_of(2 * rows * hops.chip(d), 2 * rows), 2 * rows)
            left = left_ref[:, columns]

            def block(at):
                value = dot_tn(left, right_ref[:, at])
                low, high = value[:rows], value[rows:]
                same_ref[:, at] = jnp.where(first, low, high)
                other_ref[:, at] = jnp.where(first, high, low).astype(BF)

            tiles(width // 512, 512, block)

        return produce

    def small(d, same_ref, other_ref):
        dev = hops.device(d)
        same_ref[...] = gains_ref[dev]
        other_ref[...] = gains_ref[dev + 1 - 2 * hops.core].astype(BF)

    def into(ref):
        def finish(value, at):
            ref[at, :] = value.astype(ref.dtype)

        return finish

    def ring(produce, ref, bufs):
        return hops.scatter(ref.shape[0], produce, *bufs, into(ref))

    rings = [ring(product(h1_ref, grad_ref, *qkv_ref.shape), qkv_ref, scratches[0])]
    if split_out:
        rings.append(ring(product(ob_ref, mid_ref, *out_ref.shape), out_ref, scratches[1]))
    rings.append(ring(small, gain_ref, scratches[2]))
    hops.turn(*rings)


def dense_gradients(chips, split_out, h1, grad, ob, mid, gain_blocks, collective_id):
    shard = h1.shape[1] // (2 * chips)
    width = grad.shape[1]
    half = ob.shape[1] // (2 * chips) if split_out else 32
    vmem = pl.BlockSpec(memory_space=pltpu.VMEM)
    shapes = ((shard, width), (half, D), gain_blocks.shape[1:])
    scratch = []
    for rows, columns in shapes:
        scratch += [*scatter_scratch(chips, rows, columns), *ring_sems(chips)]
    return pl.pallas_call(
        functools.partial(dense_gradients_kernel, chips, split_out),
        out_shape=tuple(
            jax.ShapeDtypeStruct(shape, kind)
            for shape, kind in zip(shapes, (BF, BF, F32), strict=True)
        ),
        in_specs=[vmem] * 5,
        out_specs=(vmem,) * 3,
        scratch_shapes=scratch,
        compiler_params=pltpu.CompilerParams(
            collective_id=collective_id, has_side_effects=True, vmem_limit_bytes=VMEM_LIMIT
        ),
        cost_estimate=pl.CostEstimate(
            flops=2 * h1.size * width, transcendentals=0, bytes_accessed=200 << 20
        ),
        name="dense_gradients",
    )(h1, grad, ob, mid, gain_blocks)


def start_kernel(
    chips, reps, heads, split_out,
    tok_ref, small_ref, wq_ref, wo_ref,
    seq_ref, smalls_ref, full_ref, out_ref,
    own_q, own_o, *sems,
):
    hops = Hops(chips)
    rep = lax.axis_index("rep")
    up, down, side, up_s, down_s, side_s, up_o, down_o, side_o, rep_sem, col_sem, own_sem, half_sem = sems
    pieces = []
    for i in range(3 * heads):
        q, j = i // heads, i % heads
        at = pl.multiple_of(((q * heads + j) * reps + rep) * HD, HD)
        pieces.append(
            pltpu.make_async_copy(
                wq_ref.at[:, pl.ds(at, HD)], own_q.at[:, pl.ds(i * HD, HD)], col_sem.at[i]
            )
        )
        pieces[-1].start()
    hops.meet(reps)
    swaps = []
    for k in range(1, reps):
        c = pltpu.make_async_remote_copy(
            src_ref=tok_ref,
            dst_ref=seq_ref.at[reps - k],
            send_sem=rep_sem.at[0, reps - k],
            recv_sem=rep_sem.at[1, reps - k],
            device_id={"rep": (rep + k) % reps},
            device_id_type=MESH,
        )
        c.start()
        swaps.append(c)
    locals_ = [
        pltpu.make_async_copy(tok_ref, seq_ref.at[0], own_sem.at[0]),
        pltpu.make_async_copy(small_ref, smalls_ref.at[hops.me], own_sem.at[1]),
    ]
    for c in locals_:
        c.start()
    for c in pieces:
        c.wait()
    mine = pltpu.make_async_copy(own_q, full_ref.at[hops.me], own_sem.at[2])
    mine.start()
    items = [
        (own_q, lambda dev: full_ref.at[dev], up, down, side),
        (small_ref, lambda dev: smalls_ref.at[dev], up_s, down_s, side_s),
    ]
    if split_out:
        rows = own_o.shape[0]
        kept = wo_ref.at[pl.ds(pl.multiple_of(hops.core * rows, rows), rows)]
        given = wo_ref.at[pl.ds(pl.multiple_of((1 - hops.core) * rows, rows), rows)]
        give = hops.copy(given, own_o, half_sem.at[0], half_sem.at[1], hops.flip)

        @pl.when(hops.core == rep)
        def _():
            give.start()
            keep = pltpu.make_async_copy(kept, own_o, half_sem.at[2])
            keep.start()
            keep.wait()
            give.wait_send()

        @pl.when(hops.core != rep)
        def _():
            give.wait_recv()

        def slot(dev):
            return out_ref.at[dev // 2, pl.ds(pl.multiple_of(dev % 2 * rows, rows), rows)]

        mine_o = pltpu.make_async_copy(own_o, slot(hops.me), half_sem.at[3])
        mine_o.start()
        items.append((own_o, slot, up_o, down_o, side_o))
    hops.turn(hops.gather(items, lambda d: None))
    for c in locals_:
        c.wait()
    mine.wait()
    if split_out:
        mine_o.wait()
    for c in swaps:
        c.wait()


def start(chips, reps, heads, split_out, tok, small, w_qkv, w_out, collective_id):
    anywhere = pl.BlockSpec(memory_space=pl.ANY)
    vmem = pl.BlockSpec(memory_space=pltpu.VMEM)
    shard, wide = w_qkv.shape[0], 3 * heads * HD
    half = w_out.shape[0] // 2
    return pl.pallas_call(
        functools.partial(start_kernel, chips, reps, heads, split_out),
        out_shape=(
            jax.ShapeDtypeStruct((reps, *tok.shape), BF),
            jax.ShapeDtypeStruct((2 * chips, *small.shape), F32),
            jax.ShapeDtypeStruct((2 * chips, shard, wide), BF),
            jax.ShapeDtypeStruct((chips, 2 * half, D), BF),
        ),
        in_specs=[vmem, vmem, anywhere, anywhere],
        out_specs=(anywhere,) * 4,
        scratch_shapes=[
            pltpu.VMEM((shard, wide), BF),
            pltpu.VMEM((half, D), BF),
            *ring_sems(chips),
            *ring_sems(chips),
            *ring_sems(chips),
            DMA((2, max(reps, 2))),
            DMA((3 * heads,)),
            DMA((3,)),
            DMA((4,)),
        ],
        compiler_params=pltpu.CompilerParams(collective_id=collective_id, has_side_effects=True),
        cost_estimate=pl.CostEstimate(
            flops=0, transcendentals=0, bytes_accessed=200 << 20
        ),
        name="start",
    )(tok, small, w_qkv, w_out)


def out_rows(ring, half, rep, grp):
    n = ring.devices

    def send(pairs):
        pairs = [(a * n + b, c * n + d) for (a, b), (c, d) in pairs]
        return lax.ppermute(half, ("rep", "grp"), pairs)

    chips = range(ring.chips)
    mate = send([((r, 2 * j + 1 - r), (r, 2 * j + r)) for r in range(2) for j in chips])
    across = [
        send([((r, 2 * j + c), (1 - r, 2 * j + r)) for r in range(2) for j in chips])
        for c in range(2)
    ]
    core = grp % 2
    first = jnp.where(core == rep, jnp.where(core == 0, half, mate), across[0])
    second = jnp.where(core == rep, jnp.where(core == 0, mate, half), across[1])
    return jnp.concatenate([first, second], axis=0).astype(F32)


def per_device(
    tokens, w_qkv, w_out, gains, w_gate, w_up, w_down, segment_ids, routes, gate_weights, cotangent
):
    groups = lax.axis_size("grp")
    reps = lax.axis_size("rep")
    ring = Ring(groups)
    rep, grp = lax.axis_index("rep"), lax.axis_index("grp")
    rel = jnp.asarray(ring.table())[grp]
    tok_rows = tokens.shape[1]
    seq_len = segment_ids.shape[1]
    heads = HEADS // reps
    wide = heads * HD

    def from_rep(v, k):
        return lax.ppermute(v, "rep", [((s + k) % reps, s) for s in range(reps)])

    def to_rep(v, k):
        return lax.ppermute(v, "rep", [(s, (s + k) % reps) for s in range(reps)])

    def rep_gather(v):
        return jnp.concatenate([v] + [from_rep(v, k) for k in range(1, reps)], axis=0)

    def rep_scatter(v):
        parts = v.reshape(reps, tok_rows, v.shape[-1])
        out = parts[0].astype(F32)
        for k in range(1, reps):
            out = out + to_rep(parts[k].astype(BF), k).astype(F32)
        return out

    own_b = tokens[0]
    gates_f = gate_weights[0]
    experts = jnp.arange(groups, dtype=jnp.int32)
    weight_of = jnp.sum(
        jnp.where(routes[0][None] == experts[:, None, None], gates_f[None], 0.0), axis=-1
    )
    gain_rows = -(-gains.shape[0] // tok_rows)
    small_rows = -(-(groups + gain_rows) // 16) * 16
    small = jnp.concatenate(
        [
            weight_of,
            jnp.pad(gains.astype(F32), (0, gain_rows * tok_rows - gains.shape[0])).reshape(
                gain_rows, tok_rows
            ),
            jnp.zeros((small_rows - groups - gain_rows, tok_rows), F32),
        ],
        axis=0,
    )
    split_out = reps == 2 and heads == ring.chips
    seq_b, smalls, full_qkv, my_out = start(
        ring.chips, reps, heads, split_out, own_b, small, w_qkv, w_out, 1
    )
    seq_b = seq_b.reshape(seq_len, D)
    shard = full_qkv.shape[1]
    full_qkv = full_qkv.reshape(D, 3 * wide)
    if not split_out:
        my_out = lax.all_gather(w_out, "grp", axis=0, tiled=True)
        my_out = lax.dynamic_index_in_dim(
            my_out.reshape(heads, reps, HD, D), rep, axis=1, keepdims=False
        )
    my_out = my_out.reshape(wide, D)
    gains_f = smalls[:, groups : groups + gain_rows].reshape(groups, -1)
    gains_f = gains_f[:, : gains.shape[0]].reshape(-1)
    weight_in = lax.dynamic_index_in_dim(smalls, grp, 1, False)
    g_attn = gains_f[:D]
    g_ffn = gains_f[D : 2 * D]
    g_query = gains_f[2 * D : 2 * D + HD]
    g_key = gains_f[2 * D + HD :]

    order = jnp.concatenate(
        [((rep + k) % reps) * tok_rows + jnp.arange(tok_rows, dtype=jnp.int32) for k in range(reps)]
    )
    frequency = rope_base ** (-2.0 * jnp.arange(HD // 2, dtype=F32) / HD)
    angles = order.astype(F32)[:, None] * frequency[None, :]
    cosine = jnp.concatenate([jnp.cos(angles)] * 2, axis=1)
    sine = jnp.concatenate([-jnp.sin(angles), jnp.sin(angles)], axis=1)
    docs = segment_ids[0][order]
    g_query, g_key = g_query[None], g_key[None]
    dy_all, h1_b, projected, attended_b, mid_rows, h2_b = attention(
        ring.chips,
        reps,
        cotangent[0],
        seq_b,
        g_attn[None],
        g_ffn[None],
        g_query,
        g_key,
        cosine,
        sine,
        docs,
        full_qkv,
        my_out,
        5,
    )

    chips = ring.chips
    entries = tok_rows * TOP
    capacity = min(tok_rows, (9 * entries + 8 * groups - 1) // (8 * groups))
    capacity = -(-capacity // 16) * 16
    named = weight_in > 0
    before = dot32(
        named.astype(BF), jnp.tri(tok_rows, dtype=BF).T
    )
    slot = jnp.where(named, before - 1.0, -1.0).astype(jnp.int32)
    rows_in, grads_in, acts, grad_gates, grad_ups = expert_rows(
        chips, capacity, h2_b, dy_all, slot, weight_in, w_gate[0], w_up[0], w_down[0], 2
    )
    all_rows = rows_in.reshape(-1, D)
    all_grads = grads_in.reshape(-1, D)
    all_acts = acts.reshape(groups * capacity, -1)
    all_gates = grad_gates.reshape(groups * capacity, -1)
    all_ups = grad_ups.reshape(groups * capacity, -1)

    def rep_send(v):
        v = v.astype(BF)
        came = [[] for _ in range(1, reps)]
        for part in jnp.split(v, 2):
            for k in range(1, reps):
                came[k - 1].append(from_rep(part, k))
        return v, came

    def rep_sum(sent, after):
        (v, came), _ = lax.optimization_barrier((sent, after))
        return v.astype(F32) + sum(jnp.concatenate(c, axis=0).astype(F32) for c in came)

    grad_wdown = rep_send(jnp.einsum("rf,rd->fd", all_acts, all_grads, preferred_element_type=F32))
    grad_wgate = rep_send(jnp.einsum("rd,rf->df", all_rows, all_gates, preferred_element_type=F32))
    grad_wup = rep_send(jnp.einsum("rd,rf->df", all_rows, all_ups, preferred_element_type=F32))

    cuts = 1 if chips <= 8 else chips // 8
    (grad_gates, grad_ups), _ = lax.optimization_barrier(
        ((grad_gates, grad_ups), (grad_wdown[0], grad_wgate[0], grad_wup[0]))
    )
    grad_h2 = jnp.concatenate(
        [
            rows_back(chips, capacity, grad_gates, grad_ups, slot[:, :, None], wg, wu, 8 + i)
            for i, (wg, wu) in enumerate(
                zip(jnp.split(w_gate[0], cuts), jnp.split(w_up[0], cuts), strict=True)
            )
        ],
        axis=1,
    )


    grad_out = cotangent[0].astype(F32)
    _, hat_two, inv_two = rms_forward(mid_rows, g_ffn)
    grad_mid_norm, ffn_terms = rms_backward(grad_h2, hat_two, inv_two, g_ffn)
    grad_mid = grad_out + grad_mid_norm
    grad_mid_b = grad_mid.astype(BF)
    pick = (slot[:, None, :] == jnp.arange(capacity, dtype=jnp.int32)[None, :, None]).astype(BF)
    row_weight = jnp.sum(pick.astype(F32) * weight_in[:, None, :], axis=-1)
    acts_late, _ = lax.optimization_barrier((all_acts, grad_mid_b))
    eout = dot32(acts_late, w_down[0]).astype(BF).astype(F32)
    eout = (row_weight.reshape(-1, 1) * eout).astype(BF).reshape(groups, capacity, D)
    out_all = jnp.einsum("gct,gcd->gtd", pick, eout, preferred_element_type=F32).astype(BF)
    out_sum = lax.psum_scatter(
        out_all.reshape(groups * tok_rows, D), "grp", scatter_dimension=0, tiled=True
    )

    grad_branch_b = rep_gather(grad_mid_b)
    grad_proj, query_terms, key_terms = attention_back(
        projected, grad_branch_b, my_out, g_query, g_key, cosine, sine, docs
    )
    _, hat_one, inv_one = rms_forward(seq_b.astype(F32), g_attn)
    grad_h1_part = jnp.einsum("te,de->td", grad_proj, full_qkv, preferred_element_type=F32)
    attn_terms = grad_h1_part * hat_one
    grad_h1 = rep_scatter(grad_h1_part)
    grad_rows_one, _ = rms_backward(grad_h1, hat_one[:tok_rows], inv_one[:tok_rows], g_attn)
    grad_tokens = grad_mid + grad_rows_one
    grad_gains = jnp.concatenate(
        [
            jnp.sum(attn_terms, axis=0),
            jnp.sum(ffn_terms, axis=0),
            query_terms[0],
            key_terms[0],
        ]
    )

    grad_wdown = rep_sum(grad_wdown, grad_h2)
    (grad_proj, grad_wdown), _ = lax.optimization_barrier(
        ((grad_proj, grad_wdown), grad_h1_part)
    )
    gain_size = gains.shape[0]
    gain_blocks = jnp.pad(
        grad_gains.reshape(groups, gain_size), ((0, 0), (0, 4096 - gain_size))
    ).reshape(groups, 32, 128)
    shard_qkv, half_out, total = dense_gradients(
        chips,
        split_out,
        h1_b,
        grad_proj,
        attended_b,
        grad_branch_b,
        gain_blocks,
        4,
    )
    total = total.reshape(-1)[:gain_size]
    qkv_all = [shard_qkv] + [from_rep(shard_qkv, k) for k in range(1, reps)]
    columns = jnp.stack(qkv_all, axis=0).reshape(reps, shard, 3, heads, HD)
    columns = columns[(jnp.arange(reps) - rep) % reps]
    shard_qkv = columns.transpose(1, 2, 3, 0, 4).reshape(shard, 3 * D).astype(F32)

    grad_wgate = rep_sum(grad_wgate, shard_qkv)
    grad_wup = rep_sum(grad_wup, shard_qkv)
    result = mid_rows + lax.optimization_barrier((out_sum, shard_qkv))[0].astype(F32)

    if split_out:
        shard_out = out_rows(ring, half_out, rep, grp)
    else:
        grad_wout = dot_tn(attended_b, grad_branch_b)
        whole = lax.dynamic_update_slice(
            jnp.zeros((heads, reps, HD, D), BF),
            grad_wout.astype(BF).reshape(heads, 1, HD, D),
            (0, rep, 0, 0),
        ).reshape(D, D)
        shard_out = lax.psum(
            lax.psum_scatter(whole, "grp", scatter_dimension=0, tiled=True), "rep"
        ).astype(F32)
    own_gains = total
    for k in range(1, reps):
        total = total + from_rep(own_gains, k)
    return (
        result[None],
        grad_tokens[None],
        shard_qkv,
        shard_out,
        total,
        grad_wgate[None],
        grad_wup[None],
        grad_wdown[None],
    )


def solution(mesh):
    in_specs = (
        P("grp", "rep", None),
        P("grp", None),
        P("grp", None),
        P("grp"),
        P("grp", None, None),
        P("grp", None, None),
        P("grp", None, None),
        P("grp", None),
        P("grp", "rep", None),
        P("grp", "rep", None),
        P("grp", "rep", None),
    )
    out_specs = (
        P("grp", "rep", None),
        P("grp", "rep", None),
        P("grp", None),
        P("grp", None),
        P("grp"),
        P("grp", None, None),
        P("grp", None, None),
        P("grp", None, None),
    )
    return jax.shard_map(
        per_device, mesh=mesh, in_specs=in_specs, out_specs=out_specs, check_vma=False
    )
```

```python
import functools

import jax
import jax.numpy as jnp
import numpy as np
from jax import lax
from jax.experimental import pallas as pl
from jax.experimental.pallas import tpu as pltpu
from jax.sharding import PartitionSpec as P

D = 2048
HEADS = 16
HD = 128
TOP = 8
BF = jnp.bfloat16
F32 = jnp.float32

epsilon = 1e-06
rope_base = 10000.0


def rms_forward(values, gain_vec):
    inverse = lax.rsqrt(jnp.mean(values * values, axis=-1, keepdims=True) + epsilon)
    normed = values * inverse
    return (normed * gain_vec, normed, inverse)


def rms_backward(grad_out, normed, inverse, gain_vec):
    scaled = grad_out * gain_vec
    grad_in = inverse * (scaled - normed * jnp.mean(scaled * normed, axis=-1, keepdims=True))
    return (grad_in, grad_out * normed)


def dot32(a, b):
    return jnp.dot(a, b, preferred_element_type=F32)


class Ring:
    def __init__(self, devices):
        self.devices = devices
        self.chips = devices // 2
        outer = 4 if self.chips % 4 == 0 else 2
        inner = self.chips // outer
        cycle = [(a, 0) for a in range(outer)]
        for step, a in enumerate(reversed(range(outer))):
            columns = range(1, inner)
            cycle += [(a, b) for b in (columns if step % 2 == 0 else reversed(columns))]
        self.cycle = [a * inner + b for a, b in cycle]
        self.place = {chip: i for i, chip in enumerate(self.cycle)}
        self.half = self.chips // 2

    def perm(self, shift):
        pairs = []
        for chip in range(self.chips):
            other = self.cycle[(self.place[chip] + shift) % self.chips]
            pairs += [(2 * chip + core, 2 * other + core) for core in range(2)]
        return pairs

    def table(self):
        out = np.zeros((self.devices, self.chips, 2), np.int32)
        for dev in range(self.devices):
            chip, core = dev // 2, dev % 2
            for d in range(self.chips):
                other = self.cycle[(self.place[chip] + d) % self.chips]
                out[dev, d, 0] = 2 * other + core
                out[dev, d, 1] = 2 * other + (1 - core)
        return out

    def ahead(self, v):
        return lax.ppermute(v, "grp", self.perm(1))

    def back(self, v):
        return lax.ppermute(v, "grp", self.perm(-1))

    def flip(self, v):
        return lax.ppermute(v, "grp", [(i, i ^ 1) for i in range(self.devices)])

    def gather(self, own):
        rows = own.shape[0] // 2
        blocks = {0: (own, self.flip(own))}
        up = down = own
        for step in range(1, self.half):
            up, down = self.ahead(up), self.back(down)
            blocks[-step % self.chips] = (up, self.flip(up))
            blocks[step] = (down, self.flip(down))
        first, last = self.ahead(up[:rows]), self.back(down[rows:])
        far = jnp.concatenate([first, last], axis=0)
        blocks[self.half] = (far, self.flip(far))
        return blocks

    def scatter_sum(self, blocks):
        def joined(d):
            same, other = blocks[d]
            return same.astype(F32) + self.flip(other.astype(BF)).astype(F32)

        far = joined(self.half).astype(BF)
        rows = far.shape[0] // 2
        up, down = self.ahead(far[:rows]), self.back(far[rows:])
        zero = jnp.zeros_like(up)
        up = jnp.concatenate([up, zero], axis=0)
        down = jnp.concatenate([zero, down], axis=0)
        for step in range(self.half - 1, 0, -1):
            up = self.ahead((joined(step) + up.astype(F32)).astype(BF))
            down = self.back((joined(-step % self.chips) + down.astype(F32)).astype(BF))
        return joined(0) + up.astype(F32) + down.astype(F32)


MESH = pl.DeviceIdType.MESH
DMA = pltpu.SemaphoreType.DMA
VMEM_LIMIT = 60 << 20


class Hops:
    def __init__(self, chips):
        self.chips, self.half = chips, chips // 2
        self.outer = 4 if chips % 4 == 0 else 2
        self.inner = chips // self.outer
        self.me = lax.axis_index("grp")
        chip, self.core = self.me // 2, self.me % 2
        a, b = chip // self.inner, chip % self.inner
        row = self.outer - 1 - a
        along = jnp.where(row % 2 == 0, b - 1, self.inner - 1 - b)
        self.place = jnp.where(b == 0, a, self.outer + row * (self.inner - 1) + along)
        self.ahead, self.back = self.device(1), self.device(-1)
        self.flip = self.me + 1 - 2 * self.core
        self.started = []

    def chip(self, d):
        p = (self.place + (d % self.chips)) % self.chips
        q = jnp.maximum(p - self.outer, 0)
        k, m = q // (self.inner - 1), q % (self.inner - 1)
        b = jnp.where(k % 2 == 0, m + 1, self.inner - 1 - m)
        return jnp.where(
            p < self.outer, p * self.inner, (self.outer - 1 - k) * self.inner + b
        )

    def device(self, d):
        return 2 * self.chip(d) + self.core

    def meet(self, reps=1):
        barrier = pltpu.get_barrier_semaphore()
        for dev in (self.ahead, self.back, self.flip):
            pl.semaphore_signal(barrier, inc=1, device_id={"grp": dev}, device_id_type=MESH)
        rep = lax.axis_index("rep")
        for k in range(1, reps):
            pl.semaphore_signal(
                barrier, inc=1, device_id={"rep": (rep + k) % reps}, device_id_type=MESH
            )
        pl.semaphore_wait(barrier, 2 + reps)

    def copy(self, src, dst, send_sem, recv_sem, dev):
        return pltpu.make_async_remote_copy(
            src_ref=src,
            dst_ref=dst,
            send_sem=send_sem,
            recv_sem=recv_sem,
            device_id={"grp": dev},
            device_id_type=MESH,
        )

    def send(self, src, dst, sems, at, dev):
        c = self.copy(src, dst, sems.at[0, at], sems.at[1, at], dev)
        c.start()
        self.started.append(c)

    def wait(self, dst, sems, at):
        self.copy(dst, dst, sems.at[0, at], sems.at[1, at], self.flip).wait_recv()

    def drain(self):
        for c in self.started:
            c.wait_send()

    def gather(self, items, use):
        half = self.half

        def parts(ref):
            cut = ref.shape[0] // 2
            return ref.at[pl.ds(0, cut)], ref.at[pl.ds(cut, ref.shape[0] - cut)]

        for own, slot, up, down, side in items:
            self.send(own, slot(self.me), up, 0, self.ahead)
            self.send(own, slot(self.me), down, 0, self.back)
            self.send(own, slot(self.me), side, 0, self.flip)
        yield

        def ready(d):
            dev = self.device(d)
            for _, slot, _, _, side in items:
                self.wait(slot(dev + 1 - 2 * self.core), side, d % self.chips)
            use(d)

        ready(0)
        for s in range(1, half):
            last = s == half - 1
            for _, slot, up, down, side in items:
                a, b = slot(self.device(-s)), slot(self.device(s))
                self.wait(a, up, s - 1)
                part = parts(a)[0] if last else a
                self.send(part, part, up, s, self.ahead)
                self.send(a, a, side, -s % self.chips, self.flip)
                self.wait(b, down, s - 1)
                part = parts(b)[1] if last else b
                self.send(part, part, down, s, self.back)
                self.send(b, b, side, s, self.flip)
            for d in (-s, s):
                ready(d)
            yield
        for _, slot, up, down, side in items:
            far = slot(self.device(half))
            low, high = parts(far)
            self.wait(low, up, half - 1)
            self.wait(high, down, half - 1)
            self.send(far, far, side, half, self.flip)
        ready(half)

    def scatter(self, rows, produce, mine, out, came, far, up_in, down_in, up, down, side, finish):
        half, chips = self.half, self.chips
        cut = rows // 2
        strip = 16
        made = {}

        def make(d):
            made[d] = len(made) % mine.shape[0]
            produce(d, mine.at[made[d]], out.at[d % chips])
            self.send(out.at[d % chips], came.at[d % chips], side, d % chips, self.flip)

        def joined(d, at):
            return mine[made[d], at, :] + came[d % chips, at, :].astype(F32)

        def strips(first, last, body):
            def step(i, carry):
                body(pl.ds(pl.multiple_of(first + i * strip, strip), strip))
                return carry

            lax.fori_loop(0, (last - first) // strip, step, 0)

        for d in (half, half - 1):
            make(d)
        self.wait(came.at[half], side, half)

        def far_sum(at):
            far[at, :] = joined(half, at).astype(BF)

        strips(0, rows, far_sum)
        low, high = pl.ds(0, cut), pl.ds(cut, rows - cut)
        self.send(far.at[low], up_in.at[0, low], up, 0, self.ahead)
        self.send(far.at[high], down_in.at[0, high], down, 0, self.back)
        make(1 - half)
        yield
        for s in range(half - 1, 0, -1):
            i = half - s
            for d in sorted({s - 1, 1 - s}):
                make(d)
            for d, buf, sems, target in (
                (s, up_in, up, self.ahead),
                (-s, down_in, down, self.back),
            ):
                self.wait(came.at[d % chips], side, d % chips)

                def fresh(at, d=d, buf=buf, i=i):
                    buf[i - 1, at, :] = joined(d, at).astype(BF)

                def onto(at, d=d, buf=buf, i=i):
                    buf[i - 1, at, :] = (joined(d, at) + buf[i - 1, at, :].astype(F32)).astype(BF)

                if i > 1:
                    self.wait(buf.at[i - 1], sems, i - 1)
                    strips(0, rows, onto)
                elif d > 0:
                    self.wait(buf.at[0, low], sems, 0)
                    strips(0, cut, onto)
                    strips(cut, rows, fresh)
                else:
                    self.wait(buf.at[0, high], sems, 0)
                    strips(0, cut, fresh)
                    strips(cut, rows, onto)
                self.send(buf.at[i - 1], buf.at[i], sems, i, target)
            yield
        self.wait(came.at[0], side, 0)
        self.wait(up_in.at[half - 1], up, half - 1)
        self.wait(down_in.at[half - 1], down, half - 1)

        def total(at):
            finish(
                joined(0, at)
                + up_in[half - 1, at, :].astype(F32)
                + down_in[half - 1, at, :].astype(F32),
                at,
            )

        strips(0, rows, total)

    def turn(self, *rings):
        rings = list(rings)
        while rings:
            rings = [r for r in rings if next(r, self) is not self]
        self.drain()


def scatter_scratch(chips, rows, width):
    half = chips // 2
    return [
        pltpu.VMEM((4, rows, width), F32),
        pltpu.VMEM((chips, rows, width), BF),
        pltpu.VMEM((chips, rows, width), BF),
        pltpu.VMEM((rows, width), BF),
        pltpu.VMEM((half, rows, width), BF),
        pltpu.VMEM((half, rows, width), BF),
    ]


def dot_nt(a, b):
    return lax.dot_general(a, b, (((1,), (1,)), ((), ())), preferred_element_type=F32)


def dot_tn(a, b):
    return lax.dot_general(a, b, (((0,), (0,)), ((), ())), preferred_element_type=F32)


def tiles(count, width, body):
    for i in range(count):
        body(pl.ds(i * width, width))


def experts_kernel(
    chips, cap,
    h2_ref, dy_ref, slot_ref, weight_ref, wg_hbm, wu_hbm, wd_hbm,
    xs_ref, de_ref, act_ref, dg_ref, du_ref,
    held, dy, wg, wu, wd, xs_b, de_b, act_b, dg_b, du_b,
    up, down, side, w_sem, dy_sem, own_sem, out_sem,
):
    hops = Hops(chips)
    half = chips // 2
    tok, width = h2_ref.shape
    ff = wg.shape[1]
    order = [0]
    for s in range(1, half):
        order += [-s, s]
    order += [half]
    number = {d: i for i, d in enumerate(order)}

    loads = [
        pltpu.make_async_copy(a, b, w_sem.at[i])
        for i, (a, b) in enumerate(((wg_hbm, wg), (wu_hbm, wu), (wd_hbm, wd)))
    ]

    def dy_copy(i):
        chip = hops.chip(order[i])
        return pltpu.make_async_copy(dy_ref.at[pl.ds(2 * chip, 2)], dy.at[i % 2], dy_sem.at[i % 2])

    def out_copies(i):
        chip = hops.chip(order[i])
        pairs = ((xs_b, xs_ref), (de_b, de_ref), (act_b, act_ref), (dg_b, dg_ref), (du_b, du_ref))
        return [
            pltpu.make_async_copy(b.at[i % 2], r.at[chip], out_sem.at[i % 2, j])
            for j, (b, r) in enumerate(pairs)
        ]

    hops.meet()
    own = pltpu.make_async_copy(h2_ref, held.at[hops.me], own_sem)
    own.start()

    def use(d):
        i = number[d]
        p = i % 2
        if i == 0:
            own.wait()
            for c in loads:
                c.start()
            dy_copy(0).start()
            for c in loads:
                c.wait()
        dy_copy(i).wait()
        if i + 1 < chips:
            dy_copy(i + 1).start()
        if i >= 2:
            for c in out_copies(i - 2):
                c.wait()
        chip = hops.chip(d)
        for k in range(2):
            dev = 2 * chip + k
            hit = slot_ref[pl.ds(dev, 1), :] == lax.broadcasted_iota(jnp.int32, (cap, tok), 0)
            pick = hit.astype(F32).astype(BF)
            scale = jnp.sum(
                jnp.where(hit, weight_ref[pl.ds(dev, 1), :], 0.0), axis=1, keepdims=True
            )
            rows = pl.ds(k * cap, cap)

            def choose(at, k=k, dev=dev, pick=pick, scale=scale, rows=rows):
                xs_b[p, rows, at] = dot32(pick, held[dev, :, at]).astype(BF)
                de_b[p, rows, at] = (scale * dot32(pick, dy[p, k, :, at])).astype(BF)

            tiles(width // 1024, 1024, choose)

        def hidden(at):
            gpre = dot32(xs_b[p], wg[:, at])
            upre = dot32(xs_b[p], wu[:, at])
            dact = dot_nt(de_b[p], wd[at, :])
            sig = 1.0 / (1.0 + jnp.exp(-gpre))
            act_b[p, :, at] = (gpre * sig * upre).astype(BF)
            dg_b[p, :, at] = (dact * upre * sig * (1.0 + gpre * (1.0 - sig))).astype(BF)
            du_b[p, :, at] = (dact * gpre * sig).astype(BF)

        tiles(ff // 512, 512, hidden)
        for c in out_copies(i):
            c.start()

    hops.turn(hops.gather([(h2_ref, lambda dev: held.at[dev], up, down, side)], use))
    for i in (chips - 2, chips - 1):
        for c in out_copies(i):
            c.wait()


def expert_rows(chips, cap, h2, dy_all, slot, weight, wg, wu, wd, collective_id):
    tok, width = h2.shape
    ff = wg.shape[1]
    anywhere = pl.BlockSpec(memory_space=pl.ANY)
    vmem = pl.BlockSpec(memory_space=pltpu.VMEM)
    wide = jax.ShapeDtypeStruct((chips, 2 * cap, width), BF)
    thin = jax.ShapeDtypeStruct((chips, 2 * cap, ff), BF)
    return pl.pallas_call(
        functools.partial(experts_kernel, chips, cap),
        out_shape=(wide, wide, thin, thin, thin),
        in_specs=[anywhere, anywhere, vmem, vmem, anywhere, anywhere, anywhere],
        out_specs=(anywhere,) * 5,
        scratch_shapes=[
            pltpu.VMEM((2 * chips, tok, width), BF),
            pltpu.VMEM((2, 2, tok, width), BF),
            pltpu.VMEM((width, ff), BF),
            pltpu.VMEM((width, ff), BF),
            pltpu.VMEM((ff, width), BF),
            pltpu.VMEM((2, 2 * cap, width), BF),
            pltpu.VMEM((2, 2 * cap, width), BF),
            pltpu.VMEM((2, 2 * cap, ff), BF),
            pltpu.VMEM((2, 2 * cap, ff), BF),
            pltpu.VMEM((2, 2 * cap, ff), BF),
            *ring_sems(chips),
            DMA((3,)),
            DMA((2,)),
            DMA,
            DMA((2, 5)),
        ],
        compiler_params=pltpu.CompilerParams(
            collective_id=collective_id, has_side_effects=True, vmem_limit_bytes=VMEM_LIMIT
        ),
        cost_estimate=pl.CostEstimate(
            flops=2 * chips * cap * width * ff * 6, transcendentals=0, bytes_accessed=200 << 20
        ),
        name="experts",
    )(h2, dy_all, slot, weight, wg, wu, wd)


def column_of(table, dev):
    lanes = lax.broadcasted_iota(jnp.int32, table.shape, 1)
    return jnp.sum(jnp.where(lanes == dev, table[...], 0.0), axis=1, keepdims=True)


def returned(hops, d, cap, tok, slot_ref, rows_ref, same_ref, other_ref, weight_ref=None):
    chip = hops.chip(d)
    lanes = lax.broadcasted_iota(jnp.int32, (tok, cap), 1).astype(F32)
    for k, ref in ((hops.core, same_ref), (1 - hops.core, other_ref)):
        pick = (column_of(slot_ref, 2 * chip + k) == lanes).astype(F32).astype(BF)
        rows = pl.ds(pl.multiple_of(k * cap, 16), cap)
        weight = None if weight_ref is None else column_of(weight_ref, 2 * chip + k)

        def spread(at, pick=pick, rows=rows, ref=ref, weight=weight):
            value = dot32(pick, rows_ref[rows, at])
            if weight is not None:
                value = weight * value
            ref[:, at] = value.astype(ref.dtype)

        tiles(rows_ref.shape[1] // 1024, 1024, spread)


def scatter_order(half):
    order = [half, half - 1, 1 - half]
    for s in range(half - 2, 0, -1):
        order += [-s, s]
    return order + [0]


def outputs_kernel(
    chips, cap,
    act_ref, xs_ref, de_ref, dg_ref, du_ref, slot_ref, weight_ref, wd_hbm,
    total_ref, down_ref, came_ref, gate_ref, up_ref,
    wd, left, right, made_d, made, act, rows_b, mine, out, came, far, up_in, down_in,
    up, down, side, w_sem, act_sem, left_sem, right_sem, made_sem, down_sem, rep_sem,
):
    hops = Hops(chips)
    replica = lax.axis_index("rep")
    tok, width = total_ref.shape
    order = scatter_order(chips // 2)
    number = {d: i for i, d in enumerate(order)}
    strip = right.shape[2]
    count = width // strip

    def act_copy(i):
        rows = pl.ds(pl.multiple_of(hops.chip(order[i]) * (2 * cap), 2 * cap), 2 * cap)
        return pltpu.make_async_copy(act_ref.at[rows], act.at[i % 2], act_sem.at[i % 2])

    jobs = [
        (thin, wide, result, i)
        for thin, wide, result in (
            (act_ref, de_ref, down_ref),
            (dg_ref, xs_ref, gate_ref),
            (du_ref, xs_ref, up_ref),
        )
        for i in range(count)
    ]
    done, stored, sent = [], {}, []

    def right_copy(n):
        at = pl.ds(jobs[n][3] * strip, strip)
        return pltpu.make_async_copy(jobs[n][1].at[:, at], right.at[n % 2], right_sem.at[n % 2])

    def job():
        n = len(done)
        if n == len(jobs):
            return
        done.append(n)
        thin, _, result, i = jobs[n]
        if i == 0:
            fresh = pltpu.make_async_copy(thin, left, left_sem)
            fresh.start()
            fresh.wait()
        right_copy(n).wait()
        if n + 1 < len(jobs):
            right_copy(n + 1).start()
        at = pl.ds(i * strip, strip)
        if n < count:
            made_d[i] = dot_tn(left[...], right[n % 2]).astype(BF)
            stored[n] = pltpu.make_async_copy(made_d.at[i], result.at[:, at], down_sem.at[i])
            c = pltpu.make_async_remote_copy(
                src_ref=made_d.at[i],
                dst_ref=came_ref.at[:, at],
                send_sem=rep_sem.at[0, i],
                recv_sem=rep_sem.at[1, i],
                device_id={"rep": 1 - replica},
                device_id_type=MESH,
            )
            c.start()
            sent.append(c)
        else:
            if n - 2 >= count:
                stored.pop(n - 2).wait()
            made[n % 2] = dot_tn(right[n % 2], left[...]).astype(BF)
            stored[n] = pltpu.make_async_copy(made.at[n % 2], result.at[at, :], made_sem.at[n % 2])
        stored[n].start()

    def produce(d, same_ref, other_ref):
        i = number[d]
        act_copy(i).wait()
        if i + 1 < chips:
            act_copy(i + 1).start()

        def last(at):
            rows_b[:, at] = dot32(act[i % 2], wd[:, at]).astype(BF)

        tiles(width // 512, 512, last)
        returned(hops, d, cap, tok, slot_ref, rows_b, same_ref, other_ref, weight_ref)

    def finish(value, at):
        total_ref[at, :] = value

    load = pltpu.make_async_copy(wd_hbm, wd, w_sem)
    load.start()
    act_copy(0).start()
    right_copy(0).start()
    hops.meet(2)
    load.wait()
    ring = hops.scatter(tok, produce, mine, out, came, far, up_in, down_in, up, down, side, finish)
    share = -(-(len(jobs) - count) // (chips // 2 - 1))
    for step in range(chips // 2):
        next(ring)
        for _ in range(share if step else count):
            job()
    hops.turn(ring)
    for c in stored.values():
        c.wait()
    for c in sent:
        c.wait()


def outputs(chips, cap, act, xs, de, dg, du, slot_t, weight_t, wd, collective_id):
    ff, width = wd.shape
    tok = slot_t.shape[0]
    strip = 512
    anywhere = pl.BlockSpec(memory_space=pl.ANY)
    vmem = pl.BlockSpec(memory_space=pltpu.VMEM)
    tall, flat = jax.ShapeDtypeStruct((width, ff), BF), jax.ShapeDtypeStruct((ff, width), BF)
    return pl.pallas_call(
        functools.partial(outputs_kernel, chips, cap),
        out_shape=(jax.ShapeDtypeStruct((tok, width), F32), flat, flat, tall, tall),
        in_specs=[anywhere] * 5 + [vmem] * 2 + [anywhere],
        out_specs=(vmem,) + (anywhere,) * 4,
        scratch_shapes=[
            pltpu.VMEM((ff, width), BF),
            pltpu.VMEM((2 * chips * cap, ff), BF),
            pltpu.VMEM((2, 2 * chips * cap, strip), BF),
            pltpu.VMEM((width // strip, ff, strip), BF),
            pltpu.VMEM((2, strip, ff), BF),
            pltpu.VMEM((2, 2 * cap, ff), BF),
            pltpu.VMEM((2 * cap, width), BF),
            *scatter_scratch(chips, tok, width),
            *ring_sems(chips),
            DMA,
            DMA((2,)),
            DMA,
            DMA((2,)),
            DMA((2,)),
            DMA((width // strip,)),
            DMA((2, width // strip)),
        ],
        compiler_params=pltpu.CompilerParams(
            collective_id=collective_id, has_side_effects=True, vmem_limit_bytes=63 << 20
        ),
        cost_estimate=pl.CostEstimate(
            flops=2 * 2 * chips * cap * width * ff * 4, transcendentals=0, bytes_accessed=200 << 20
        ),
        name="outputs",
    )(act, xs, de, dg, du, slot_t, weight_t, wd)


def rows_back_kernel(
    chips, cap,
    dg_ref, du_ref, slot_ref, wg_hbm, wu_hbm, total_ref,
    wg, wu, dg, du, drow, mine, out, came, far, up_in, down_in,
    up, down, side, w_sem, in_sem,
):
    hops = Hops(chips)
    tok, width = total_ref.shape
    order = scatter_order(chips // 2)
    number = {d: i for i, d in enumerate(order)}
    loads = [
        pltpu.make_async_copy(a, b, w_sem.at[i])
        for i, (a, b) in enumerate(((wg_hbm, wg), (wu_hbm, wu)))
    ]

    def in_copies(i):
        chip = hops.chip(order[i])
        return [
            pltpu.make_async_copy(r.at[chip], b.at[i % 2], in_sem.at[i % 2, j])
            for j, (r, b) in enumerate(((dg_ref, dg), (du_ref, du)))
        ]

    for c in loads + in_copies(0):
        c.start()
    hops.meet()
    for c in loads:
        c.wait()

    def produce(d, same_ref, other_ref):
        i = number[d]
        p = i % 2
        for c in in_copies(i):
            c.wait()
        if i + 1 < chips:
            for c in in_copies(i + 1):
                c.start()

        def back(at):
            drow[:, at] = (dot_nt(dg[p], wg[at, :]) + dot_nt(du[p], wu[at, :])).astype(BF)

        tiles(width // 512, 512, back)
        returned(hops, d, cap, tok, slot_ref, drow, same_ref, other_ref)

    def finish(value, at):
        total_ref[at, :] = value

    hops.turn(
        hops.scatter(tok, produce, mine, out, came, far, up_in, down_in, up, down, side, finish)
    )


def rows_back(chips, cap, dg, du, slot, wg, wu, collective_id):
    tok = slot.shape[0]
    width, ff = wg.shape
    anywhere = pl.BlockSpec(memory_space=pl.ANY)
    vmem = pl.BlockSpec(memory_space=pltpu.VMEM)
    return pl.pallas_call(
        functools.partial(rows_back_kernel, chips, cap),
        out_shape=jax.ShapeDtypeStruct((tok, width), F32),
        in_specs=[anywhere, anywhere, vmem, anywhere, anywhere],
        out_specs=vmem,
        scratch_shapes=[
            pltpu.VMEM((width, ff), BF),
            pltpu.VMEM((width, ff), BF),
            pltpu.VMEM((2, 2 * cap, ff), BF),
            pltpu.VMEM((2, 2 * cap, ff), BF),
            pltpu.VMEM((2 * cap, width), BF),
            *scatter_scratch(chips, tok, width),
            *ring_sems(chips),
            DMA((2,)),
            DMA((2, 2)),
        ],
        compiler_params=pltpu.CompilerParams(
            collective_id=collective_id, has_side_effects=True, vmem_limit_bytes=VMEM_LIMIT
        ),
        cost_estimate=pl.CostEstimate(
            flops=2 * chips * cap * width * ff * 6, transcendentals=0, bytes_accessed=200 << 20
        ),
        name="rows_back",
    )(dg, du, slot, wg, wu)


def turned(v, cosine, sine):
    return v * cosine + pltpu.roll(v, HD // 2, 1) * sine


def head_of(proj, at, gain, cosine, sine):
    value = proj[:, at]
    inverse = lax.rsqrt(jnp.mean(value * value, axis=-1, keepdims=True) + epsilon)
    hat = value * inverse
    return hat, inverse, turned(hat * gain, cosine, sine).astype(BF)


def softmax_rows(queries, keys, docs_q, docs_k):
    raw = dot_nt(queries, keys) * HD ** (-0.5)
    raw = jnp.where(docs_q == docs_k, raw, -1e30)
    grown = jnp.exp(raw - jnp.max(raw, axis=-1, keepdims=True))
    return grown * (1.0 / jnp.sum(grown, axis=-1, keepdims=True))


def columns_of(block, head, heads):
    return pl.ds(pl.multiple_of((block * heads + head) * HD, HD), HD)


def attention_kernel(
    chips, reps, heads,
    cot_ref, seq_ref, ga_ref, gf_ref, gq_ref, gk_ref, cos_ref, sin_ref, dc_ref, dr_ref, wq_hbm, wo_hbm,
    dy_ref, h1_ref, proj_ref, ob_ref, mid_ref, h2_ref,
    wq, wo, give, came, up, down, side, rep_sem, own_sem,
):
    hops = Hops(chips)
    rep = lax.axis_index("rep")
    seq_len, width = seq_ref.shape
    tok = mid_ref.shape[0]
    block = min(256, seq_len)
    loads = [
        pltpu.make_async_copy(a, b, own_sem.at[i])
        for i, (a, b) in enumerate(((wq_hbm, wq), (wo_hbm, wo), (cot_ref, dy_ref.at[hops.me])))
    ]
    hops.meet(reps)
    ring = hops.gather([(cot_ref, lambda dev: dy_ref.at[dev], up, down, side)], lambda d: None)
    next(ring)
    for c in loads:
        c.start()

    def normed(i, carry):
        rows = pl.ds(pl.multiple_of(i * 64, 64), 64)
        v = seq_ref[rows, :].astype(F32)
        v = v * lax.rsqrt(jnp.mean(v * v, axis=-1, keepdims=True) + epsilon)
        h1_ref[rows, :] = (v * ga_ref[...]).astype(BF)
        return carry

    lax.fori_loop(0, seq_len // 64, normed, 0)
    loads[0].wait()
    total = 3 * heads * HD
    step = 512 if total % 512 == 0 else HD
    for i in range(total // step):
        at = pl.ds(i * step, step)
        proj_ref[:, at] = dot32(h1_ref[...], wq[:, at])

    def one(head, carry):
        _, _, q_b = head_of(
            proj_ref, columns_of(0, head, heads), gq_ref[...], cos_ref[...], sin_ref[...]
        )
        _, _, k_b = head_of(
            proj_ref, columns_of(1, head, heads), gk_ref[...], cos_ref[...], sin_ref[...]
        )
        v_b = proj_ref[:, columns_of(2, head, heads)].astype(BF)
        for i in range(seq_len // block):
            rows = slice(i * block, (i + 1) * block)
            probs = softmax_rows(q_b[rows], k_b, dc_ref[rows, :], dr_ref[...])
            ob_ref[rows, columns_of(0, head, heads)] = dot32(probs.astype(BF), v_b).astype(BF)
        return carry

    lax.fori_loop(0, heads // 2, one, 0)
    next(ring)
    lax.fori_loop(heads // 2, heads, one, 0)
    loads[1].wait()
    swaps = []
    for k in range(1, reps):
        for i in range(width // 512):
            at = pl.ds(i * 512, 512)
            give[k - 1, :, at] = dot32(ob_ref[pl.ds(k * tok, tok), :], wo[:, at]).astype(BF)
        c = pltpu.make_async_remote_copy(
            src_ref=give.at[k - 1],
            dst_ref=came.at[k - 1],
            send_sem=rep_sem.at[0, k - 1],
            recv_sem=rep_sem.at[1, k - 1],
            device_id={"rep": (rep + k) % reps},
            device_id_type=MESH,
        )
        c.start()
        swaps.append(c)
    for i in range(width // 512):
        at = pl.ds(i * 512, 512)
        mid_ref[:, at] = dot32(ob_ref[pl.ds(0, tok), :], wo[:, at])
    next(ring)
    for c in swaps:
        c.wait()

    def second(i, carry):
        rows = pl.ds(pl.multiple_of(i * 64, 64), 64)
        v = seq_ref[rows, :].astype(F32) + mid_ref[rows, :]
        for k in range(1, reps):
            v = v + came[k - 1, rows, :].astype(F32)
        mid_ref[rows, :] = v
        v = v * lax.rsqrt(jnp.mean(v * v, axis=-1, keepdims=True) + epsilon)
        h2_ref[rows, :] = (v * gf_ref[...]).astype(BF)
        return carry

    lax.fori_loop(0, tok // 64, second, 0)
    loads[2].wait()
    hops.turn(ring)


def attention(chips, reps, cot, seq, ga, gf, gq, gk, cosine, sine, docs, w_qkv, w_out, collective_id):
    seq_len, width = seq.shape
    tok = cot.shape[0]
    heads = w_out.shape[0] // HD
    anywhere = pl.BlockSpec(memory_space=pl.ANY)
    vmem = pl.BlockSpec(memory_space=pltpu.VMEM)
    return pl.pallas_call(
        functools.partial(attention_kernel, chips, reps, heads),
        out_shape=(
            jax.ShapeDtypeStruct((2 * chips, tok, width), BF),
            jax.ShapeDtypeStruct((seq_len, width), BF),
            jax.ShapeDtypeStruct((seq_len, 3 * heads * HD), F32),
            jax.ShapeDtypeStruct((seq_len, heads * HD), BF),
            jax.ShapeDtypeStruct((tok, width), F32),
            jax.ShapeDtypeStruct((tok, width), BF),
        ),
        in_specs=[anywhere] + [vmem] * 9 + [anywhere] * 2,
        out_specs=(anywhere,) + (vmem,) * 5,
        scratch_shapes=[
            pltpu.VMEM(w_qkv.shape, BF),
            pltpu.VMEM(w_out.shape, BF),
            pltpu.VMEM((reps - 1, tok, width), BF),
            pltpu.VMEM((reps - 1, tok, width), BF),
            *ring_sems(chips),
            DMA((2, reps - 1)),
            DMA((3,)),
        ],
        compiler_params=pltpu.CompilerParams(
            collective_id=collective_id, has_side_effects=True, vmem_limit_bytes=VMEM_LIMIT
        ),
        cost_estimate=pl.CostEstimate(
            flops=2 * seq_len * w_qkv.size, transcendentals=0, bytes_accessed=100 << 20
        ),
        name="attention",
    )(cot, seq, ga, gf, gq, gk, cosine, sine, docs[:, None], docs[None, :], w_qkv, w_out)


def attention_back_kernel(
    heads,
    proj_ref, mid_ref, wo_ref, gq_ref, gk_ref, cos_ref, sin_ref, dc_ref, dr_ref,
    grad_ref, qt_ref, kt_ref,
    dob, dk, dv,
):
    seq_len = proj_ref.shape[0]
    block = min(256, seq_len)
    scale = HD ** (-0.5)
    for i in range(heads * HD // 512):
        at = pl.ds(i * 512, 512)
        dob[:, at] = dot_nt(mid_ref[...], wo_ref[at, :]).astype(BF)
    qt_ref[...] = jnp.zeros_like(qt_ref)
    kt_ref[...] = jnp.zeros_like(kt_ref)

    def unturned(grad, hat, inverse, gain, rows):
        grad = turned(grad, cos_ref[rows, :], -sin_ref[rows, :])
        scaled = grad * gain
        pre = inverse * (scaled - hat * jnp.mean(scaled * hat, axis=-1, keepdims=True))
        return pre.astype(BF), jnp.sum(grad * hat, axis=0, keepdims=True)

    def one(head, carry):
        q_at, k_at, v_at = (columns_of(b, head, heads) for b in range(3))
        q_hat, q_inv, q_b = head_of(proj_ref, q_at, gq_ref[...], cos_ref[...], sin_ref[...])
        k_hat, k_inv, k_b = head_of(proj_ref, k_at, gk_ref[...], cos_ref[...], sin_ref[...])
        v_b = proj_ref[:, v_at].astype(BF)
        for i in range(seq_len // block):
            rows = slice(i * block, (i + 1) * block)
            probs = softmax_rows(q_b[rows], k_b, dc_ref[rows, :], dr_ref[...])
            grad_o = dob[rows, columns_of(0, head, heads)]
            grad_p = dot_nt(grad_o, v_b)
            grad_s = (
                probs * (grad_p - jnp.sum(probs * grad_p, axis=-1, keepdims=True))
            ).astype(BF)
            dv_part = dot_tn(probs.astype(BF), grad_o)
            dk_part = dot_tn(grad_s, q_b[rows])
            if i == 0:
                dv[...] = dv_part
                dk[...] = dk_part
            else:
                dv[...] += dv_part
                dk[...] += dk_part
            pre, terms = unturned(
                dot32(grad_s, k_b) * scale, q_hat[rows], q_inv[rows], gq_ref[...], rows
            )
            grad_ref[rows, q_at] = pre
            qt_ref[...] += terms
        pre, terms = unturned(dk[...] * scale, k_hat, k_inv, gk_ref[...], slice(0, seq_len))
        grad_ref[:, k_at] = pre
        kt_ref[...] += terms
        grad_ref[:, v_at] = dv[...].astype(BF)
        return carry

    lax.fori_loop(0, heads, one, 0)


def attention_back(proj, mid, w_out, gq, gk, cosine, sine, docs):
    seq_len = proj.shape[0]
    heads = w_out.shape[0] // HD
    vmem = pl.BlockSpec(memory_space=pltpu.VMEM)
    return pl.pallas_call(
        functools.partial(attention_back_kernel, heads),
        out_shape=(
            jax.ShapeDtypeStruct(proj.shape, BF),
            jax.ShapeDtypeStruct((1, HD), F32),
            jax.ShapeDtypeStruct((1, HD), F32),
        ),
        in_specs=[vmem] * 9,
        out_specs=(vmem,) * 3,
        scratch_shapes=[
            pltpu.VMEM((seq_len, heads * HD), BF),
            pltpu.VMEM((seq_len, HD), F32),
            pltpu.VMEM((seq_len, HD), F32),
        ],
        compiler_params=pltpu.CompilerParams(vmem_limit_bytes=VMEM_LIMIT),
        cost_estimate=pl.CostEstimate(
            flops=20 * heads * seq_len * seq_len * HD, transcendentals=0, bytes_accessed=20 << 20
        ),
        name="attention_back",
    )(proj, mid, w_out, gq, gk, cosine, sine, docs[:, None], docs[None, :])


def ring_sems(chips):
    return [DMA((2, chips // 2)), DMA((2, chips // 2)), DMA((2, chips))]


def dense_gradients_kernel(
    chips, split_out, h1_ref, grad_ref, ob_ref, mid_ref, gains_ref, qkv_ref, out_ref, gain_ref, *scratch
):
    hops = Hops(chips)
    scratches = [scratch[9 * i : 9 * i + 9] for i in range(3)]
    hops.meet(2 if split_out else 1)
    first = hops.core == 0
    if split_out:
        q_sum, q_came, o_sum, o_came, o_give, o_got, g_sum, g_came, rep_sem, flip_sem = scratch[27:]
    else:
        q_sum, o_sum, g_sum = qkv_ref, out_ref, gain_ref

    def product(left_ref, right_ref, rows, width):
        def produce(d, same_ref, other_ref):
            columns = pl.ds(pl.multiple_of(2 * rows * hops.chip(d), 2 * rows), 2 * rows)
            left = left_ref[:, columns]

            def block(at):
                value = dot_tn(left, right_ref[:, at])
                low, high = value[:rows], value[rows:]
                same_ref[:, at] = jnp.where(first, low, high)
                other_ref[:, at] = jnp.where(first, high, low).astype(BF)

            tiles(width // 512, 512, block)

        return produce

    def small(d, same_ref, other_ref):
        dev = hops.device(d)
        same_ref[...] = gains_ref[dev]
        other_ref[...] = gains_ref[dev + 1 - 2 * hops.core].astype(BF)

    def into(ref):
        def finish(value, at):
            ref[at, :] = value.astype(ref.dtype)

        return finish

    def ring(produce, ref, bufs):
        return hops.scatter(ref.shape[0], produce, *bufs, into(ref))

    rings = [ring(product(h1_ref, grad_ref, *q_sum.shape), q_sum, scratches[0])]
    if split_out:
        rings.insert(0, ring(product(ob_ref, mid_ref, *o_sum.shape), o_sum, scratches[1]))
    rings.append(ring(small, g_sum, scratches[2]))
    hops.turn(*rings)
    if not split_out:
        return

    replica = lax.axis_index("rep")
    pairs = ((o_sum, o_came), (q_sum, q_came), (g_sum, g_came))
    swaps = [
        pltpu.make_async_remote_copy(
            src_ref=src,
            dst_ref=dst,
            send_sem=rep_sem.at[0, i],
            recv_sem=rep_sem.at[1, i],
            device_id={"rep": 1 - replica},
            device_id_type=MESH,
        )
        for i, (src, dst) in enumerate(pairs)
    ]
    for c in swaps:
        c.start()
    mine = hops.core == replica
    swaps[0].wait()
    o_give[...] = jnp.where(mine, o_came[...], o_sum[...])
    give = hops.copy(o_give, o_got, flip_sem.at[0], flip_sem.at[1], hops.flip)
    give.start()
    keep = jnp.where(mine, o_sum[...], o_came[...])
    swaps[2].wait()
    gain_ref[...] = g_sum[...] + g_came[...]
    swaps[1].wait()
    _, wide = q_sum.shape
    even = replica == 0
    for i in range(wide // HD):
        own, came = q_sum[:, pl.ds(i * HD, HD)], q_came[:, pl.ds(i * HD, HD)]
        qkv_ref[:, pl.ds(2 * i * HD, HD)] = jnp.where(even, own, came).astype(F32)
        qkv_ref[:, pl.ds((2 * i + 1) * HD, HD)] = jnp.where(even, came, own).astype(F32)
    give.wait()
    half = o_sum.shape[0]
    got = o_got[...]
    out_ref[pl.ds(0, half), :] = jnp.where(first, keep, got).astype(F32)
    out_ref[pl.ds(half, half), :] = jnp.where(first, got, keep).astype(F32)


def dense_gradients(chips, split_out, h1, grad, ob, mid, gain_blocks, collective_id):
    shard = h1.shape[1] // (2 * chips)
    width = grad.shape[1]
    half = ob.shape[1] // (2 * chips) if split_out else 32
    vmem = pl.BlockSpec(memory_space=pltpu.VMEM)
    shapes = ((shard, width), (half, D), gain_blocks.shape[1:])
    scratch = []
    for rows, columns in shapes:
        scratch += [*scatter_scratch(chips, rows, columns), *ring_sems(chips)]
    if split_out:
        scratch += [pltpu.VMEM(shapes[0], BF)] * 2 + [pltpu.VMEM(shapes[1], BF)] * 4
        scratch += [pltpu.VMEM(shapes[2], F32)] * 2 + [DMA((2, 3)), DMA((2,))]
        shapes = ((shard, 2 * width), (2 * half, D), shapes[2])
    kinds = (F32, F32, F32) if split_out else (BF, BF, F32)
    return pl.pallas_call(
        functools.partial(dense_gradients_kernel, chips, split_out),
        out_shape=tuple(
            jax.ShapeDtypeStruct(shape, kind) for shape, kind in zip(shapes, kinds, strict=True)
        ),
        in_specs=[vmem] * 5,
        out_specs=(vmem,) * 3,
        scratch_shapes=scratch,
        compiler_params=pltpu.CompilerParams(
            collective_id=collective_id, has_side_effects=True, vmem_limit_bytes=VMEM_LIMIT
        ),
        cost_estimate=pl.CostEstimate(
            flops=2 * h1.size * width, transcendentals=0, bytes_accessed=200 << 20
        ),
        name="dense_gradients",
    )(h1, grad, ob, mid, gain_blocks)


def start_kernel(
    chips, reps, heads, split_out,
    tok_ref, small_ref, wq_ref, wo_ref,
    seq_ref, smalls_ref, full_ref, out_ref,
    own_q, own_o, *sems,
):
    hops = Hops(chips)
    rep = lax.axis_index("rep")
    up, down, side, up_s, down_s, side_s, up_o, down_o, side_o, rep_sem, col_sem, own_sem, half_sem = sems
    pieces = []
    for i in range(3 * heads):
        q, j = i // heads, i % heads
        at = pl.multiple_of(((q * heads + j) * reps + rep) * HD, HD)
        pieces.append(
            pltpu.make_async_copy(
                wq_ref.at[:, pl.ds(at, HD)], own_q.at[:, pl.ds(i * HD, HD)], col_sem.at[i]
            )
        )
        pieces[-1].start()
    hops.meet(reps)
    swaps = []
    for k in range(1, reps):
        c = pltpu.make_async_remote_copy(
            src_ref=tok_ref,
            dst_ref=seq_ref.at[reps - k],
            send_sem=rep_sem.at[0, reps - k],
            recv_sem=rep_sem.at[1, reps - k],
            device_id={"rep": (rep + k) % reps},
            device_id_type=MESH,
        )
        c.start()
        swaps.append(c)
    locals_ = [
        pltpu.make_async_copy(tok_ref, seq_ref.at[0], own_sem.at[0]),
        pltpu.make_async_copy(small_ref, smalls_ref.at[hops.me], own_sem.at[1]),
    ]
    for c in locals_:
        c.start()
    for c in pieces:
        c.wait()
    mine = pltpu.make_async_copy(own_q, full_ref.at[hops.me], own_sem.at[2])
    mine.start()
    items = [
        (own_q, lambda dev: full_ref.at[dev], up, down, side),
        (small_ref, lambda dev: smalls_ref.at[dev], up_s, down_s, side_s),
    ]
    if split_out:
        rows = own_o.shape[0]
        kept = wo_ref.at[pl.ds(pl.multiple_of(hops.core * rows, rows), rows)]
        given = wo_ref.at[pl.ds(pl.multiple_of((1 - hops.core) * rows, rows), rows)]
        give = hops.copy(given, own_o, half_sem.at[0], half_sem.at[1], hops.flip)

        @pl.when(hops.core == rep)
        def _():
            give.start()
            keep = pltpu.make_async_copy(kept, own_o, half_sem.at[2])
            keep.start()
            keep.wait()
            give.wait_send()

        @pl.when(hops.core != rep)
        def _():
            give.wait_recv()

        def slot(dev):
            return out_ref.at[dev // 2, pl.ds(pl.multiple_of(dev % 2 * rows, rows), rows)]

        mine_o = pltpu.make_async_copy(own_o, slot(hops.me), half_sem.at[3])
        mine_o.start()
        items.append((own_o, slot, up_o, down_o, side_o))
    hops.turn(hops.gather(items, lambda d: None))
    for c in locals_:
        c.wait()
    mine.wait()
    if split_out:
        mine_o.wait()
    for c in swaps:
        c.wait()


def start(chips, reps, heads, split_out, tok, small, w_qkv, w_out, collective_id):
    anywhere = pl.BlockSpec(memory_space=pl.ANY)
    vmem = pl.BlockSpec(memory_space=pltpu.VMEM)
    shard, wide = w_qkv.shape[0], 3 * heads * HD
    half = w_out.shape[0] // 2
    return pl.pallas_call(
        functools.partial(start_kernel, chips, reps, heads, split_out),
        out_shape=(
            jax.ShapeDtypeStruct((reps, *tok.shape), BF),
            jax.ShapeDtypeStruct((2 * chips, *small.shape), F32),
            jax.ShapeDtypeStruct((2 * chips, shard, wide), BF),
            jax.ShapeDtypeStruct((chips, 2 * half, D), BF),
        ),
        in_specs=[vmem, vmem, anywhere, anywhere],
        out_specs=(anywhere,) * 4,
        scratch_shapes=[
            pltpu.VMEM((shard, wide), BF),
            pltpu.VMEM((half, D), BF),
            *ring_sems(chips),
            *ring_sems(chips),
            *ring_sems(chips),
            DMA((2, max(reps, 2))),
            DMA((3 * heads,)),
            DMA((3,)),
            DMA((4,)),
        ],
        compiler_params=pltpu.CompilerParams(collective_id=collective_id, has_side_effects=True),
        cost_estimate=pl.CostEstimate(
            flops=0, transcendentals=0, bytes_accessed=200 << 20
        ),
        name="start",
    )(tok, small, w_qkv, w_out)


def per_device(
    tokens, w_qkv, w_out, gains, w_gate, w_up, w_down, segment_ids, routes, gate_weights, cotangent
):
    groups = lax.axis_size("grp")
    reps = lax.axis_size("rep")
    ring = Ring(groups)
    rep, grp = lax.axis_index("rep"), lax.axis_index("grp")
    rel = jnp.asarray(ring.table())[grp]
    tok_rows = tokens.shape[1]
    seq_len = segment_ids.shape[1]
    heads = HEADS // reps
    wide = heads * HD

    def from_rep(v, k):
        return lax.ppermute(v, "rep", [((s + k) % reps, s) for s in range(reps)])

    def to_rep(v, k):
        return lax.ppermute(v, "rep", [(s, (s + k) % reps) for s in range(reps)])

    def rep_gather(v):
        return jnp.concatenate([v] + [from_rep(v, k) for k in range(1, reps)], axis=0)

    def rep_scatter(v):
        parts = v.reshape(reps, tok_rows, v.shape[-1])
        out = parts[0].astype(F32)
        for k in range(1, reps):
            out = out + to_rep(parts[k].astype(BF), k).astype(F32)
        return out

    own_b = tokens[0]
    gates_f = gate_weights[0]
    experts = jnp.arange(groups, dtype=jnp.int32)
    weight_of = jnp.sum(
        jnp.where(routes[0][None] == experts[:, None, None], gates_f[None], 0.0), axis=-1
    )
    gain_rows = -(-gains.shape[0] // tok_rows)
    small_rows = -(-(groups + gain_rows) // 16) * 16
    small = jnp.concatenate(
        [
            weight_of,
            jnp.pad(gains.astype(F32), (0, gain_rows * tok_rows - gains.shape[0])).reshape(
                gain_rows, tok_rows
            ),
            jnp.zeros((small_rows - groups - gain_rows, tok_rows), F32),
        ],
        axis=0,
    )
    split_out = reps == 2 and heads == ring.chips
    seq_b, smalls, full_qkv, my_out = start(
        ring.chips, reps, heads, split_out, own_b, small, w_qkv, w_out, 1
    )
    seq_b = seq_b.reshape(seq_len, D)
    shard = full_qkv.shape[1]
    full_qkv = full_qkv.reshape(D, 3 * wide)
    if not split_out:
        my_out = lax.all_gather(w_out, "grp", axis=0, tiled=True)
        my_out = lax.dynamic_index_in_dim(
            my_out.reshape(heads, reps, HD, D), rep, axis=1, keepdims=False
        )
    my_out = my_out.reshape(wide, D)
    gains_f = smalls[:, groups : groups + gain_rows].reshape(groups, -1)
    gains_f = gains_f[:, : gains.shape[0]].reshape(-1)
    weight_in = lax.dynamic_index_in_dim(smalls, grp, 1, False)
    g_attn = gains_f[:D]
    g_ffn = gains_f[D : 2 * D]
    g_query = gains_f[2 * D : 2 * D + HD]
    g_key = gains_f[2 * D + HD :]

    def this_first(table):
        return lax.dynamic_slice_in_dim(
            jnp.concatenate([table, table], axis=0), rep * tok_rows, seq_len, axis=0
        )

    frequency = np.float32(rope_base) ** (-2.0 * np.arange(HD // 2, dtype=np.float32) / HD)
    angles = np.arange(seq_len, dtype=np.float32)[:, None] * frequency.astype(np.float32)[None, :]
    cosine = this_first(jnp.asarray(np.concatenate([np.cos(angles)] * 2, axis=1)))
    sine = this_first(jnp.asarray(np.concatenate([-np.sin(angles), np.sin(angles)], axis=1)))
    docs = this_first(segment_ids[0])
    g_query, g_key = g_query[None], g_key[None]
    dy_all, h1_b, projected, attended_b, mid_rows, h2_b = attention(
        ring.chips,
        reps,
        cotangent[0],
        seq_b,
        g_attn[None],
        g_ffn[None],
        g_query,
        g_key,
        cosine,
        sine,
        docs,
        full_qkv,
        my_out,
        5,
    )

    chips = ring.chips
    entries = tok_rows * TOP
    capacity = min(tok_rows, (9 * entries + 8 * groups - 1) // (8 * groups))
    capacity = -(-capacity // 16) * 16
    named = weight_in > 0
    before = dot32(
        named.astype(BF), jnp.tri(tok_rows, dtype=BF).T
    )
    slot = jnp.where(named, before - 1.0, -1.0).astype(jnp.int32)
    rows_in, grads_in, acts, grad_gates, grad_ups = expert_rows(
        chips, capacity, h2_b, dy_all, slot, weight_in, w_gate[0], w_up[0], w_down[0], 2
    )
    all_rows = rows_in.reshape(-1, D)
    all_grads = grads_in.reshape(-1, D)
    all_acts = acts.reshape(groups * capacity, -1)
    all_gates = grad_gates.reshape(groups * capacity, -1)
    all_ups = grad_ups.reshape(groups * capacity, -1)

    def rep_send(v):
        return v, [from_rep(v, k) for k in range(1, reps)]

    def rep_sum(sent, after):
        (v, came), _ = lax.optimization_barrier((sent, after))
        return v.astype(F32) + sum(c.astype(F32) for c in came)

    slot_t, weight_t = slot.astype(F32).T, weight_in.T
    together = split_out and chips <= 8
    if together:
        out_sum, own_down, came_down, grad_wgate, grad_wup = outputs(
            chips, capacity, all_acts, all_rows, all_grads, all_gates, all_ups,
            slot_t, weight_t, w_down[0], 6,
        )
        grad_wdown = (own_down, [came_down])
    else:
        grad_wdown = rep_send(
            jnp.einsum("rf,rd->fd", all_acts, all_grads, preferred_element_type=F32).astype(BF)
        )
        grad_wgate = jnp.einsum("rd,rf->df", all_rows, all_gates, preferred_element_type=F32).astype(BF)
        grad_wup = jnp.einsum("rd,rf->df", all_rows, all_ups, preferred_element_type=F32).astype(BF)
    grad_wgate = rep_send(grad_wgate)
    grad_wup = rep_send(grad_wup)

    cuts = 1 if chips <= 8 else chips // 8
    (grad_gates, grad_ups), _ = lax.optimization_barrier(
        ((grad_gates, grad_ups), (grad_wdown[0], grad_wgate[0], grad_wup[0]))
    )
    grad_h2 = jnp.concatenate(
        [
            rows_back(chips, capacity, grad_gates, grad_ups, slot_t, wg, wu, 8 + i)
            for i, (wg, wu) in enumerate(
                zip(jnp.split(w_gate[0], cuts), jnp.split(w_up[0], cuts), strict=True)
            )
        ],
        axis=1,
    )


    grad_out = cotangent[0].astype(F32)
    _, hat_two, inv_two = rms_forward(mid_rows, g_ffn)
    grad_mid_norm, ffn_terms = rms_backward(grad_h2, hat_two, inv_two, g_ffn)
    grad_mid = grad_out + grad_mid_norm
    grad_mid_b = grad_mid.astype(BF)
    if not together:
        pick = (slot[:, None, :] == jnp.arange(capacity, dtype=jnp.int32)[None, :, None]).astype(BF)
        row_weight = jnp.sum(pick.astype(F32) * weight_in[:, None, :], axis=-1)
        acts_late, _ = lax.optimization_barrier((all_acts, grad_mid_b))
        eout = dot32(acts_late, w_down[0]).astype(BF).astype(F32)
        eout = (row_weight.reshape(-1, 1) * eout).astype(BF).reshape(groups, capacity, D)
        out_all = jnp.einsum("gct,gcd->gtd", pick, eout, preferred_element_type=F32).astype(BF)
        out_sum = lax.psum_scatter(
            out_all.reshape(groups * tok_rows, D), "grp", scatter_dimension=0, tiled=True
        )
    result = mid_rows + lax.optimization_barrier((out_sum, grad_mid_b))[0].astype(F32)
    grad_wdown = rep_sum(grad_wdown, grad_mid_b)
    grad_wgate = rep_sum(grad_wgate, grad_mid_b)
    grad_branch_b = rep_gather(grad_mid_b)
    (grad_branch_b, result, grad_wdown, grad_wgate), _ = lax.optimization_barrier(
        ((grad_branch_b, result, grad_wdown, grad_wgate), grad_mid_b)
    )
    grad_proj, query_terms, key_terms = attention_back(
        projected, grad_branch_b, my_out, g_query, g_key, cosine, sine, docs
    )
    _, hat_one, inv_one = rms_forward(seq_b.astype(F32), g_attn)
    grad_h1_part = jnp.einsum("te,de->td", grad_proj, full_qkv, preferred_element_type=F32)
    attn_terms = grad_h1_part * hat_one
    grad_h1 = rep_scatter(grad_h1_part)
    grad_rows_one, _ = rms_backward(grad_h1, hat_one[:tok_rows], inv_one[:tok_rows], g_attn)
    grad_tokens = grad_mid + grad_rows_one
    grad_gains = jnp.concatenate(
        [
            jnp.sum(attn_terms, axis=0),
            jnp.sum(ffn_terms, axis=0),
            query_terms[0],
            key_terms[0],
        ]
    )

    gain_size = gains.shape[0]
    gain_blocks = jnp.pad(
        grad_gains.reshape(groups, gain_size), ((0, 0), (0, 4096 - gain_size))
    ).reshape(groups, 32, 128)
    shard_qkv, half_out, total = dense_gradients(
        chips,
        split_out,
        h1_b,
        grad_proj,
        attended_b,
        grad_branch_b,
        gain_blocks,
        4,
    )
    total = total.reshape(-1)[:gain_size]
    grad_wup = rep_sum(grad_wup, shard_qkv)

    if split_out:
        shard_out = half_out
    else:
        qkv_all = [shard_qkv] + [from_rep(shard_qkv, k) for k in range(1, reps)]
        columns = jnp.stack(qkv_all, axis=0).reshape(reps, shard, 3, heads, HD)
        columns = columns[(jnp.arange(reps) - rep) % reps]
        shard_qkv = columns.transpose(1, 2, 3, 0, 4).reshape(shard, 3 * D).astype(F32)
        grad_wout = dot_tn(attended_b, grad_branch_b)
        whole = lax.dynamic_update_slice(
            jnp.zeros((heads, reps, HD, D), BF),
            grad_wout.astype(BF).reshape(heads, 1, HD, D),
            (0, rep, 0, 0),
        ).reshape(D, D)
        shard_out = lax.psum(
            lax.psum_scatter(whole, "grp", scatter_dimension=0, tiled=True), "rep"
        ).astype(F32)
        own_gains = total
        for k in range(1, reps):
            total = total + from_rep(own_gains, k)
    return (
        result[None],
        grad_tokens[None],
        shard_qkv,
        shard_out,
        total,
        grad_wgate[None],
        grad_wup[None],
        grad_wdown[None],
    )


def solution(mesh):
    in_specs = (
        P("grp", "rep", None),
        P("grp", None),
        P("grp", None),
        P("grp"),
        P("grp", None, None),
        P("grp", None, None),
        P("grp", None, None),
        P("grp", None),
        P("grp", "rep", None),
        P("grp", "rep", None),
        P("grp", "rep", None),
    )
    out_specs = (
        P("grp", "rep", None),
        P("grp", "rep", None),
        P("grp", None),
        P("grp", None),
        P("grp"),
        P("grp", None, None),
        P("grp", None, None),
        P("grp", None, None),
    )
    return jax.shard_map(
        per_device, mesh=mesh, in_specs=in_specs, out_specs=out_specs, check_vma=False
    )
```

```python
import functools

import jax
import jax.numpy as jnp
import numpy as np
from jax import lax
from jax.experimental import pallas as pl
from jax.experimental.pallas import tpu as pltpu
from jax.sharding import PartitionSpec as P

D = 2048
HEADS = 16
HD = 128
TOP = 8
BF = jnp.bfloat16
F32 = jnp.float32

epsilon = 1e-06
rope_base = 10000.0


def rms_forward(values, gain_vec):
    inverse = lax.rsqrt(jnp.mean(values * values, axis=-1, keepdims=True) + epsilon)
    normed = values * inverse
    return (normed * gain_vec, normed, inverse)


def rms_backward(grad_out, normed, inverse, gain_vec):
    scaled = grad_out * gain_vec
    grad_in = inverse * (scaled - normed * jnp.mean(scaled * normed, axis=-1, keepdims=True))
    return (grad_in, grad_out * normed)


def dot32(a, b):
    return jnp.dot(a, b, preferred_element_type=F32)


class Ring:
    def __init__(self, devices):
        self.devices = devices
        self.chips = devices // 2
        outer = 4 if self.chips % 4 == 0 else 2
        inner = self.chips // outer
        cycle = [(a, 0) for a in range(outer)]
        for step, a in enumerate(reversed(range(outer))):
            columns = range(1, inner)
            cycle += [(a, b) for b in (columns if step % 2 == 0 else reversed(columns))]
        self.cycle = [a * inner + b for a, b in cycle]
        self.place = {chip: i for i, chip in enumerate(self.cycle)}
        self.half = self.chips // 2

    def perm(self, shift):
        pairs = []
        for chip in range(self.chips):
            other = self.cycle[(self.place[chip] + shift) % self.chips]
            pairs += [(2 * chip + core, 2 * other + core) for core in range(2)]
        return pairs

    def table(self):
        out = np.zeros((self.devices, self.chips, 2), np.int32)
        for dev in range(self.devices):
            chip, core = dev // 2, dev % 2
            for d in range(self.chips):
                other = self.cycle[(self.place[chip] + d) % self.chips]
                out[dev, d, 0] = 2 * other + core
                out[dev, d, 1] = 2 * other + (1 - core)
        return out

    def ahead(self, v):
        return lax.ppermute(v, "grp", self.perm(1))

    def back(self, v):
        return lax.ppermute(v, "grp", self.perm(-1))

    def flip(self, v):
        return lax.ppermute(v, "grp", [(i, i ^ 1) for i in range(self.devices)])

    def gather(self, own):
        rows = own.shape[0] // 2
        blocks = {0: (own, self.flip(own))}
        up = down = own
        for step in range(1, self.half):
            up, down = self.ahead(up), self.back(down)
            blocks[-step % self.chips] = (up, self.flip(up))
            blocks[step] = (down, self.flip(down))
        first, last = self.ahead(up[:rows]), self.back(down[rows:])
        far = jnp.concatenate([first, last], axis=0)
        blocks[self.half] = (far, self.flip(far))
        return blocks

    def scatter_sum(self, blocks):
        def joined(d):
            same, other = blocks[d]
            return same.astype(F32) + self.flip(other.astype(BF)).astype(F32)

        far = joined(self.half).astype(BF)
        rows = far.shape[0] // 2
        up, down = self.ahead(far[:rows]), self.back(far[rows:])
        zero = jnp.zeros_like(up)
        up = jnp.concatenate([up, zero], axis=0)
        down = jnp.concatenate([zero, down], axis=0)
        for step in range(self.half - 1, 0, -1):
            up = self.ahead((joined(step) + up.astype(F32)).astype(BF))
            down = self.back((joined(-step % self.chips) + down.astype(F32)).astype(BF))
        return joined(0) + up.astype(F32) + down.astype(F32)


MESH = pl.DeviceIdType.MESH
DMA = pltpu.SemaphoreType.DMA
VMEM_LIMIT = 60 << 20


class Hops:
    def __init__(self, chips):
        self.chips, self.half = chips, chips // 2
        self.outer = 4 if chips % 4 == 0 else 2
        self.inner = chips // self.outer
        self.me = lax.axis_index("grp")
        chip, self.core = self.me // 2, self.me % 2
        a, b = chip // self.inner, chip % self.inner
        row = self.outer - 1 - a
        along = jnp.where(row % 2 == 0, b - 1, self.inner - 1 - b)
        self.place = jnp.where(b == 0, a, self.outer + row * (self.inner - 1) + along)
        self.ahead, self.back = self.device(1), self.device(-1)
        self.flip = self.me + 1 - 2 * self.core
        self.started = []

    def chip(self, d):
        p = (self.place + (d % self.chips)) % self.chips
        q = jnp.maximum(p - self.outer, 0)
        k, m = q // (self.inner - 1), q % (self.inner - 1)
        b = jnp.where(k % 2 == 0, m + 1, self.inner - 1 - m)
        return jnp.where(
            p < self.outer, p * self.inner, (self.outer - 1 - k) * self.inner + b
        )

    def device(self, d):
        return 2 * self.chip(d) + self.core

    def meet(self, reps=1):
        barrier = pltpu.get_barrier_semaphore()
        for dev in (self.ahead, self.back, self.flip):
            pl.semaphore_signal(barrier, inc=1, device_id={"grp": dev}, device_id_type=MESH)
        rep = lax.axis_index("rep")
        for k in range(1, reps):
            pl.semaphore_signal(
                barrier, inc=1, device_id={"rep": (rep + k) % reps}, device_id_type=MESH
            )
        pl.semaphore_wait(barrier, 2 + reps)

    def copy(self, src, dst, send_sem, recv_sem, dev):
        return pltpu.make_async_remote_copy(
            src_ref=src,
            dst_ref=dst,
            send_sem=send_sem,
            recv_sem=recv_sem,
            device_id={"grp": dev},
            device_id_type=MESH,
        )

    def send(self, src, dst, sems, at, dev):
        c = self.copy(src, dst, sems.at[0, at], sems.at[1, at], dev)
        c.start()
        self.started.append(c)

    def wait(self, dst, sems, at):
        self.copy(dst, dst, sems.at[0, at], sems.at[1, at], self.flip).wait_recv()

    def drain(self):
        for c in self.started:
            c.wait_send()

    def gather(self, items, use):
        half = self.half

        def parts(ref):
            cut = ref.shape[0] // 2
            return ref.at[pl.ds(0, cut)], ref.at[pl.ds(cut, ref.shape[0] - cut)]

        for own, slot, up, down, side in items:
            self.send(own, slot(self.me), up, 0, self.ahead)
            self.send(own, slot(self.me), down, 0, self.back)
            self.send(own, slot(self.me), side, 0, self.flip)
        yield

        def ready(d):
            dev = self.device(d)
            for _, slot, _, _, side in items:
                self.wait(slot(dev + 1 - 2 * self.core), side, d % self.chips)
            use(d)

        ready(0)
        for s in range(1, half):
            last = s == half - 1
            for _, slot, up, down, side in items:
                a, b = slot(self.device(-s)), slot(self.device(s))
                self.wait(a, up, s - 1)
                part = parts(a)[0] if last else a
                self.send(part, part, up, s, self.ahead)
                self.send(a, a, side, -s % self.chips, self.flip)
                self.wait(b, down, s - 1)
                part = parts(b)[1] if last else b
                self.send(part, part, down, s, self.back)
                self.send(b, b, side, s, self.flip)
            for d in (-s, s):
                ready(d)
            yield
        for _, slot, up, down, side in items:
            far = slot(self.device(half))
            low, high = parts(far)
            self.wait(low, up, half - 1)
            self.wait(high, down, half - 1)
            self.send(far, far, side, half, self.flip)
        ready(half)

    def scatter(self, rows, produce, mine, out, came, far, up_in, down_in, up, down, side, finish):
        half, chips = self.half, self.chips
        cut = rows // 2
        strip = 16
        made = {}

        def make(d):
            made[d] = len(made) % mine.shape[0]
            produce(d, mine.at[made[d]], out.at[d % chips])
            self.send(out.at[d % chips], came.at[d % chips], side, d % chips, self.flip)

        def joined(d, at):
            return mine[made[d], at, :] + came[d % chips, at, :].astype(F32)

        def strips(first, last, body):
            def step(i, carry):
                body(pl.ds(pl.multiple_of(first + i * strip, strip), strip))
                return carry

            lax.fori_loop(0, (last - first) // strip, step, 0)

        for d in (half, half - 1):
            make(d)
        self.wait(came.at[half], side, half)

        def far_sum(at):
            far[at, :] = joined(half, at).astype(BF)

        strips(0, rows, far_sum)
        low, high = pl.ds(0, cut), pl.ds(cut, rows - cut)
        self.send(far.at[low], up_in.at[0, low], up, 0, self.ahead)
        self.send(far.at[high], down_in.at[0, high], down, 0, self.back)
        make(1 - half)
        yield
        for s in range(half - 1, 0, -1):
            i = half - s
            for d in sorted({s - 1, 1 - s}):
                make(d)
            for d, buf, sems, target in (
                (s, up_in, up, self.ahead),
                (-s, down_in, down, self.back),
            ):
                self.wait(came.at[d % chips], side, d % chips)

                def fresh(at, d=d, buf=buf, i=i):
                    buf[i - 1, at, :] = joined(d, at).astype(BF)

                def onto(at, d=d, buf=buf, i=i):
                    buf[i - 1, at, :] = (joined(d, at) + buf[i - 1, at, :].astype(F32)).astype(BF)

                if i > 1:
                    self.wait(buf.at[i - 1], sems, i - 1)
                    strips(0, rows, onto)
                elif d > 0:
                    self.wait(buf.at[0, low], sems, 0)
                    strips(0, cut, onto)
                    strips(cut, rows, fresh)
                else:
                    self.wait(buf.at[0, high], sems, 0)
                    strips(0, cut, fresh)
                    strips(cut, rows, onto)
                self.send(buf.at[i - 1], buf.at[i], sems, i, target)
            yield
        self.wait(came.at[0], side, 0)
        self.wait(up_in.at[half - 1], up, half - 1)
        self.wait(down_in.at[half - 1], down, half - 1)

        def total(at):
            finish(
                joined(0, at)
                + up_in[half - 1, at, :].astype(F32)
                + down_in[half - 1, at, :].astype(F32),
                at,
            )

        strips(0, rows, total)

    def turn(self, *rings):
        rings = list(rings)
        while rings:
            rings = [r for r in rings if next(r, self) is not self]
        self.drain()


def scatter_scratch(chips, rows, width):
    half = chips // 2
    return [
        pltpu.VMEM((4, rows, width), F32),
        pltpu.VMEM((chips, rows, width), BF),
        pltpu.VMEM((chips, rows, width), BF),
        pltpu.VMEM((rows, width), BF),
        pltpu.VMEM((half, rows, width), BF),
        pltpu.VMEM((half, rows, width), BF),
    ]


def dot_nt(a, b):
    return lax.dot_general(a, b, (((1,), (1,)), ((), ())), preferred_element_type=F32)


def dot_tn(a, b):
    return lax.dot_general(a, b, (((0,), (0,)), ((), ())), preferred_element_type=F32)


def tiles(count, width, body):
    for i in range(count):
        body(pl.ds(i * width, width))


def experts_kernel(
    chips, cap,
    h2_ref, dy_ref, slot_ref, weight_ref, wg_hbm, wu_hbm, wd_hbm,
    xs_ref, de_ref, act_ref, dg_ref, du_ref,
    held, dy, wg, wu, wd, xs_b, de_b, act_b, dg_b, du_b,
    up, down, side, w_sem, dy_sem, own_sem, out_sem,
):
    hops = Hops(chips)
    half = chips // 2
    tok, width = h2_ref.shape
    ff = wg.shape[1]
    order = [0]
    for s in range(1, half):
        order += [-s, s]
    order += [half]
    number = {d: i for i, d in enumerate(order)}

    loads = [
        pltpu.make_async_copy(a, b, w_sem.at[i])
        for i, (a, b) in enumerate(((wg_hbm, wg), (wu_hbm, wu), (wd_hbm, wd)))
    ]

    def dy_copy(i):
        chip = hops.chip(order[i])
        return pltpu.make_async_copy(dy_ref.at[pl.ds(2 * chip, 2)], dy.at[i % 2], dy_sem.at[i % 2])

    def out_copies(i):
        chip = hops.chip(order[i])
        pairs = ((xs_b, xs_ref), (de_b, de_ref), (act_b, act_ref), (dg_b, dg_ref), (du_b, du_ref))
        return [
            pltpu.make_async_copy(b.at[i % 2], r.at[chip], out_sem.at[i % 2, j])
            for j, (b, r) in enumerate(pairs)
        ]

    hops.meet()
    own = pltpu.make_async_copy(h2_ref, held.at[hops.me], own_sem)
    own.start()

    def use(d):
        i = number[d]
        p = i % 2
        if i == 0:
            own.wait()
            for c in loads:
                c.start()
            dy_copy(0).start()
            for c in loads:
                c.wait()
        dy_copy(i).wait()
        if i + 1 < chips:
            dy_copy(i + 1).start()
        if i >= 2:
            for c in out_copies(i - 2):
                c.wait()
        chip = hops.chip(d)
        for k in range(2):
            dev = 2 * chip + k
            hit = slot_ref[pl.ds(dev, 1), :] == lax.broadcasted_iota(jnp.int32, (cap, tok), 0)
            pick = hit.astype(F32).astype(BF)
            scale = jnp.sum(
                jnp.where(hit, weight_ref[pl.ds(dev, 1), :], 0.0), axis=1, keepdims=True
            )
            rows = pl.ds(k * cap, cap)

            def choose(at, k=k, dev=dev, pick=pick, scale=scale, rows=rows):
                xs_b[p, rows, at] = dot32(pick, held[dev, :, at]).astype(BF)
                de_b[p, rows, at] = (scale * dot32(pick, dy[p, k, :, at])).astype(BF)

            tiles(width // 1024, 1024, choose)

        def hidden(at):
            gpre = dot32(xs_b[p], wg[:, at])
            upre = dot32(xs_b[p], wu[:, at])
            dact = dot_nt(de_b[p], wd[at, :])
            sig = 1.0 / (1.0 + jnp.exp(-gpre))
            act_b[p, :, at] = (gpre * sig * upre).astype(BF)
            dg_b[p, :, at] = (dact * upre * sig * (1.0 + gpre * (1.0 - sig))).astype(BF)
            du_b[p, :, at] = (dact * gpre * sig).astype(BF)

        tiles(ff // 512, 512, hidden)
        for c in out_copies(i):
            c.start()

    hops.turn(hops.gather([(h2_ref, lambda dev: held.at[dev], up, down, side)], use))
    for i in (chips - 2, chips - 1):
        for c in out_copies(i):
            c.wait()


def expert_rows(chips, cap, h2, dy_all, slot, weight, wg, wu, wd, collective_id):
    tok, width = h2.shape
    ff = wg.shape[1]
    anywhere = pl.BlockSpec(memory_space=pl.ANY)
    vmem = pl.BlockSpec(memory_space=pltpu.VMEM)
    wide = jax.ShapeDtypeStruct((chips, 2 * cap, width), BF)
    thin = jax.ShapeDtypeStruct((chips, 2 * cap, ff), BF)
    return pl.pallas_call(
        functools.partial(experts_kernel, chips, cap),
        out_shape=(wide, wide, thin, thin, thin),
        in_specs=[anywhere, anywhere, vmem, vmem, anywhere, anywhere, anywhere],
        out_specs=(anywhere,) * 5,
        scratch_shapes=[
            pltpu.VMEM((2 * chips, tok, width), BF),
            pltpu.VMEM((2, 2, tok, width), BF),
            pltpu.VMEM((width, ff), BF),
            pltpu.VMEM((width, ff), BF),
            pltpu.VMEM((ff, width), BF),
            pltpu.VMEM((2, 2 * cap, width), BF),
            pltpu.VMEM((2, 2 * cap, width), BF),
            pltpu.VMEM((2, 2 * cap, ff), BF),
            pltpu.VMEM((2, 2 * cap, ff), BF),
            pltpu.VMEM((2, 2 * cap, ff), BF),
            *ring_sems(chips),
            DMA((3,)),
            DMA((2,)),
            DMA,
            DMA((2, 5)),
        ],
        compiler_params=pltpu.CompilerParams(
            collective_id=collective_id, has_side_effects=True, vmem_limit_bytes=VMEM_LIMIT
        ),
        cost_estimate=pl.CostEstimate(
            flops=2 * chips * cap * width * ff * 6, transcendentals=0, bytes_accessed=200 << 20
        ),
        name="experts",
    )(h2, dy_all, slot, weight, wg, wu, wd)


def column_of(table, dev):
    lanes = lax.broadcasted_iota(jnp.int32, table.shape, 1)
    return jnp.sum(jnp.where(lanes == dev, table[...], 0.0), axis=1, keepdims=True)


def returned(hops, d, cap, tok, slot_ref, rows_ref, same_ref, other_ref, weight_ref=None):
    chip = hops.chip(d)
    lanes = lax.broadcasted_iota(jnp.int32, (tok, cap), 1).astype(F32)
    for k, ref in ((hops.core, same_ref), (1 - hops.core, other_ref)):
        pick = (column_of(slot_ref, 2 * chip + k) == lanes).astype(F32).astype(BF)
        rows = pl.ds(pl.multiple_of(k * cap, 16), cap)
        weight = None if weight_ref is None else column_of(weight_ref, 2 * chip + k)

        def spread(at, pick=pick, rows=rows, ref=ref, weight=weight):
            value = dot32(pick, rows_ref[rows, at])
            if weight is not None:
                value = weight * value
            ref[:, at] = value.astype(ref.dtype)

        tiles(rows_ref.shape[1] // 1024, 1024, spread)


def scatter_order(half):
    order = [half, half - 1, 1 - half]
    for s in range(half - 2, 0, -1):
        order += [-s, s]
    return order + [0]


def outputs_kernel(
    chips, cap,
    act_ref, xs_ref, de_ref, dg_ref, du_ref, slot_ref, weight_ref, wd_hbm,
    total_ref, down_ref, came_ref, gate_ref, up_ref,
    wd, left, right, made_d, made, act, rows_b, mine, out, came, far, up_in, down_in,
    up, down, side, w_sem, act_sem, left_sem, right_sem, made_sem, down_sem, rep_sem,
):
    hops = Hops(chips)
    replica = lax.axis_index("rep")
    tok, width = total_ref.shape
    order = scatter_order(chips // 2)
    number = {d: i for i, d in enumerate(order)}
    strip = right.shape[2]
    count = width // strip

    def act_copy(i):
        rows = pl.ds(pl.multiple_of(hops.chip(order[i]) * (2 * cap), 2 * cap), 2 * cap)
        return pltpu.make_async_copy(act_ref.at[rows], act.at[i % 2], act_sem.at[i % 2])

    jobs = [
        (thin, wide, result, i)
        for thin, wide, result in (
            (act_ref, de_ref, down_ref),
            (dg_ref, xs_ref, gate_ref),
            (du_ref, xs_ref, up_ref),
        )
        for i in range(count)
    ]
    done, stored, sent = [], {}, []

    def right_copy(n):
        at = pl.ds(jobs[n][3] * strip, strip)
        return pltpu.make_async_copy(jobs[n][1].at[:, at], right.at[n % 2], right_sem.at[n % 2])

    def job():
        n = len(done)
        if n == len(jobs):
            return
        done.append(n)
        thin, _, result, i = jobs[n]
        if i == 0:
            fresh = pltpu.make_async_copy(thin, left, left_sem)
            fresh.start()
            fresh.wait()
        right_copy(n).wait()
        if n + 1 < len(jobs):
            right_copy(n + 1).start()
        at = pl.ds(i * strip, strip)
        if n < count:
            made_d[i] = dot_tn(left[...], right[n % 2]).astype(BF)
            stored[n] = pltpu.make_async_copy(made_d.at[i], result.at[:, at], down_sem.at[i])
            c = pltpu.make_async_remote_copy(
                src_ref=made_d.at[i],
                dst_ref=came_ref.at[:, at],
                send_sem=rep_sem.at[0, i],
                recv_sem=rep_sem.at[1, i],
                device_id={"rep": 1 - replica},
                device_id_type=MESH,
            )
            c.start()
            sent.append(c)
        else:
            if n - 2 >= count:
                stored.pop(n - 2).wait()
            made[n % 2] = dot_tn(right[n % 2], left[...]).astype(BF)
            stored[n] = pltpu.make_async_copy(made.at[n % 2], result.at[at, :], made_sem.at[n % 2])
        stored[n].start()

    def produce(d, same_ref, other_ref):
        i = number[d]
        act_copy(i).wait()
        if i + 1 < chips:
            act_copy(i + 1).start()

        def last(at):
            rows_b[:, at] = dot32(act[i % 2], wd[:, at]).astype(BF)

        tiles(width // 512, 512, last)
        returned(hops, d, cap, tok, slot_ref, rows_b, same_ref, other_ref, weight_ref)

    def finish(value, at):
        total_ref[at, :] = value

    load = pltpu.make_async_copy(wd_hbm, wd, w_sem)
    load.start()
    act_copy(0).start()
    right_copy(0).start()
    hops.meet(2)
    load.wait()
    ring = hops.scatter(tok, produce, mine, out, came, far, up_in, down_in, up, down, side, finish)
    job()
    share = -(-(len(jobs) - 2) // (chips // 2 - 1))
    for step in range(chips // 2):
        next(ring)
        for _ in range(share if step else 1):
            job()
    hops.turn(ring)
    for c in stored.values():
        c.wait()
    for c in sent:
        c.wait()


def outputs(chips, cap, act, xs, de, dg, du, slot_t, weight_t, wd, collective_id):
    ff, width = wd.shape
    tok = slot_t.shape[0]
    strip = 512
    anywhere = pl.BlockSpec(memory_space=pl.ANY)
    vmem = pl.BlockSpec(memory_space=pltpu.VMEM)
    tall, flat = jax.ShapeDtypeStruct((width, ff), BF), jax.ShapeDtypeStruct((ff, width), BF)
    return pl.pallas_call(
        functools.partial(outputs_kernel, chips, cap),
        out_shape=(jax.ShapeDtypeStruct((tok, width), F32), flat, flat, tall, tall),
        in_specs=[anywhere] * 5 + [vmem] * 2 + [anywhere],
        out_specs=(vmem,) + (anywhere,) * 4,
        scratch_shapes=[
            pltpu.VMEM((ff, width), BF),
            pltpu.VMEM((2 * chips * cap, ff), BF),
            pltpu.VMEM((2, 2 * chips * cap, strip), BF),
            pltpu.VMEM((width // strip, ff, strip), BF),
            pltpu.VMEM((2, strip, ff), BF),
            pltpu.VMEM((2, 2 * cap, ff), BF),
            pltpu.VMEM((2 * cap, width), BF),
            *scatter_scratch(chips, tok, width),
            *ring_sems(chips),
            DMA,
            DMA((2,)),
            DMA,
            DMA((2,)),
            DMA((2,)),
            DMA((width // strip,)),
            DMA((2, width // strip)),
        ],
        compiler_params=pltpu.CompilerParams(
            collective_id=collective_id, has_side_effects=True, vmem_limit_bytes=63 << 20
        ),
        cost_estimate=pl.CostEstimate(
            flops=2 * 2 * chips * cap * width * ff * 4, transcendentals=0, bytes_accessed=200 << 20
        ),
        name="outputs",
    )(act, xs, de, dg, du, slot_t, weight_t, wd)


def rows_back_kernel(
    chips, cap,
    dg_ref, du_ref, slot_ref, wg_hbm, wu_hbm, total_ref,
    wg, wu, dg, du, drow, mine, out, came, far, up_in, down_in,
    up, down, side, w_sem, in_sem,
):
    hops = Hops(chips)
    tok, width = total_ref.shape
    order = scatter_order(chips // 2)
    number = {d: i for i, d in enumerate(order)}
    loads = [
        pltpu.make_async_copy(a, b, w_sem.at[i])
        for i, (a, b) in enumerate(((wg_hbm, wg), (wu_hbm, wu)))
    ]

    def in_copies(i):
        chip = hops.chip(order[i])
        return [
            pltpu.make_async_copy(r.at[chip], b.at[i % 2], in_sem.at[i % 2, j])
            for j, (r, b) in enumerate(((dg_ref, dg), (du_ref, du)))
        ]

    for c in loads + in_copies(0):
        c.start()
    hops.meet()
    for c in loads:
        c.wait()

    def produce(d, same_ref, other_ref):
        i = number[d]
        p = i % 2
        for c in in_copies(i):
            c.wait()
        if i + 1 < chips:
            for c in in_copies(i + 1):
                c.start()

        def back(at):
            drow[:, at] = (dot_nt(dg[p], wg[at, :]) + dot_nt(du[p], wu[at, :])).astype(BF)

        tiles(width // 512, 512, back)
        returned(hops, d, cap, tok, slot_ref, drow, same_ref, other_ref)

    def finish(value, at):
        total_ref[at, :] = value

    hops.turn(
        hops.scatter(tok, produce, mine, out, came, far, up_in, down_in, up, down, side, finish)
    )


def rows_back(chips, cap, dg, du, slot, wg, wu, collective_id):
    tok = slot.shape[0]
    width, ff = wg.shape
    anywhere = pl.BlockSpec(memory_space=pl.ANY)
    vmem = pl.BlockSpec(memory_space=pltpu.VMEM)
    return pl.pallas_call(
        functools.partial(rows_back_kernel, chips, cap),
        out_shape=jax.ShapeDtypeStruct((tok, width), F32),
        in_specs=[anywhere, anywhere, vmem, anywhere, anywhere],
        out_specs=vmem,
        scratch_shapes=[
            pltpu.VMEM((width, ff), BF),
            pltpu.VMEM((width, ff), BF),
            pltpu.VMEM((2, 2 * cap, ff), BF),
            pltpu.VMEM((2, 2 * cap, ff), BF),
            pltpu.VMEM((2 * cap, width), BF),
            *scatter_scratch(chips, tok, width),
            *ring_sems(chips),
            DMA((2,)),
            DMA((2, 2)),
        ],
        compiler_params=pltpu.CompilerParams(
            collective_id=collective_id, has_side_effects=True, vmem_limit_bytes=VMEM_LIMIT
        ),
        cost_estimate=pl.CostEstimate(
            flops=2 * chips * cap * width * ff * 6, transcendentals=0, bytes_accessed=200 << 20
        ),
        name="rows_back",
    )(dg, du, slot, wg, wu)


def turned(v, cosine, sine):
    return v * cosine + pltpu.roll(v, HD // 2, 1) * sine


def head_of(proj, at, gain, cosine, sine):
    value = proj[:, at]
    inverse = lax.rsqrt(jnp.mean(value * value, axis=-1, keepdims=True) + epsilon)
    hat = value * inverse
    return hat, inverse, turned(hat * gain, cosine, sine).astype(BF)


def softmax_rows(queries, keys, docs_q, docs_k):
    raw = dot_nt(queries, keys) * HD ** (-0.5)
    raw = jnp.where(docs_q == docs_k, raw, -1e30)
    grown = jnp.exp(raw - jnp.max(raw, axis=-1, keepdims=True))
    return grown * (1.0 / jnp.sum(grown, axis=-1, keepdims=True))


def columns_of(block, head, heads):
    return pl.ds(pl.multiple_of((block * heads + head) * HD, HD), HD)


def attention_kernel(
    chips, reps, heads,
    cot_ref, seq_ref, ga_ref, gf_ref, gq_ref, gk_ref, cos_ref, sin_ref, dc_ref, dr_ref, wq_hbm, wo_hbm,
    dy_ref, h1_out, proj_out, ob_out, mid_ref, h2_ref,
    wq, wo, give, came, h1_ref, proj_ref, ob_ref, up, down, side, rep_sem, own_sem, out_sem,
):
    hops = Hops(chips)
    rep = lax.axis_index("rep")
    seq_len, width = seq_ref.shape
    tok = mid_ref.shape[0]
    block = min(256, seq_len)
    loads = [
        pltpu.make_async_copy(a, b, own_sem.at[i])
        for i, (a, b) in enumerate(((wq_hbm, wq), (wo_hbm, wo), (cot_ref, dy_ref.at[hops.me])))
    ]
    hops.meet(reps)
    ring = hops.gather([(cot_ref, lambda dev: dy_ref.at[dev], up, down, side)], lambda d: None)
    next(ring)
    for c in loads:
        c.start()

    def normed(i, carry):
        rows = pl.ds(pl.multiple_of(i * 64, 64), 64)
        v = seq_ref[rows, :].astype(F32)
        v = v * lax.rsqrt(jnp.mean(v * v, axis=-1, keepdims=True) + epsilon)
        h1_ref[rows, :] = (v * ga_ref[...]).astype(BF)
        return carry

    lax.fori_loop(0, seq_len // 64, normed, 0)
    loads[0].wait()
    total = 3 * heads * HD
    step = 512 if total % 512 == 0 else HD
    for i in range(total // step):
        at = pl.ds(i * step, step)
        proj_ref[:, at] = dot32(h1_ref[...], wq[:, at])

    stores = [
        pltpu.make_async_copy(a, b, out_sem.at[i])
        for i, (a, b) in enumerate(((h1_ref, h1_out), (proj_ref, proj_out), (ob_ref, ob_out)))
    ]
    stores[0].start()
    stores[1].start()

    def one(head, carry):
        _, _, q_b = head_of(
            proj_ref, columns_of(0, head, heads), gq_ref[...], cos_ref[...], sin_ref[...]
        )
        _, _, k_b = head_of(
            proj_ref, columns_of(1, head, heads), gk_ref[...], cos_ref[...], sin_ref[...]
        )
        v_b = proj_ref[:, columns_of(2, head, heads)].astype(BF)
        for i in range(seq_len // block):
            rows = slice(i * block, (i + 1) * block)
            probs = softmax_rows(q_b[rows], k_b, dc_ref[rows, :], dr_ref[...])
            ob_ref[rows, columns_of(0, head, heads)] = dot32(probs.astype(BF), v_b).astype(BF)
        return carry

    lax.fori_loop(0, heads // 2, one, 0)
    next(ring)
    lax.fori_loop(heads // 2, heads, one, 0)
    stores[2].start()
    loads[1].wait()
    swaps = []
    for k in range(1, reps):
        for i in range(width // 512):
            at = pl.ds(i * 512, 512)
            give[k - 1, :, at] = dot32(ob_ref[pl.ds(k * tok, tok), :], wo[:, at]).astype(BF)
        c = pltpu.make_async_remote_copy(
            src_ref=give.at[k - 1],
            dst_ref=came.at[k - 1],
            send_sem=rep_sem.at[0, k - 1],
            recv_sem=rep_sem.at[1, k - 1],
            device_id={"rep": (rep + k) % reps},
            device_id_type=MESH,
        )
        c.start()
        swaps.append(c)
    for i in range(width // 512):
        at = pl.ds(i * 512, 512)
        mid_ref[:, at] = dot32(ob_ref[pl.ds(0, tok), :], wo[:, at])
    next(ring)
    for c in swaps:
        c.wait()

    def second(i, carry):
        rows = pl.ds(pl.multiple_of(i * 64, 64), 64)
        v = seq_ref[rows, :].astype(F32) + mid_ref[rows, :]
        for k in range(1, reps):
            v = v + came[k - 1, rows, :].astype(F32)
        mid_ref[rows, :] = v
        v = v * lax.rsqrt(jnp.mean(v * v, axis=-1, keepdims=True) + epsilon)
        h2_ref[rows, :] = (v * gf_ref[...]).astype(BF)
        return carry

    lax.fori_loop(0, tok // 64, second, 0)
    loads[2].wait()
    hops.turn(ring)
    for c in stores:
        c.wait()


def attention(chips, reps, cot, seq, ga, gf, gq, gk, cosine, sine, docs, w_qkv, w_out, collective_id):
    seq_len, width = seq.shape
    tok = cot.shape[0]
    heads = w_out.shape[0] // HD
    anywhere = pl.BlockSpec(memory_space=pl.ANY)
    vmem = pl.BlockSpec(memory_space=pltpu.VMEM)
    return pl.pallas_call(
        functools.partial(attention_kernel, chips, reps, heads),
        out_shape=(
            jax.ShapeDtypeStruct((2 * chips, tok, width), BF),
            jax.ShapeDtypeStruct((seq_len, width), BF),
            jax.ShapeDtypeStruct((seq_len, 3 * heads * HD), F32),
            jax.ShapeDtypeStruct((seq_len, heads * HD), BF),
            jax.ShapeDtypeStruct((tok, width), F32),
            jax.ShapeDtypeStruct((tok, width), BF),
        ),
        in_specs=[anywhere] + [vmem] * 9 + [anywhere] * 2,
        out_specs=(anywhere,) * 4 + (vmem,) * 2,
        scratch_shapes=[
            pltpu.VMEM(w_qkv.shape, BF),
            pltpu.VMEM(w_out.shape, BF),
            pltpu.VMEM((reps - 1, tok, width), BF),
            pltpu.VMEM((reps - 1, tok, width), BF),
            pltpu.VMEM((seq_len, width), BF),
            pltpu.VMEM((seq_len, 3 * heads * HD), F32),
            pltpu.VMEM((seq_len, heads * HD), BF),
            *ring_sems(chips),
            DMA((2, reps - 1)),
            DMA((3,)),
            DMA((3,)),
        ],
        compiler_params=pltpu.CompilerParams(
            collective_id=collective_id, has_side_effects=True, vmem_limit_bytes=VMEM_LIMIT
        ),
        cost_estimate=pl.CostEstimate(
            flops=2 * seq_len * w_qkv.size, transcendentals=0, bytes_accessed=100 << 20
        ),
        name="attention",
    )(cot, seq, ga, gf, gq, gk, cosine, sine, docs[:, None], docs[None, :], w_qkv, w_out)


def attention_back_kernel(
    heads,
    proj_ref, mid_ref, wo_ref, gq_ref, gk_ref, cos_ref, sin_ref, dc_ref, dr_ref,
    grad_ref, qt_ref, kt_ref,
    dob, dk, dv,
):
    seq_len = proj_ref.shape[0]
    block = min(256, seq_len)
    scale = HD ** (-0.5)
    for i in range(heads * HD // 512):
        at = pl.ds(i * 512, 512)
        dob[:, at] = dot_nt(mid_ref[...], wo_ref[at, :]).astype(BF)
    qt_ref[...] = jnp.zeros_like(qt_ref)
    kt_ref[...] = jnp.zeros_like(kt_ref)

    def unturned(grad, hat, inverse, gain, rows):
        grad = turned(grad, cos_ref[rows, :], -sin_ref[rows, :])
        scaled = grad * gain
        pre = inverse * (scaled - hat * jnp.mean(scaled * hat, axis=-1, keepdims=True))
        return pre.astype(BF), jnp.sum(grad * hat, axis=0, keepdims=True)

    def one(head, carry):
        q_at, k_at, v_at = (columns_of(b, head, heads) for b in range(3))
        q_hat, q_inv, q_b = head_of(proj_ref, q_at, gq_ref[...], cos_ref[...], sin_ref[...])
        k_hat, k_inv, k_b = head_of(proj_ref, k_at, gk_ref[...], cos_ref[...], sin_ref[...])
        v_b = proj_ref[:, v_at].astype(BF)
        for i in range(seq_len // block):
            rows = slice(i * block, (i + 1) * block)
            probs = softmax_rows(q_b[rows], k_b, dc_ref[rows, :], dr_ref[...])
            grad_o = dob[rows, columns_of(0, head, heads)]
            grad_p = dot_nt(grad_o, v_b)
            grad_s = (
                probs * (grad_p - jnp.sum(probs * grad_p, axis=-1, keepdims=True))
            ).astype(BF)
            dv_part = dot_tn(probs.astype(BF), grad_o)
            dk_part = dot_tn(grad_s, q_b[rows])
            if i == 0:
                dv[...] = dv_part
                dk[...] = dk_part
            else:
                dv[...] += dv_part
                dk[...] += dk_part
            pre, terms = unturned(
                dot32(grad_s, k_b) * scale, q_hat[rows], q_inv[rows], gq_ref[...], rows
            )
            grad_ref[rows, q_at] = pre
            qt_ref[...] += terms
        pre, terms = unturned(dk[...] * scale, k_hat, k_inv, gk_ref[...], slice(0, seq_len))
        grad_ref[:, k_at] = pre
        kt_ref[...] += terms
        grad_ref[:, v_at] = dv[...].astype(BF)
        return carry

    lax.fori_loop(0, heads, one, 0)


def attention_back(proj, mid, w_out, gq, gk, cosine, sine, docs):
    seq_len = proj.shape[0]
    heads = w_out.shape[0] // HD
    vmem = pl.BlockSpec(memory_space=pltpu.VMEM)
    return pl.pallas_call(
        functools.partial(attention_back_kernel, heads),
        out_shape=(
            jax.ShapeDtypeStruct(proj.shape, BF),
            jax.ShapeDtypeStruct((1, HD), F32),
            jax.ShapeDtypeStruct((1, HD), F32),
        ),
        in_specs=[vmem] * 9,
        out_specs=(vmem,) * 3,
        scratch_shapes=[
            pltpu.VMEM((seq_len, heads * HD), BF),
            pltpu.VMEM((seq_len, HD), F32),
            pltpu.VMEM((seq_len, HD), F32),
        ],
        compiler_params=pltpu.CompilerParams(vmem_limit_bytes=VMEM_LIMIT),
        cost_estimate=pl.CostEstimate(
            flops=20 * heads * seq_len * seq_len * HD, transcendentals=0, bytes_accessed=20 << 20
        ),
        name="attention_back",
    )(proj, mid, w_out, gq, gk, cosine, sine, docs[:, None], docs[None, :])


def ring_sems(chips):
    return [DMA((2, chips // 2)), DMA((2, chips // 2)), DMA((2, chips))]


def dense_gradients_kernel(
    chips, split_out, h1_ref, grad_ref, ob_ref, mid_ref, gains_ref, qkv_ref, out_ref, gain_ref, *scratch
):
    hops = Hops(chips)
    scratches = [scratch[9 * i : 9 * i + 9] for i in range(4)]
    hops.meet(2 if split_out else 1)
    first = hops.core == 0
    if split_out:
        q_sum, q_came, o_sum, o_came, o_give, o_got, g_sum, g_came, rep_sem, flip_sem = scratch[36:]
    else:
        q_sum, o_sum, g_sum = qkv_ref, out_ref, gain_ref

    def product(left_ref, right_ref, rows, width):
        step = 512 if width % 512 == 0 else 256

        def produce(d, same_ref, other_ref):
            columns = pl.ds(pl.multiple_of(2 * rows * hops.chip(d), 2 * rows), 2 * rows)
            left = left_ref[:, columns]

            def block(at):
                value = dot_tn(left, right_ref[:, at])
                low, high = value[:rows], value[rows:]
                same_ref[:, at] = jnp.where(first, low, high)
                other_ref[:, at] = jnp.where(first, high, low).astype(BF)

            tiles(width // step, step, block)

        return produce

    def small(d, same_ref, other_ref):
        dev = hops.device(d)
        same_ref[...] = gains_ref[dev]
        other_ref[...] = gains_ref[dev + 1 - 2 * hops.core].astype(BF)

    def into(ref):
        def finish(value, at):
            ref[at, :] = value.astype(ref.dtype)

        return finish

    def ring(produce, ref, bufs):
        return hops.scatter(ref.shape[0], produce, *bufs, into(ref))

    shard, wide = q_sum.shape
    replica = lax.axis_index("rep")
    halves = [pl.ds(0, wide // 2), pl.ds(wide // 2, wide // 2)]
    if split_out:
        pairs = [(o_sum, o_came), *((q_sum.at[:, h], q_came.at[:, h]) for h in halves), (g_sum, g_came)]
        swaps = [
            pltpu.make_async_remote_copy(
                src_ref=src,
                dst_ref=dst,
                send_sem=rep_sem.at[0, i],
                recv_sem=rep_sem.at[1, i],
                device_id={"rep": 1 - replica},
                device_id_type=MESH,
            )
            for i, (src, dst) in enumerate(pairs)
        ]

    def then_swap(ring_steps, i):
        yield from ring_steps
        if split_out:
            swaps[i].start()

    rings = []
    if split_out:
        steps = ring(product(ob_ref, mid_ref, *o_sum.shape), o_sum, scratches[2])
        rings.append(then_swap(steps, 0))
    for i, h in enumerate(halves):
        part = product(h1_ref, grad_ref.at[:, h], shard, wide // 2)
        rings.append(then_swap(ring(part, q_sum.at[:, h], scratches[i]), 1 + i))
    rings.append(then_swap(ring(small, g_sum, scratches[3]), 3))
    hops.turn(*rings)
    if not split_out:
        return

    mine = hops.core == replica
    swaps[0].wait()
    o_give[...] = jnp.where(mine, o_came[...], o_sum[...])
    give = hops.copy(o_give, o_got, flip_sem.at[0], flip_sem.at[1], hops.flip)
    give.start()
    keep = jnp.where(mine, o_sum[...], o_came[...])
    even = replica == 0
    for i in range(wide // HD):
        if i * HD == 0 or i * HD == wide // 2:
            swaps[1 + (i > 0)].wait()
        own, came = q_sum[:, pl.ds(i * HD, HD)], q_came[:, pl.ds(i * HD, HD)]
        qkv_ref[:, pl.ds(2 * i * HD, HD)] = jnp.where(even, own, came).astype(F32)
        qkv_ref[:, pl.ds((2 * i + 1) * HD, HD)] = jnp.where(even, came, own).astype(F32)
    swaps[3].wait()
    gain_ref[...] = g_sum[...] + g_came[...]
    give.wait()
    half = o_sum.shape[0]
    got = o_got[...]
    out_ref[pl.ds(0, half), :] = jnp.where(first, keep, got).astype(F32)
    out_ref[pl.ds(half, half), :] = jnp.where(first, got, keep).astype(F32)


def dense_gradients(chips, split_out, h1, grad, ob, mid, gain_blocks, collective_id):
    shard = h1.shape[1] // (2 * chips)
    width = grad.shape[1]
    half = ob.shape[1] // (2 * chips) if split_out else 32
    vmem = pl.BlockSpec(memory_space=pltpu.VMEM)
    shapes = ((shard, width), (half, D), gain_blocks.shape[1:])
    scratch = []
    for rows, columns in ((shard, width // 2), (shard, width // 2), *shapes[1:]):
        scratch += [*scatter_scratch(chips, rows, columns), *ring_sems(chips)]
    if split_out:
        scratch += [pltpu.VMEM(shapes[0], BF)] * 2 + [pltpu.VMEM(shapes[1], BF)] * 4
        scratch += [pltpu.VMEM(shapes[2], F32)] * 2 + [DMA((2, 4)), DMA((2,))]
        shapes = ((shard, 2 * width), (2 * half, D), shapes[2])
    kinds = (F32, F32, F32) if split_out else (BF, BF, F32)
    return pl.pallas_call(
        functools.partial(dense_gradients_kernel, chips, split_out),
        out_shape=tuple(
            jax.ShapeDtypeStruct(shape, kind) for shape, kind in zip(shapes, kinds, strict=True)
        ),
        in_specs=[vmem] * 5,
        out_specs=(vmem,) * 3,
        scratch_shapes=scratch,
        compiler_params=pltpu.CompilerParams(
            collective_id=collective_id, has_side_effects=True, vmem_limit_bytes=VMEM_LIMIT
        ),
        cost_estimate=pl.CostEstimate(
            flops=2 * h1.size * width, transcendentals=0, bytes_accessed=200 << 20
        ),
        name="dense_gradients",
    )(h1, grad, ob, mid, gain_blocks)


def start_kernel(
    chips, reps, heads, split_out,
    tok_ref, small_ref, wq_ref, wo_ref,
    seq_ref, smalls_ref, full_ref, out_ref,
    own_q, own_o, *sems,
):
    hops = Hops(chips)
    rep = lax.axis_index("rep")
    up, down, side, up_s, down_s, side_s, up_o, down_o, side_o, rep_sem, col_sem, own_sem, half_sem = sems
    pieces = []
    for i in range(3 * heads):
        q, j = i // heads, i % heads
        at = pl.multiple_of(((q * heads + j) * reps + rep) * HD, HD)
        pieces.append(
            pltpu.make_async_copy(
                wq_ref.at[:, pl.ds(at, HD)], own_q.at[:, pl.ds(i * HD, HD)], col_sem.at[i]
            )
        )
        pieces[-1].start()
    hops.meet(reps)
    swaps = []
    for k in range(1, reps):
        c = pltpu.make_async_remote_copy(
            src_ref=tok_ref,
            dst_ref=seq_ref.at[reps - k],
            send_sem=rep_sem.at[0, reps - k],
            recv_sem=rep_sem.at[1, reps - k],
            device_id={"rep": (rep + k) % reps},
            device_id_type=MESH,
        )
        c.start()
        swaps.append(c)
    locals_ = [
        pltpu.make_async_copy(tok_ref, seq_ref.at[0], own_sem.at[0]),
        pltpu.make_async_copy(small_ref, smalls_ref.at[hops.me], own_sem.at[1]),
    ]
    for c in locals_:
        c.start()
    for c in pieces:
        c.wait()
    mine = pltpu.make_async_copy(own_q, full_ref.at[hops.me], own_sem.at[2])
    mine.start()
    items = [
        (own_q, lambda dev: full_ref.at[dev], up, down, side),
        (small_ref, lambda dev: smalls_ref.at[dev], up_s, down_s, side_s),
    ]
    if split_out:
        rows = own_o.shape[0]
        kept = wo_ref.at[pl.ds(pl.multiple_of(hops.core * rows, rows), rows)]
        given = wo_ref.at[pl.ds(pl.multiple_of((1 - hops.core) * rows, rows), rows)]
        give = hops.copy(given, own_o, half_sem.at[0], half_sem.at[1], hops.flip)

        @pl.when(hops.core == rep)
        def _():
            give.start()
            keep = pltpu.make_async_copy(kept, own_o, half_sem.at[2])
            keep.start()
            keep.wait()
            give.wait_send()

        @pl.when(hops.core != rep)
        def _():
            give.wait_recv()

        def slot(dev):
            return out_ref.at[dev // 2, pl.ds(pl.multiple_of(dev % 2 * rows, rows), rows)]

        mine_o = pltpu.make_async_copy(own_o, slot(hops.me), half_sem.at[3])
        mine_o.start()
        items.append((own_o, slot, up_o, down_o, side_o))
    hops.turn(hops.gather(items, lambda d: None))
    for c in locals_:
        c.wait()
    mine.wait()
    if split_out:
        mine_o.wait()
    for c in swaps:
        c.wait()


def start(chips, reps, heads, split_out, tok, small, w_qkv, w_out, collective_id):
    anywhere = pl.BlockSpec(memory_space=pl.ANY)
    vmem = pl.BlockSpec(memory_space=pltpu.VMEM)
    shard, wide = w_qkv.shape[0], 3 * heads * HD
    half = w_out.shape[0] // 2
    return pl.pallas_call(
        functools.partial(start_kernel, chips, reps, heads, split_out),
        out_shape=(
            jax.ShapeDtypeStruct((reps, *tok.shape), BF),
            jax.ShapeDtypeStruct((2 * chips, *small.shape), F32),
            jax.ShapeDtypeStruct((2 * chips, shard, wide), BF),
            jax.ShapeDtypeStruct((chips, 2 * half, D), BF),
        ),
        in_specs=[vmem, vmem, anywhere, anywhere],
        out_specs=(anywhere,) * 4,
        scratch_shapes=[
            pltpu.VMEM((shard, wide), BF),
            pltpu.VMEM((half, D), BF),
            *ring_sems(chips),
            *ring_sems(chips),
            *ring_sems(chips),
            DMA((2, max(reps, 2))),
            DMA((3 * heads,)),
            DMA((3,)),
            DMA((4,)),
        ],
        compiler_params=pltpu.CompilerParams(collective_id=collective_id, has_side_effects=True),
        cost_estimate=pl.CostEstimate(
            flops=0, transcendentals=0, bytes_accessed=200 << 20
        ),
        name="start",
    )(tok, small, w_qkv, w_out)


def per_device(
    tokens, w_qkv, w_out, gains, w_gate, w_up, w_down, segment_ids, routes, gate_weights, cotangent
):
    groups = lax.axis_size("grp")
    reps = lax.axis_size("rep")
    ring = Ring(groups)
    rep, grp = lax.axis_index("rep"), lax.axis_index("grp")
    rel = jnp.asarray(ring.table())[grp]
    tok_rows = tokens.shape[1]
    seq_len = segment_ids.shape[1]
    heads = HEADS // reps
    wide = heads * HD

    def from_rep(v, k):
        return lax.ppermute(v, "rep", [((s + k) % reps, s) for s in range(reps)])

    def to_rep(v, k):
        return lax.ppermute(v, "rep", [(s, (s + k) % reps) for s in range(reps)])

    def rep_gather(v):
        return jnp.concatenate([v] + [from_rep(v, k) for k in range(1, reps)], axis=0)

    def rep_scatter(v):
        parts = v.reshape(reps, tok_rows, v.shape[-1])
        out = parts[0].astype(F32)
        for k in range(1, reps):
            out = out + to_rep(parts[k].astype(BF), k).astype(F32)
        return out

    own_b = tokens[0]
    gates_f = gate_weights[0]
    experts = jnp.arange(groups, dtype=jnp.int32)
    weight_of = jnp.sum(
        jnp.where(routes[0][None] == experts[:, None, None], gates_f[None], 0.0), axis=-1
    )
    gain_rows = -(-gains.shape[0] // tok_rows)
    small_rows = -(-(groups + gain_rows) // 16) * 16
    small = jnp.concatenate(
        [
            weight_of,
            jnp.pad(gains.astype(F32), (0, gain_rows * tok_rows - gains.shape[0])).reshape(
                gain_rows, tok_rows
            ),
            jnp.zeros((small_rows - groups - gain_rows, tok_rows), F32),
        ],
        axis=0,
    )
    split_out = reps == 2 and heads == ring.chips
    seq_b, smalls, full_qkv, my_out = start(
        ring.chips, reps, heads, split_out, own_b, small, w_qkv, w_out, 1
    )
    seq_b = seq_b.reshape(seq_len, D)
    shard = full_qkv.shape[1]
    full_qkv = full_qkv.reshape(D, 3 * wide)
    if not split_out:
        my_out = lax.all_gather(w_out, "grp", axis=0, tiled=True)
        my_out = lax.dynamic_index_in_dim(
            my_out.reshape(heads, reps, HD, D), rep, axis=1, keepdims=False
        )
    my_out = my_out.reshape(wide, D)
    gains_f = smalls[:, groups : groups + gain_rows].reshape(groups, -1)
    gains_f = gains_f[:, : gains.shape[0]].reshape(-1)
    weight_in = lax.dynamic_index_in_dim(smalls, grp, 1, False)
    g_attn = gains_f[:D]
    g_ffn = gains_f[D : 2 * D]
    g_query = gains_f[2 * D : 2 * D + HD]
    g_key = gains_f[2 * D + HD :]

    def this_first(table):
        return lax.dynamic_slice_in_dim(
            jnp.concatenate([table, table], axis=0), rep * tok_rows, seq_len, axis=0
        )

    frequency = np.float32(rope_base) ** (-2.0 * np.arange(HD // 2, dtype=np.float32) / HD)
    angles = np.arange(seq_len, dtype=np.float32)[:, None] * frequency.astype(np.float32)[None, :]
    cosine = this_first(jnp.asarray(np.concatenate([np.cos(angles)] * 2, axis=1)))
    sine = this_first(jnp.asarray(np.concatenate([-np.sin(angles), np.sin(angles)], axis=1)))
    docs = this_first(segment_ids[0])
    g_query, g_key = g_query[None], g_key[None]
    dy_all, h1_b, projected, attended_b, mid_rows, h2_b = attention(
        ring.chips,
        reps,
        cotangent[0],
        seq_b,
        g_attn[None],
        g_ffn[None],
        g_query,
        g_key,
        cosine,
        sine,
        docs,
        full_qkv,
        my_out,
        5,
    )

    chips = ring.chips
    entries = tok_rows * TOP
    capacity = min(tok_rows, (9 * entries + 8 * groups - 1) // (8 * groups))
    capacity = -(-capacity // 16) * 16
    named = weight_in > 0
    before = dot32(
        named.astype(BF), jnp.tri(tok_rows, dtype=BF).T
    )
    slot = jnp.where(named, before - 1.0, -1.0).astype(jnp.int32)
    rows_in, grads_in, acts, grad_gates, grad_ups = expert_rows(
        chips, capacity, h2_b, dy_all, slot, weight_in, w_gate[0], w_up[0], w_down[0], 2
    )
    all_rows = rows_in.reshape(-1, D)
    all_grads = grads_in.reshape(-1, D)
    all_acts = acts.reshape(groups * capacity, -1)
    all_gates = grad_gates.reshape(groups * capacity, -1)
    all_ups = grad_ups.reshape(groups * capacity, -1)

    def rep_send(v):
        return v, [from_rep(v, k) for k in range(1, reps)]

    def rep_sum(sent, after):
        (v, came), _ = lax.optimization_barrier((sent, after))
        return v.astype(F32) + sum(c.astype(F32) for c in came)

    slot_t, weight_t = slot.astype(F32).T, weight_in.T
    together = split_out and chips <= 8
    if together:
        out_sum, own_down, came_down, grad_wgate, grad_wup = outputs(
            chips, capacity, all_acts, all_rows, all_grads, all_gates, all_ups,
            slot_t, weight_t, w_down[0], 6,
        )
        grad_wdown = (own_down, [came_down])
    else:
        grad_wdown = rep_send(
            jnp.einsum("rf,rd->fd", all_acts, all_grads, preferred_element_type=F32).astype(BF)
        )
        grad_wgate = jnp.einsum("rd,rf->df", all_rows, all_gates, preferred_element_type=F32).astype(BF)
        grad_wup = jnp.einsum("rd,rf->df", all_rows, all_ups, preferred_element_type=F32).astype(BF)
    grad_wgate = rep_send(grad_wgate)
    grad_wup = rep_send(grad_wup)

    cuts = 1 if chips <= 8 else chips // 8
    (grad_gates, grad_ups), _ = lax.optimization_barrier(
        ((grad_gates, grad_ups), (grad_wdown[0], grad_wgate[0], grad_wup[0]))
    )
    grad_h2 = jnp.concatenate(
        [
            rows_back(chips, capacity, grad_gates, grad_ups, slot_t, wg, wu, 8 + i)
            for i, (wg, wu) in enumerate(
                zip(jnp.split(w_gate[0], cuts), jnp.split(w_up[0], cuts), strict=True)
            )
        ],
        axis=1,
    )


    grad_out = cotangent[0].astype(F32)
    _, hat_two, inv_two = rms_forward(mid_rows, g_ffn)
    grad_mid_norm, ffn_terms = rms_backward(grad_h2, hat_two, inv_two, g_ffn)
    grad_mid = grad_out + grad_mid_norm
    grad_mid_b = grad_mid.astype(BF)
    if not together:
        pick = (slot[:, None, :] == jnp.arange(capacity, dtype=jnp.int32)[None, :, None]).astype(BF)
        row_weight = jnp.sum(pick.astype(F32) * weight_in[:, None, :], axis=-1)
        acts_late, _ = lax.optimization_barrier((all_acts, grad_mid_b))
        eout = dot32(acts_late, w_down[0]).astype(BF).astype(F32)
        eout = (row_weight.reshape(-1, 1) * eout).astype(BF).reshape(groups, capacity, D)
        out_all = jnp.einsum("gct,gcd->gtd", pick, eout, preferred_element_type=F32).astype(BF)
        out_sum = lax.psum_scatter(
            out_all.reshape(groups * tok_rows, D), "grp", scatter_dimension=0, tiled=True
        )
    result = mid_rows + lax.optimization_barrier((out_sum, grad_mid_b))[0].astype(F32)
    grad_wdown = rep_sum(grad_wdown, grad_mid_b)
    grad_wgate = rep_sum(grad_wgate, grad_mid_b)
    grad_branch_b = rep_gather(grad_mid_b)
    (grad_branch_b, result, grad_wdown, grad_wgate), _ = lax.optimization_barrier(
        ((grad_branch_b, result, grad_wdown, grad_wgate), grad_mid_b)
    )
    grad_proj, query_terms, key_terms = attention_back(
        projected, grad_branch_b, my_out, g_query, g_key, cosine, sine, docs
    )
    _, hat_one, inv_one = rms_forward(seq_b.astype(F32), g_attn)
    grad_h1_part = jnp.einsum("te,de->td", grad_proj, full_qkv, preferred_element_type=F32)
    attn_terms = grad_h1_part * hat_one
    grad_h1 = rep_scatter(grad_h1_part)
    grad_rows_one, _ = rms_backward(grad_h1, hat_one[:tok_rows], inv_one[:tok_rows], g_attn)
    grad_tokens = grad_mid + grad_rows_one
    grad_gains = jnp.concatenate(
        [
            jnp.sum(attn_terms, axis=0),
            jnp.sum(ffn_terms, axis=0),
            query_terms[0],
            key_terms[0],
        ]
    )

    gain_size = gains.shape[0]
    gain_blocks = jnp.pad(
        grad_gains.reshape(groups, gain_size), ((0, 0), (0, 4096 - gain_size))
    ).reshape(groups, 32, 128)
    shard_qkv, half_out, total = dense_gradients(
        chips,
        split_out,
        h1_b,
        grad_proj,
        attended_b,
        grad_branch_b,
        gain_blocks,
        4,
    )
    total = total.reshape(-1)[:gain_size]
    grad_wup = rep_sum(grad_wup, shard_qkv)

    if split_out:
        shard_out = half_out
    else:
        qkv_all = [shard_qkv] + [from_rep(shard_qkv, k) for k in range(1, reps)]
        columns = jnp.stack(qkv_all, axis=0).reshape(reps, shard, 3, heads, HD)
        columns = columns[(jnp.arange(reps) - rep) % reps]
        shard_qkv = columns.transpose(1, 2, 3, 0, 4).reshape(shard, 3 * D).astype(F32)
        grad_wout = dot_tn(attended_b, grad_branch_b)
        whole = lax.dynamic_update_slice(
            jnp.zeros((heads, reps, HD, D), BF),
            grad_wout.astype(BF).reshape(heads, 1, HD, D),
            (0, rep, 0, 0),
        ).reshape(D, D)
        shard_out = lax.psum(
            lax.psum_scatter(whole, "grp", scatter_dimension=0, tiled=True), "rep"
        ).astype(F32)
        own_gains = total
        for k in range(1, reps):
            total = total + from_rep(own_gains, k)
    return (
        result[None],
        grad_tokens[None],
        shard_qkv,
        shard_out,
        total,
        grad_wgate[None],
        grad_wup[None],
        grad_wdown[None],
    )


def solution(mesh):
    in_specs = (
        P("grp", "rep", None),
        P("grp", None),
        P("grp", None),
        P("grp"),
        P("grp", None, None),
        P("grp", None, None),
        P("grp", None, None),
        P("grp", None),
        P("grp", "rep", None),
        P("grp", "rep", None),
        P("grp", "rep", None),
    )
    out_specs = (
        P("grp", "rep", None),
        P("grp", "rep", None),
        P("grp", None),
        P("grp", None),
        P("grp"),
        P("grp", None, None),
        P("grp", None, None),
        P("grp", None, None),
    )
    return jax.shard_map(
        per_device, mesh=mesh, in_specs=in_specs, out_specs=out_specs, check_vma=False
    )
```

```python
import functools

import jax
import jax.numpy as jnp
import numpy as np
from jax import lax
from jax.experimental import pallas as pl
from jax.experimental.pallas import tpu as pltpu
from jax.sharding import PartitionSpec as P

D = 2048
HEADS = 16
HD = 128
TOP = 8
BF = jnp.bfloat16
F32 = jnp.float32

epsilon = 1e-06
rope_base = 10000.0


def rms_forward(values, gain_vec):
    inverse = lax.rsqrt(jnp.mean(values * values, axis=-1, keepdims=True) + epsilon)
    normed = values * inverse
    return (normed * gain_vec, normed, inverse)


def rms_backward(grad_out, normed, inverse, gain_vec):
    scaled = grad_out * gain_vec
    grad_in = inverse * (scaled - normed * jnp.mean(scaled * normed, axis=-1, keepdims=True))
    return (grad_in, grad_out * normed)


def dot32(a, b):
    return jnp.dot(a, b, preferred_element_type=F32)


class Ring:
    def __init__(self, devices):
        self.devices = devices
        self.chips = devices // 2
        outer = 4 if self.chips % 4 == 0 else 2
        inner = self.chips // outer
        cycle = [(a, 0) for a in range(outer)]
        for step, a in enumerate(reversed(range(outer))):
            columns = range(1, inner)
            cycle += [(a, b) for b in (columns if step % 2 == 0 else reversed(columns))]
        self.cycle = [a * inner + b for a, b in cycle]
        self.place = {chip: i for i, chip in enumerate(self.cycle)}
        self.half = self.chips // 2

    def perm(self, shift):
        pairs = []
        for chip in range(self.chips):
            other = self.cycle[(self.place[chip] + shift) % self.chips]
            pairs += [(2 * chip + core, 2 * other + core) for core in range(2)]
        return pairs

    def table(self):
        out = np.zeros((self.devices, self.chips, 2), np.int32)
        for dev in range(self.devices):
            chip, core = dev // 2, dev % 2
            for d in range(self.chips):
                other = self.cycle[(self.place[chip] + d) % self.chips]
                out[dev, d, 0] = 2 * other + core
                out[dev, d, 1] = 2 * other + (1 - core)
        return out

    def ahead(self, v):
        return lax.ppermute(v, "grp", self.perm(1))

    def back(self, v):
        return lax.ppermute(v, "grp", self.perm(-1))

    def flip(self, v):
        return lax.ppermute(v, "grp", [(i, i ^ 1) for i in range(self.devices)])

    def gather(self, own):
        rows = own.shape[0] // 2
        blocks = {0: (own, self.flip(own))}
        up = down = own
        for step in range(1, self.half):
            up, down = self.ahead(up), self.back(down)
            blocks[-step % self.chips] = (up, self.flip(up))
            blocks[step] = (down, self.flip(down))
        first, last = self.ahead(up[:rows]), self.back(down[rows:])
        far = jnp.concatenate([first, last], axis=0)
        blocks[self.half] = (far, self.flip(far))
        return blocks

    def scatter_sum(self, blocks):
        def joined(d):
            same, other = blocks[d]
            return same.astype(F32) + self.flip(other.astype(BF)).astype(F32)

        far = joined(self.half).astype(BF)
        rows = far.shape[0] // 2
        up, down = self.ahead(far[:rows]), self.back(far[rows:])
        zero = jnp.zeros_like(up)
        up = jnp.concatenate([up, zero], axis=0)
        down = jnp.concatenate([zero, down], axis=0)
        for step in range(self.half - 1, 0, -1):
            up = self.ahead((joined(step) + up.astype(F32)).astype(BF))
            down = self.back((joined(-step % self.chips) + down.astype(F32)).astype(BF))
        return joined(0) + up.astype(F32) + down.astype(F32)


MESH = pl.DeviceIdType.MESH
DMA = pltpu.SemaphoreType.DMA
VMEM_LIMIT = 60 << 20


class Hops:
    def __init__(self, chips):
        self.chips, self.half = chips, chips // 2
        self.outer = 4 if chips % 4 == 0 else 2
        self.inner = chips // self.outer
        self.me = lax.axis_index("grp")
        chip, self.core = self.me // 2, self.me % 2
        a, b = chip // self.inner, chip % self.inner
        row = self.outer - 1 - a
        along = jnp.where(row % 2 == 0, b - 1, self.inner - 1 - b)
        self.place = jnp.where(b == 0, a, self.outer + row * (self.inner - 1) + along)
        self.ahead, self.back = self.device(1), self.device(-1)
        self.flip = self.me + 1 - 2 * self.core
        self.started = []

    def chip(self, d):
        p = (self.place + (d % self.chips)) % self.chips
        q = jnp.maximum(p - self.outer, 0)
        k, m = q // (self.inner - 1), q % (self.inner - 1)
        b = jnp.where(k % 2 == 0, m + 1, self.inner - 1 - m)
        return jnp.where(
            p < self.outer, p * self.inner, (self.outer - 1 - k) * self.inner + b
        )

    def device(self, d):
        return 2 * self.chip(d) + self.core

    def meet(self, reps=1):
        barrier = pltpu.get_barrier_semaphore()
        for dev in (self.ahead, self.back, self.flip):
            pl.semaphore_signal(barrier, inc=1, device_id={"grp": dev}, device_id_type=MESH)
        rep = lax.axis_index("rep")
        for k in range(1, reps):
            pl.semaphore_signal(
                barrier, inc=1, device_id={"rep": (rep + k) % reps}, device_id_type=MESH
            )
        pl.semaphore_wait(barrier, 2 + reps)

    def copy(self, src, dst, send_sem, recv_sem, dev):
        return pltpu.make_async_remote_copy(
            src_ref=src,
            dst_ref=dst,
            send_sem=send_sem,
            recv_sem=recv_sem,
            device_id={"grp": dev},
            device_id_type=MESH,
        )

    def send(self, src, dst, sems, at, dev):
        c = self.copy(src, dst, sems.at[0, at], sems.at[1, at], dev)
        c.start()
        self.started.append(c)

    def wait(self, dst, sems, at):
        self.copy(dst, dst, sems.at[0, at], sems.at[1, at], self.flip).wait_recv()

    def drain(self):
        for c in self.started:
            c.wait_send()

    def gather(self, items, use):
        half = self.half

        def parts(ref):
            cut = ref.shape[0] // 2
            return ref.at[pl.ds(0, cut)], ref.at[pl.ds(cut, ref.shape[0] - cut)]

        for own, slot, up, down, side in items:
            self.send(own, slot(self.me), up, 0, self.ahead)
            self.send(own, slot(self.me), down, 0, self.back)
            self.send(own, slot(self.me), side, 0, self.flip)
        yield

        def ready(d):
            dev = self.device(d)
            for _, slot, _, _, side in items:
                self.wait(slot(dev + 1 - 2 * self.core), side, d % self.chips)
            use(d)

        ready(0)
        for s in range(1, half):
            last = s == half - 1
            for _, slot, up, down, side in items:
                a, b = slot(self.device(-s)), slot(self.device(s))
                self.wait(a, up, s - 1)
                part = parts(a)[0] if last else a
                self.send(part, part, up, s, self.ahead)
                self.send(a, a, side, -s % self.chips, self.flip)
                self.wait(b, down, s - 1)
                part = parts(b)[1] if last else b
                self.send(part, part, down, s, self.back)
                self.send(b, b, side, s, self.flip)
            for d in (-s, s):
                ready(d)
            yield
        for _, slot, up, down, side in items:
            far = slot(self.device(half))
            low, high = parts(far)
            self.wait(low, up, half - 1)
            self.wait(high, down, half - 1)
            self.send(far, far, side, half, self.flip)
        ready(half)

    def scatter(self, rows, produce, mine, out, came, far, up_in, down_in, up, down, side, finish):
        half, chips = self.half, self.chips
        cut = rows // 2
        strip = 16
        made = {}

        def make(d):
            made[d] = len(made) % mine.shape[0]
            produce(d, mine.at[made[d]], out.at[d % chips])
            self.send(out.at[d % chips], came.at[d % chips], side, d % chips, self.flip)

        def joined(d, at):
            return mine[made[d], at, :] + came[d % chips, at, :].astype(F32)

        def strips(first, last, body):
            def step(i, carry):
                body(pl.ds(pl.multiple_of(first + i * strip, strip), strip))
                return carry

            lax.fori_loop(0, (last - first) // strip, step, 0)

        for d in (half, half - 1):
            make(d)
        self.wait(came.at[half], side, half)

        def far_sum(at):
            far[at, :] = joined(half, at).astype(BF)

        strips(0, rows, far_sum)
        low, high = pl.ds(0, cut), pl.ds(cut, rows - cut)
        self.send(far.at[low], up_in.at[0, low], up, 0, self.ahead)
        self.send(far.at[high], down_in.at[0, high], down, 0, self.back)
        make(1 - half)
        yield
        for s in range(half - 1, 0, -1):
            i = half - s
            for d in sorted({s - 1, 1 - s}):
                make(d)
            for d, buf, sems, target in (
                (s, up_in, up, self.ahead),
                (-s, down_in, down, self.back),
            ):
                self.wait(came.at[d % chips], side, d % chips)

                def fresh(at, d=d, buf=buf, i=i):
                    buf[i - 1, at, :] = joined(d, at).astype(BF)

                def onto(at, d=d, buf=buf, i=i):
                    buf[i - 1, at, :] = (joined(d, at) + buf[i - 1, at, :].astype(F32)).astype(BF)

                if i > 1:
                    self.wait(buf.at[i - 1], sems, i - 1)
                    strips(0, rows, onto)
                elif d > 0:
                    self.wait(buf.at[0, low], sems, 0)
                    strips(0, cut, onto)
                    strips(cut, rows, fresh)
                else:
                    self.wait(buf.at[0, high], sems, 0)
                    strips(0, cut, fresh)
                    strips(cut, rows, onto)
                self.send(buf.at[i - 1], buf.at[i], sems, i, target)
            yield
        self.wait(came.at[0], side, 0)
        self.wait(up_in.at[half - 1], up, half - 1)
        self.wait(down_in.at[half - 1], down, half - 1)

        def total(at):
            finish(
                joined(0, at)
                + up_in[half - 1, at, :].astype(F32)
                + down_in[half - 1, at, :].astype(F32),
                at,
            )

        strips(0, rows, total)

    def turn(self, *rings):
        rings = list(rings)
        while rings:
            rings = [r for r in rings if next(r, self) is not self]
        self.drain()


def scatter_scratch(chips, rows, width):
    half = chips // 2
    return [
        pltpu.VMEM((4, rows, width), F32),
        pltpu.VMEM((chips, rows, width), BF),
        pltpu.VMEM((chips, rows, width), BF),
        pltpu.VMEM((rows, width), BF),
        pltpu.VMEM((half, rows, width), BF),
        pltpu.VMEM((half, rows, width), BF),
    ]


def dot_nt(a, b):
    return lax.dot_general(a, b, (((1,), (1,)), ((), ())), preferred_element_type=F32)


def dot_tn(a, b):
    return lax.dot_general(a, b, (((0,), (0,)), ((), ())), preferred_element_type=F32)


def tiles(count, width, body):
    for i in range(count):
        body(pl.ds(i * width, width))


def experts_kernel(
    chips, cap,
    h2_ref, dy_ref, slot_ref, weight_ref, wg_hbm, wu_hbm, wd_hbm,
    xs_ref, de_ref, act_ref, dg_ref, du_ref,
    held, dy, wg, wu, wd, xs_b, de_b, act_b, dg_b, du_b,
    up, down, side, w_sem, dy_sem, own_sem, out_sem,
):
    hops = Hops(chips)
    half = chips // 2
    tok, width = h2_ref.shape
    ff = wg.shape[1]
    order = [0]
    for s in range(1, half):
        order += [-s, s]
    order += [half]
    number = {d: i for i, d in enumerate(order)}

    loads = [
        pltpu.make_async_copy(a, b, w_sem.at[i])
        for i, (a, b) in enumerate(((wg_hbm, wg), (wu_hbm, wu), (wd_hbm, wd)))
    ]

    def dy_copy(i):
        chip = hops.chip(order[i])
        return pltpu.make_async_copy(dy_ref.at[pl.ds(2 * chip, 2)], dy.at[i % 2], dy_sem.at[i % 2])

    def out_copies(i):
        chip = hops.chip(order[i])
        pairs = ((xs_b, xs_ref), (de_b, de_ref), (act_b, act_ref), (dg_b, dg_ref), (du_b, du_ref))
        return [
            pltpu.make_async_copy(b.at[i % 2], r.at[chip], out_sem.at[i % 2, j])
            for j, (b, r) in enumerate(pairs)
        ]

    hops.meet()
    own = pltpu.make_async_copy(h2_ref, held.at[hops.me], own_sem)
    own.start()

    def use(d):
        i = number[d]
        p = i % 2
        if i == 0:
            own.wait()
            for c in loads:
                c.start()
            dy_copy(0).start()
            for c in loads:
                c.wait()
        dy_copy(i).wait()
        if i + 1 < chips:
            dy_copy(i + 1).start()
        if i >= 2:
            for c in out_copies(i - 2):
                c.wait()
        chip = hops.chip(d)
        for k in range(2):
            dev = 2 * chip + k
            hit = slot_ref[pl.ds(dev, 1), :] == lax.broadcasted_iota(jnp.int32, (cap, tok), 0)
            pick = hit.astype(F32).astype(BF)
            scale = jnp.sum(
                jnp.where(hit, weight_ref[pl.ds(dev, 1), :], 0.0), axis=1, keepdims=True
            )
            rows = pl.ds(k * cap, cap)

            def choose(at, k=k, dev=dev, pick=pick, scale=scale, rows=rows):
                xs_b[p, rows, at] = dot32(pick, held[dev, :, at]).astype(BF)
                de_b[p, rows, at] = (scale * dot32(pick, dy[p, k, :, at])).astype(BF)

            tiles(width // 1024, 1024, choose)

        def hidden(at):
            gpre = dot32(xs_b[p], wg[:, at])
            upre = dot32(xs_b[p], wu[:, at])
            dact = dot_nt(de_b[p], wd[at, :])
            sig = 1.0 / (1.0 + jnp.exp(-gpre))
            act_b[p, :, at] = (gpre * sig * upre).astype(BF)
            dg_b[p, :, at] = (dact * upre * sig * (1.0 + gpre * (1.0 - sig))).astype(BF)
            du_b[p, :, at] = (dact * gpre * sig).astype(BF)

        tiles(ff // 512, 512, hidden)
        for c in out_copies(i):
            c.start()

    hops.turn(hops.gather([(h2_ref, lambda dev: held.at[dev], up, down, side)], use))
    for i in (chips - 2, chips - 1):
        for c in out_copies(i):
            c.wait()


def expert_rows(chips, cap, h2, dy_all, slot, weight, wg, wu, wd, collective_id):
    tok, width = h2.shape
    ff = wg.shape[1]
    anywhere = pl.BlockSpec(memory_space=pl.ANY)
    vmem = pl.BlockSpec(memory_space=pltpu.VMEM)
    wide = jax.ShapeDtypeStruct((chips, 2 * cap, width), BF)
    thin = jax.ShapeDtypeStruct((chips, 2 * cap, ff), BF)
    return pl.pallas_call(
        functools.partial(experts_kernel, chips, cap),
        out_shape=(wide, wide, thin, thin, thin),
        in_specs=[anywhere, anywhere, vmem, vmem, anywhere, anywhere, anywhere],
        out_specs=(anywhere,) * 5,
        scratch_shapes=[
            pltpu.VMEM((2 * chips, tok, width), BF),
            pltpu.VMEM((2, 2, tok, width), BF),
            pltpu.VMEM((width, ff), BF),
            pltpu.VMEM((width, ff), BF),
            pltpu.VMEM((ff, width), BF),
            pltpu.VMEM((2, 2 * cap, width), BF),
            pltpu.VMEM((2, 2 * cap, width), BF),
            pltpu.VMEM((2, 2 * cap, ff), BF),
            pltpu.VMEM((2, 2 * cap, ff), BF),
            pltpu.VMEM((2, 2 * cap, ff), BF),
            *ring_sems(chips),
            DMA((3,)),
            DMA((2,)),
            DMA,
            DMA((2, 5)),
        ],
        compiler_params=pltpu.CompilerParams(
            collective_id=collective_id, has_side_effects=True, vmem_limit_bytes=VMEM_LIMIT
        ),
        cost_estimate=pl.CostEstimate(
            flops=2 * chips * cap * width * ff * 6, transcendentals=0, bytes_accessed=200 << 20
        ),
        name="experts",
    )(h2, dy_all, slot, weight, wg, wu, wd)


def column_of(table, dev):
    lanes = lax.broadcasted_iota(jnp.int32, table.shape, 1)
    return jnp.sum(jnp.where(lanes == dev, table[...], 0.0), axis=1, keepdims=True)


def returned(hops, d, cap, tok, slot_ref, rows_ref, same_ref, other_ref, weight_ref=None):
    chip = hops.chip(d)
    lanes = lax.broadcasted_iota(jnp.int32, (tok, cap), 1).astype(F32)
    for k, ref in ((hops.core, same_ref), (1 - hops.core, other_ref)):
        pick = (column_of(slot_ref, 2 * chip + k) == lanes).astype(F32).astype(BF)
        rows = pl.ds(pl.multiple_of(k * cap, 16), cap)
        weight = None if weight_ref is None else column_of(weight_ref, 2 * chip + k)

        def spread(at, pick=pick, rows=rows, ref=ref, weight=weight):
            value = dot32(pick, rows_ref[rows, at])
            if weight is not None:
                value = weight * value
            ref[:, at] = value.astype(ref.dtype)

        tiles(rows_ref.shape[1] // 1024, 1024, spread)


def scatter_order(half):
    order = [half, half - 1, 1 - half]
    for s in range(half - 2, 0, -1):
        order += [-s, s]
    return order + [0]


def outputs_kernel(
    chips, cap,
    act_ref, xs_ref, de_ref, dg_ref, du_ref, slot_ref, weight_ref, wd_hbm,
    total_ref, down_ref, came_ref, gate_ref, up_ref,
    wd, left, right, made_d, made, act, rows_b, mine, out, came, far, up_in, down_in,
    up, down, side, w_sem, act_sem, left_sem, right_sem, made_sem, down_sem, rep_sem,
):
    hops = Hops(chips)
    replica = lax.axis_index("rep")
    tok, width = total_ref.shape
    order = scatter_order(chips // 2)
    number = {d: i for i, d in enumerate(order)}
    strip = right.shape[2]
    count = width // strip

    def act_copy(i):
        rows = pl.ds(pl.multiple_of(hops.chip(order[i]) * (2 * cap), 2 * cap), 2 * cap)
        return pltpu.make_async_copy(act_ref.at[rows], act.at[i % 2], act_sem.at[i % 2])

    jobs = [
        (thin, wide, result, i)
        for thin, wide, result in (
            (act_ref, de_ref, down_ref),
            (dg_ref, xs_ref, gate_ref),
            (du_ref, xs_ref, up_ref),
        )
        for i in range(count)
    ]
    done, stored, sent = [], {}, []

    def right_copy(n):
        at = pl.ds(jobs[n][3] * strip, strip)
        return pltpu.make_async_copy(jobs[n][1].at[:, at], right.at[n % 2], right_sem.at[n % 2])

    def left_copy(n):
        return pltpu.make_async_copy(jobs[n][0], left, left_sem)

    def job():
        n = len(done)
        if n == len(jobs):
            return
        done.append(n)
        _, _, result, i = jobs[n]
        if i == 0:
            left_copy(n).wait()
        right_copy(n).wait()
        if n + 1 < len(jobs):
            right_copy(n + 1).start()
        at = pl.ds(i * strip, strip)
        if n < count:
            made_d[i] = dot_tn(left[...], right[n % 2]).astype(BF)
            stored[n] = pltpu.make_async_copy(made_d.at[i], result.at[:, at], down_sem.at[i])
            c = pltpu.make_async_remote_copy(
                src_ref=made_d.at[i],
                dst_ref=came_ref.at[:, at],
                send_sem=rep_sem.at[0, i],
                recv_sem=rep_sem.at[1, i],
                device_id={"rep": 1 - replica},
                device_id_type=MESH,
            )
            c.start()
            sent.append(c)
        else:
            if n - 2 >= count:
                stored.pop(n - 2).wait()
            made[n % 2] = dot_tn(right[n % 2], left[...]).astype(BF)
            stored[n] = pltpu.make_async_copy(made.at[n % 2], result.at[at, :], made_sem.at[n % 2])
        stored[n].start()
        if i == count - 1 and n + 1 < len(jobs):
            left_copy(n + 1).start()

    def produce(d, same_ref, other_ref):
        i = number[d]
        act_copy(i).wait()
        if i + 1 < chips:
            act_copy(i + 1).start()

        def last(at):
            rows_b[:, at] = dot32(act[i % 2], wd[:, at]).astype(BF)

        tiles(width // 512, 512, last)
        returned(hops, d, cap, tok, slot_ref, rows_b, same_ref, other_ref, weight_ref)

    def finish(value, at):
        total_ref[at, :] = value

    load = pltpu.make_async_copy(wd_hbm, wd, w_sem)
    left_copy(0).start()
    right_copy(0).start()
    act_copy(0).start()
    load.start()
    hops.meet(2)
    ring = hops.scatter(tok, produce, mine, out, came, far, up_in, down_in, up, down, side, finish)
    job()
    load.wait()
    share = -(-(len(jobs) - 2) // (chips // 2 - 1))
    for step in range(chips // 2):
        next(ring)
        for _ in range(share if step else 1):
            job()
    hops.turn(ring)
    for c in stored.values():
        c.wait()
    for c in sent:
        c.wait()


def outputs(chips, cap, act, xs, de, dg, du, slot_t, weight_t, wd, collective_id):
    ff, width = wd.shape
    tok = slot_t.shape[0]
    strip = 512
    anywhere = pl.BlockSpec(memory_space=pl.ANY)
    vmem = pl.BlockSpec(memory_space=pltpu.VMEM)
    tall, flat = jax.ShapeDtypeStruct((width, ff), BF), jax.ShapeDtypeStruct((ff, width), BF)
    return pl.pallas_call(
        functools.partial(outputs_kernel, chips, cap),
        out_shape=(jax.ShapeDtypeStruct((tok, width), F32), flat, flat, tall, tall),
        in_specs=[anywhere] * 5 + [vmem] * 2 + [anywhere],
        out_specs=(vmem,) + (anywhere,) * 4,
        scratch_shapes=[
            pltpu.VMEM((ff, width), BF),
            pltpu.VMEM((2 * chips * cap, ff), BF),
            pltpu.VMEM((2, 2 * chips * cap, strip), BF),
            pltpu.VMEM((width // strip, ff, strip), BF),
            pltpu.VMEM((2, strip, ff), BF),
            pltpu.VMEM((2, 2 * cap, ff), BF),
            pltpu.VMEM((2 * cap, width), BF),
            *scatter_scratch(chips, tok, width),
            *ring_sems(chips),
            DMA,
            DMA((2,)),
            DMA,
            DMA((2,)),
            DMA((2,)),
            DMA((width // strip,)),
            DMA((2, width // strip)),
        ],
        compiler_params=pltpu.CompilerParams(
            collective_id=collective_id, has_side_effects=True, vmem_limit_bytes=63 << 20
        ),
        cost_estimate=pl.CostEstimate(
            flops=2 * 2 * chips * cap * width * ff * 4, transcendentals=0, bytes_accessed=200 << 20
        ),
        name="outputs",
    )(act, xs, de, dg, du, slot_t, weight_t, wd)


def rows_back_kernel(
    chips, cap,
    dg_ref, du_ref, slot_ref, wg_hbm, wu_hbm, total_ref,
    wg, wu, dg, du, drow, mine, out, came, far, up_in, down_in,
    up, down, side, w_sem, in_sem,
):
    hops = Hops(chips)
    tok, width = total_ref.shape
    order = scatter_order(chips // 2)
    number = {d: i for i, d in enumerate(order)}
    loads = [
        pltpu.make_async_copy(a, b, w_sem.at[i])
        for i, (a, b) in enumerate(((wg_hbm, wg), (wu_hbm, wu)))
    ]

    def in_copies(i):
        chip = hops.chip(order[i])
        return [
            pltpu.make_async_copy(r.at[chip], b.at[i % 2], in_sem.at[i % 2, j])
            for j, (r, b) in enumerate(((dg_ref, dg), (du_ref, du)))
        ]

    for c in loads + in_copies(0):
        c.start()
    hops.meet()
    for c in loads:
        c.wait()

    def produce(d, same_ref, other_ref):
        i = number[d]
        p = i % 2
        for c in in_copies(i):
            c.wait()
        if i + 1 < chips:
            for c in in_copies(i + 1):
                c.start()

        def back(at):
            drow[:, at] = (dot_nt(dg[p], wg[at, :]) + dot_nt(du[p], wu[at, :])).astype(BF)

        tiles(width // 512, 512, back)
        returned(hops, d, cap, tok, slot_ref, drow, same_ref, other_ref)

    def finish(value, at):
        total_ref[at, :] = value

    hops.turn(
        hops.scatter(tok, produce, mine, out, came, far, up_in, down_in, up, down, side, finish)
    )


def rows_back(chips, cap, dg, du, slot, wg, wu, collective_id):
    tok = slot.shape[0]
    width, ff = wg.shape
    anywhere = pl.BlockSpec(memory_space=pl.ANY)
    vmem = pl.BlockSpec(memory_space=pltpu.VMEM)
    return pl.pallas_call(
        functools.partial(rows_back_kernel, chips, cap),
        out_shape=jax.ShapeDtypeStruct((tok, width), F32),
        in_specs=[anywhere, anywhere, vmem, anywhere, anywhere],
        out_specs=vmem,
        scratch_shapes=[
            pltpu.VMEM((width, ff), BF),
            pltpu.VMEM((width, ff), BF),
            pltpu.VMEM((2, 2 * cap, ff), BF),
            pltpu.VMEM((2, 2 * cap, ff), BF),
            pltpu.VMEM((2 * cap, width), BF),
            *scatter_scratch(chips, tok, width),
            *ring_sems(chips),
            DMA((2,)),
            DMA((2, 2)),
        ],
        compiler_params=pltpu.CompilerParams(
            collective_id=collective_id, has_side_effects=True, vmem_limit_bytes=VMEM_LIMIT
        ),
        cost_estimate=pl.CostEstimate(
            flops=2 * chips * cap * width * ff * 6, transcendentals=0, bytes_accessed=200 << 20
        ),
        name="rows_back",
    )(dg, du, slot, wg, wu)


def turned(v, cosine, sine):
    return v * cosine + pltpu.roll(v, HD // 2, 1) * sine


def head_of(proj, at, gain, cosine, sine):
    value = proj[:, at]
    inverse = lax.rsqrt(jnp.mean(value * value, axis=-1, keepdims=True) + epsilon)
    hat = value * inverse
    return hat, inverse, turned(hat * gain, cosine, sine).astype(BF)


def softmax_rows(queries, keys, docs_q, docs_k):
    raw = dot_nt(queries, keys) * HD ** (-0.5)
    raw = jnp.where(docs_q == docs_k, raw, -1e30)
    grown = jnp.exp(raw - jnp.max(raw, axis=-1, keepdims=True))
    return grown * (1.0 / jnp.sum(grown, axis=-1, keepdims=True))


def columns_of(block, head, heads):
    return pl.ds(pl.multiple_of((block * heads + head) * HD, HD), HD)


def attention_kernel(
    chips, reps, heads,
    cot_ref, seq_ref, ga_ref, gf_ref, gq_ref, gk_ref, cos_ref, sin_ref, dc_ref, dr_ref, wq_hbm, wo_hbm,
    dy_ref, h1_out, proj_out, ob_out, mid_ref, h2_ref,
    wq, wo, give, came, h1_ref, proj_ref, ob_ref, up, down, side, rep_sem, own_sem, out_sem,
):
    hops = Hops(chips)
    rep = lax.axis_index("rep")
    seq_len, width = seq_ref.shape
    tok = mid_ref.shape[0]
    block = min(256, seq_len)
    loads = [
        pltpu.make_async_copy(a, b, own_sem.at[i])
        for i, (a, b) in enumerate(((wq_hbm, wq), (wo_hbm, wo), (cot_ref, dy_ref.at[hops.me])))
    ]
    hops.meet(reps)
    ring = hops.gather([(cot_ref, lambda dev: dy_ref.at[dev], up, down, side)], lambda d: None)
    next(ring)
    for c in loads:
        c.start()

    def normed(i, carry):
        rows = pl.ds(pl.multiple_of(i * 64, 64), 64)
        v = seq_ref[rows, :].astype(F32)
        v = v * lax.rsqrt(jnp.mean(v * v, axis=-1, keepdims=True) + epsilon)
        h1_ref[rows, :] = (v * ga_ref[...]).astype(BF)
        return carry

    lax.fori_loop(0, seq_len // 64, normed, 0)
    loads[0].wait()
    total = 3 * heads * HD
    step = 512 if total % 512 == 0 else HD
    for i in range(total // step):
        at = pl.ds(i * step, step)
        proj_ref[:, at] = dot32(h1_ref[...], wq[:, at])

    stores = [
        pltpu.make_async_copy(a, b, out_sem.at[i])
        for i, (a, b) in enumerate(((h1_ref, h1_out), (proj_ref, proj_out), (ob_ref, ob_out)))
    ]
    stores[0].start()
    stores[1].start()

    def one(head, carry):
        _, _, q_b = head_of(
            proj_ref, columns_of(0, head, heads), gq_ref[...], cos_ref[...], sin_ref[...]
        )
        _, _, k_b = head_of(
            proj_ref, columns_of(1, head, heads), gk_ref[...], cos_ref[...], sin_ref[...]
        )
        v_b = proj_ref[:, columns_of(2, head, heads)].astype(BF)
        for i in range(seq_len // block):
            rows = slice(i * block, (i + 1) * block)
            probs = softmax_rows(q_b[rows], k_b, dc_ref[rows, :], dr_ref[...])
            ob_ref[rows, columns_of(0, head, heads)] = dot32(probs.astype(BF), v_b).astype(BF)
        return carry

    lax.fori_loop(0, heads // 2, one, 0)
    next(ring)
    lax.fori_loop(heads // 2, heads, one, 0)
    stores[2].start()
    loads[1].wait()
    swaps = []
    for k in range(1, reps):
        for i in range(width // 512):
            at = pl.ds(i * 512, 512)
            give[k - 1, :, at] = dot32(ob_ref[pl.ds(k * tok, tok), :], wo[:, at]).astype(BF)
        c = pltpu.make_async_remote_copy(
            src_ref=give.at[k - 1],
            dst_ref=came.at[k - 1],
            send_sem=rep_sem.at[0, k - 1],
            recv_sem=rep_sem.at[1, k - 1],
            device_id={"rep": (rep + k) % reps},
            device_id_type=MESH,
        )
        c.start()
        swaps.append(c)
    for i in range(width // 512):
        at = pl.ds(i * 512, 512)
        mid_ref[:, at] = dot32(ob_ref[pl.ds(0, tok), :], wo[:, at])
    next(ring)
    for c in swaps:
        c.wait()

    def second(i, carry):
        rows = pl.ds(pl.multiple_of(i * 64, 64), 64)
        v = seq_ref[rows, :].astype(F32) + mid_ref[rows, :]
        for k in range(1, reps):
            v = v + came[k - 1, rows, :].astype(F32)
        mid_ref[rows, :] = v
        v = v * lax.rsqrt(jnp.mean(v * v, axis=-1, keepdims=True) + epsilon)
        h2_ref[rows, :] = (v * gf_ref[...]).astype(BF)
        return carry

    lax.fori_loop(0, tok // 64, second, 0)
    loads[2].wait()
    hops.turn(ring)
    for c in stores:
        c.wait()


def attention(chips, reps, cot, seq, ga, gf, gq, gk, cosine, sine, docs, w_qkv, w_out, collective_id):
    seq_len, width = seq.shape
    tok = cot.shape[0]
    heads = w_out.shape[0] // HD
    anywhere = pl.BlockSpec(memory_space=pl.ANY)
    vmem = pl.BlockSpec(memory_space=pltpu.VMEM)
    return pl.pallas_call(
        functools.partial(attention_kernel, chips, reps, heads),
        out_shape=(
            jax.ShapeDtypeStruct((2 * chips, tok, width), BF),
            jax.ShapeDtypeStruct((seq_len, width), BF),
            jax.ShapeDtypeStruct((seq_len, 3 * heads * HD), F32),
            jax.ShapeDtypeStruct((seq_len, heads * HD), BF),
            jax.ShapeDtypeStruct((tok, width), F32),
            jax.ShapeDtypeStruct((tok, width), BF),
        ),
        in_specs=[anywhere] + [vmem] * 9 + [anywhere] * 2,
        out_specs=(anywhere,) * 4 + (vmem,) * 2,
        scratch_shapes=[
            pltpu.VMEM(w_qkv.shape, BF),
            pltpu.VMEM(w_out.shape, BF),
            pltpu.VMEM((reps - 1, tok, width), BF),
            pltpu.VMEM((reps - 1, tok, width), BF),
            pltpu.VMEM((seq_len, width), BF),
            pltpu.VMEM((seq_len, 3 * heads * HD), F32),
            pltpu.VMEM((seq_len, heads * HD), BF),
            *ring_sems(chips),
            DMA((2, reps - 1)),
            DMA((3,)),
            DMA((3,)),
        ],
        compiler_params=pltpu.CompilerParams(
            collective_id=collective_id, has_side_effects=True, vmem_limit_bytes=VMEM_LIMIT
        ),
        cost_estimate=pl.CostEstimate(
            flops=2 * seq_len * w_qkv.size, transcendentals=0, bytes_accessed=100 << 20
        ),
        name="attention",
    )(cot, seq, ga, gf, gq, gk, cosine, sine, docs[:, None], docs[None, :], w_qkv, w_out)


def attention_back_kernel(
    heads,
    proj_ref, mid_ref, wo_ref, seq_ref, gq_ref, gk_ref, cos_ref, sin_ref, dc_ref, dr_ref, wq_hbm,
    grad_ref, qt_ref, kt_ref, own_ref, rest_ref, at_ref,
    dob, dk, dv, wq, scale_b, w_sem,
):
    seq_len = proj_ref.shape[0]
    load = pltpu.make_async_copy(wq_hbm, wq, w_sem)
    load.start()
    block = min(256, seq_len)
    scale = HD ** (-0.5)
    for i in range(heads * HD // 512):
        at = pl.ds(i * 512, 512)
        dob[:, at] = dot_nt(mid_ref[...], wo_ref[at, :]).astype(BF)
    qt_ref[...] = jnp.zeros_like(qt_ref)
    kt_ref[...] = jnp.zeros_like(kt_ref)

    def unturned(grad, hat, inverse, gain, rows):
        grad = turned(grad, cos_ref[rows, :], -sin_ref[rows, :])
        scaled = grad * gain
        pre = inverse * (scaled - hat * jnp.mean(scaled * hat, axis=-1, keepdims=True))
        return pre.astype(BF), jnp.sum(grad * hat, axis=0, keepdims=True)

    def one(head, carry):
        q_at, k_at, v_at = (columns_of(b, head, heads) for b in range(3))
        q_hat, q_inv, q_b = head_of(proj_ref, q_at, gq_ref[...], cos_ref[...], sin_ref[...])
        k_hat, k_inv, k_b = head_of(proj_ref, k_at, gk_ref[...], cos_ref[...], sin_ref[...])
        v_b = proj_ref[:, v_at].astype(BF)
        for i in range(seq_len // block):
            rows = slice(i * block, (i + 1) * block)
            probs = softmax_rows(q_b[rows], k_b, dc_ref[rows, :], dr_ref[...])
            grad_o = dob[rows, columns_of(0, head, heads)]
            grad_p = dot_nt(grad_o, v_b)
            grad_s = (
                probs * (grad_p - jnp.sum(probs * grad_p, axis=-1, keepdims=True))
            ).astype(BF)
            dv_part = dot_tn(probs.astype(BF), grad_o)
            dk_part = dot_tn(grad_s, q_b[rows])
            if i == 0:
                dv[...] = dv_part
                dk[...] = dk_part
            else:
                dv[...] += dv_part
                dk[...] += dk_part
            pre, terms = unturned(
                dot32(grad_s, k_b) * scale, q_hat[rows], q_inv[rows], gq_ref[...], rows
            )
            grad_ref[rows, q_at] = pre
            qt_ref[...] += terms
        pre, terms = unturned(dk[...] * scale, k_hat, k_inv, gk_ref[...], slice(0, seq_len))
        grad_ref[:, k_at] = pre
        kt_ref[...] += terms
        grad_ref[:, v_at] = dv[...].astype(BF)
        return carry

    lax.fori_loop(0, heads, one, 0)

    tok = own_ref.shape[0]

    def inverses(i, carry):
        rows = pl.ds(pl.multiple_of(i * 64, 64), 64)
        v = seq_ref[rows, :].astype(F32)
        scale_b[rows, :] = lax.rsqrt(jnp.mean(v * v, axis=-1, keepdims=True) + epsilon)
        return carry

    lax.fori_loop(0, seq_len // 64, inverses, 0)
    load.wait()
    for i in range(wq.shape[0] // 256):
        at = pl.ds(i * 256, 256)
        part = dot_nt(grad_ref[...], wq[at, :])
        own_ref[:, at] = part[:tok]
        rest_ref[:, at] = part[tok:].astype(BF)
        hat = seq_ref[:, at].astype(F32) * scale_b[...]
        at_ref[:, at] = jnp.sum(part * hat, axis=0, keepdims=True)


def attention_back(tok, proj, mid, w_out, seq, gq, gk, cosine, sine, docs, w_qkv):
    seq_len = proj.shape[0]
    heads = w_out.shape[0] // HD
    vmem = pl.BlockSpec(memory_space=pltpu.VMEM)
    return pl.pallas_call(
        functools.partial(attention_back_kernel, heads),
        out_shape=(
            jax.ShapeDtypeStruct(proj.shape, BF),
            jax.ShapeDtypeStruct((1, HD), F32),
            jax.ShapeDtypeStruct((1, HD), F32),
            jax.ShapeDtypeStruct((tok, D), F32),
            jax.ShapeDtypeStruct((seq_len - tok, D), BF),
            jax.ShapeDtypeStruct((1, D), F32),
        ),
        in_specs=[vmem] * 10 + [pl.BlockSpec(memory_space=pl.ANY)],
        out_specs=(vmem,) * 6,
        scratch_shapes=[
            pltpu.VMEM((seq_len, heads * HD), BF),
            pltpu.VMEM((seq_len, HD), F32),
            pltpu.VMEM((seq_len, HD), F32),
            pltpu.VMEM(w_qkv.shape, BF),
            pltpu.VMEM((seq_len, 1), F32),
            DMA,
        ],
        compiler_params=pltpu.CompilerParams(vmem_limit_bytes=VMEM_LIMIT),
        cost_estimate=pl.CostEstimate(
            flops=20 * heads * seq_len * seq_len * HD, transcendentals=0, bytes_accessed=20 << 20
        ),
        name="attention_back",
    )(proj, mid, w_out, seq, gq, gk, cosine, sine, docs[:, None], docs[None, :], w_qkv)


def ring_sems(chips):
    return [DMA((2, chips // 2)), DMA((2, chips // 2)), DMA((2, chips))]


def dense_gradients_kernel(
    chips, split_out, h1_ref, grad_ref, ob_ref, mid_ref, gains_ref, qkv_ref, out_ref, gain_ref, *scratch
):
    hops = Hops(chips)
    scratches = [scratch[9 * i : 9 * i + 9] for i in range(4)]
    hops.meet(2 if split_out else 1)
    first = hops.core == 0
    if split_out:
        q_sum, q_came, o_sum, o_came, o_give, o_got, g_sum, g_came, rep_sem, flip_sem = scratch[36:]
    else:
        q_sum, o_sum, g_sum = qkv_ref, out_ref, gain_ref

    def product(left_ref, right_ref, rows, width):
        step = 512 if width % 512 == 0 else 256

        def produce(d, same_ref, other_ref):
            columns = pl.ds(pl.multiple_of(2 * rows * hops.chip(d), 2 * rows), 2 * rows)
            left = left_ref[:, columns]

            def block(at):
                value = dot_tn(left, right_ref[:, at])
                low, high = value[:rows], value[rows:]
                same_ref[:, at] = jnp.where(first, low, high)
                other_ref[:, at] = jnp.where(first, high, low).astype(BF)

            tiles(width // step, step, block)

        return produce

    def small(d, same_ref, other_ref):
        dev = hops.device(d)
        same_ref[...] = gains_ref[dev]
        other_ref[...] = gains_ref[dev + 1 - 2 * hops.core].astype(BF)

    def into(ref):
        def finish(value, at):
            ref[at, :] = value.astype(ref.dtype)

        return finish

    def ring(produce, ref, bufs):
        return hops.scatter(ref.shape[0], produce, *bufs, into(ref))

    shard, wide = q_sum.shape
    replica = lax.axis_index("rep")
    halves = [pl.ds(0, wide // 2), pl.ds(wide // 2, wide // 2)]
    if split_out:
        pairs = [(o_sum, o_came), *((q_sum.at[:, h], q_came.at[:, h]) for h in halves), (g_sum, g_came)]
        swaps = [
            pltpu.make_async_remote_copy(
                src_ref=src,
                dst_ref=dst,
                send_sem=rep_sem.at[0, i],
                recv_sem=rep_sem.at[1, i],
                device_id={"rep": 1 - replica},
                device_id_type=MESH,
            )
            for i, (src, dst) in enumerate(pairs)
        ]

    def then_swap(ring_steps, i):
        yield from ring_steps
        if split_out:
            swaps[i].start()

    rings = []
    if split_out:
        steps = ring(product(ob_ref, mid_ref, *o_sum.shape), o_sum, scratches[2])
        rings.append(then_swap(steps, 0))
    for i, h in enumerate(halves):
        part = product(h1_ref, grad_ref.at[:, h], shard, wide // 2)
        rings.append(then_swap(ring(part, q_sum.at[:, h], scratches[i]), 1 + i))
    rings.append(then_swap(ring(small, g_sum, scratches[3]), 3))
    hops.turn(*rings)
    if not split_out:
        return

    mine = hops.core == replica
    swaps[0].wait()
    o_give[...] = jnp.where(mine, o_came[...], o_sum[...])
    give = hops.copy(o_give, o_got, flip_sem.at[0], flip_sem.at[1], hops.flip)
    give.start()
    keep = jnp.where(mine, o_sum[...], o_came[...])
    even = replica == 0
    for i in range(wide // HD):
        if i * HD == 0 or i * HD == wide // 2:
            swaps[1 + (i > 0)].wait()
        own, came = q_sum[:, pl.ds(i * HD, HD)], q_came[:, pl.ds(i * HD, HD)]
        qkv_ref[:, pl.ds(2 * i * HD, HD)] = jnp.where(even, own, came).astype(F32)
        qkv_ref[:, pl.ds((2 * i + 1) * HD, HD)] = jnp.where(even, came, own).astype(F32)
    swaps[3].wait()
    gain_ref[...] = g_sum[...] + g_came[...]
    give.wait()
    half = o_sum.shape[0]
    got = o_got[...]
    out_ref[pl.ds(0, half), :] = jnp.where(first, keep, got).astype(F32)
    out_ref[pl.ds(half, half), :] = jnp.where(first, got, keep).astype(F32)


def dense_gradients(chips, split_out, h1, grad, ob, mid, gain_blocks, collective_id):
    shard = h1.shape[1] // (2 * chips)
    width = grad.shape[1]
    half = ob.shape[1] // (2 * chips) if split_out else 32
    vmem = pl.BlockSpec(memory_space=pltpu.VMEM)
    shapes = ((shard, width), (half, D), gain_blocks.shape[1:])
    scratch = []
    for rows, columns in ((shard, width // 2), (shard, width // 2), *shapes[1:]):
        scratch += [*scatter_scratch(chips, rows, columns), *ring_sems(chips)]
    if split_out:
        scratch += [pltpu.VMEM(shapes[0], BF)] * 2 + [pltpu.VMEM(shapes[1], BF)] * 4
        scratch += [pltpu.VMEM(shapes[2], F32)] * 2 + [DMA((2, 4)), DMA((2,))]
        shapes = ((shard, 2 * width), (2 * half, D), shapes[2])
    kinds = (F32, F32, F32) if split_out else (BF, BF, F32)
    return pl.pallas_call(
        functools.partial(dense_gradients_kernel, chips, split_out),
        out_shape=tuple(
            jax.ShapeDtypeStruct(shape, kind) for shape, kind in zip(shapes, kinds, strict=True)
        ),
        in_specs=[vmem] * 5,
        out_specs=(vmem,) * 3,
        scratch_shapes=scratch,
        compiler_params=pltpu.CompilerParams(
            collective_id=collective_id, has_side_effects=True, vmem_limit_bytes=VMEM_LIMIT
        ),
        cost_estimate=pl.CostEstimate(
            flops=2 * h1.size * width, transcendentals=0, bytes_accessed=200 << 20
        ),
        name="dense_gradients",
    )(h1, grad, ob, mid, gain_blocks)


def start_kernel(
    chips, reps, heads, split_out,
    tok_ref, small_ref, wq_ref, wo_ref,
    seq_ref, smalls_ref, full_ref, out_ref,
    own_q, own_o, *sems,
):
    hops = Hops(chips)
    rep = lax.axis_index("rep")
    up, down, side, up_s, down_s, side_s, up_o, down_o, side_o, rep_sem, col_sem, own_sem, half_sem = sems
    pieces = []
    for i in range(3 * heads):
        q, j = i // heads, i % heads
        at = pl.multiple_of(((q * heads + j) * reps + rep) * HD, HD)
        pieces.append(
            pltpu.make_async_copy(
                wq_ref.at[:, pl.ds(at, HD)], own_q.at[:, pl.ds(i * HD, HD)], col_sem.at[i]
            )
        )
        pieces[-1].start()
    hops.meet(reps)
    swaps = []
    for k in range(1, reps):
        c = pltpu.make_async_remote_copy(
            src_ref=tok_ref,
            dst_ref=seq_ref.at[reps - k],
            send_sem=rep_sem.at[0, reps - k],
            recv_sem=rep_sem.at[1, reps - k],
            device_id={"rep": (rep + k) % reps},
            device_id_type=MESH,
        )
        c.start()
        swaps.append(c)
    locals_ = [
        pltpu.make_async_copy(tok_ref, seq_ref.at[0], own_sem.at[0]),
        pltpu.make_async_copy(small_ref, smalls_ref.at[hops.me], own_sem.at[1]),
    ]
    for c in locals_:
        c.start()
    for c in pieces:
        c.wait()
    mine = pltpu.make_async_copy(own_q, full_ref.at[hops.me], own_sem.at[2])
    mine.start()
    items = [
        (own_q, lambda dev: full_ref.at[dev], up, down, side),
        (small_ref, lambda dev: smalls_ref.at[dev], up_s, down_s, side_s),
    ]
    if split_out:
        rows = own_o.shape[0]
        kept = wo_ref.at[pl.ds(pl.multiple_of(hops.core * rows, rows), rows)]
        given = wo_ref.at[pl.ds(pl.multiple_of((1 - hops.core) * rows, rows), rows)]
        give = hops.copy(given, own_o, half_sem.at[0], half_sem.at[1], hops.flip)

        @pl.when(hops.core == rep)
        def _():
            give.start()
            keep = pltpu.make_async_copy(kept, own_o, half_sem.at[2])
            keep.start()
            keep.wait()
            give.wait_send()

        @pl.when(hops.core != rep)
        def _():
            give.wait_recv()

        def slot(dev):
            return out_ref.at[dev // 2, pl.ds(pl.multiple_of(dev % 2 * rows, rows), rows)]

        mine_o = pltpu.make_async_copy(own_o, slot(hops.me), half_sem.at[3])
        mine_o.start()
        items.append((own_o, slot, up_o, down_o, side_o))
    hops.turn(hops.gather(items, lambda d: None))
    for c in locals_:
        c.wait()
    mine.wait()
    if split_out:
        mine_o.wait()
    for c in swaps:
        c.wait()


def start(chips, reps, heads, split_out, tok, small, w_qkv, w_out, collective_id):
    anywhere = pl.BlockSpec(memory_space=pl.ANY)
    vmem = pl.BlockSpec(memory_space=pltpu.VMEM)
    shard, wide = w_qkv.shape[0], 3 * heads * HD
    half = w_out.shape[0] // 2
    return pl.pallas_call(
        functools.partial(start_kernel, chips, reps, heads, split_out),
        out_shape=(
            jax.ShapeDtypeStruct((reps, *tok.shape), BF),
            jax.ShapeDtypeStruct((2 * chips, *small.shape), F32),
            jax.ShapeDtypeStruct((2 * chips, shard, wide), BF),
            jax.ShapeDtypeStruct((chips, 2 * half, D), BF),
        ),
        in_specs=[vmem, vmem, anywhere, anywhere],
        out_specs=(anywhere,) * 4,
        scratch_shapes=[
            pltpu.VMEM((shard, wide), BF),
            pltpu.VMEM((half, D), BF),
            *ring_sems(chips),
            *ring_sems(chips),
            *ring_sems(chips),
            DMA((2, max(reps, 2))),
            DMA((3 * heads,)),
            DMA((3,)),
            DMA((4,)),
        ],
        compiler_params=pltpu.CompilerParams(collective_id=collective_id, has_side_effects=True),
        cost_estimate=pl.CostEstimate(
            flops=0, transcendentals=0, bytes_accessed=200 << 20
        ),
        name="start",
    )(tok, small, w_qkv, w_out)


def per_device(
    tokens, w_qkv, w_out, gains, w_gate, w_up, w_down, segment_ids, routes, gate_weights, cotangent
):
    groups = lax.axis_size("grp")
    reps = lax.axis_size("rep")
    ring = Ring(groups)
    rep, grp = lax.axis_index("rep"), lax.axis_index("grp")
    rel = jnp.asarray(ring.table())[grp]
    tok_rows = tokens.shape[1]
    seq_len = segment_ids.shape[1]
    heads = HEADS // reps
    wide = heads * HD

    def from_rep(v, k):
        return lax.ppermute(v, "rep", [((s + k) % reps, s) for s in range(reps)])

    def to_rep(v, k):
        return lax.ppermute(v, "rep", [(s, (s + k) % reps) for s in range(reps)])

    def rep_gather(v):
        return jnp.concatenate([v] + [from_rep(v, k) for k in range(1, reps)], axis=0)

    own_b = tokens[0]
    gates_f = gate_weights[0]
    experts = jnp.arange(groups, dtype=jnp.int32)
    weight_of = jnp.sum(
        jnp.where(routes[0][None] == experts[:, None, None], gates_f[None], 0.0), axis=-1
    )
    gain_rows = -(-gains.shape[0] // tok_rows)
    small_rows = -(-(groups + gain_rows) // 16) * 16
    small = jnp.concatenate(
        [
            weight_of,
            jnp.pad(gains.astype(F32), (0, gain_rows * tok_rows - gains.shape[0])).reshape(
                gain_rows, tok_rows
            ),
            jnp.zeros((small_rows - groups - gain_rows, tok_rows), F32),
        ],
        axis=0,
    )
    split_out = reps == 2 and heads == ring.chips
    seq_b, smalls, full_qkv, my_out = start(
        ring.chips, reps, heads, split_out, own_b, small, w_qkv, w_out, 1
    )
    seq_b = seq_b.reshape(seq_len, D)
    shard = full_qkv.shape[1]
    full_qkv = full_qkv.reshape(D, 3 * wide)
    if not split_out:
        my_out = lax.all_gather(w_out, "grp", axis=0, tiled=True)
        my_out = lax.dynamic_index_in_dim(
            my_out.reshape(heads, reps, HD, D), rep, axis=1, keepdims=False
        )
    my_out = my_out.reshape(wide, D)
    gains_f = smalls[:, groups : groups + gain_rows].reshape(groups, -1)
    gains_f = gains_f[:, : gains.shape[0]].reshape(-1)
    weight_in = lax.dynamic_index_in_dim(smalls, grp, 1, False)
    g_attn = gains_f[:D]
    g_ffn = gains_f[D : 2 * D]
    g_query = gains_f[2 * D : 2 * D + HD]
    g_key = gains_f[2 * D + HD :]

    def this_first(table):
        return lax.dynamic_slice_in_dim(
            jnp.concatenate([table, table], axis=0), rep * tok_rows, seq_len, axis=0
        )

    frequency = np.float32(rope_base) ** (-2.0 * np.arange(HD // 2, dtype=np.float32) / HD)
    angles = np.arange(seq_len, dtype=np.float32)[:, None] * frequency.astype(np.float32)[None, :]
    cosine = this_first(jnp.asarray(np.concatenate([np.cos(angles)] * 2, axis=1)))
    sine = this_first(jnp.asarray(np.concatenate([-np.sin(angles), np.sin(angles)], axis=1)))
    docs = this_first(segment_ids[0])
    g_query, g_key = g_query[None], g_key[None]
    dy_all, h1_b, projected, attended_b, mid_rows, h2_b = attention(
        ring.chips,
        reps,
        cotangent[0],
        seq_b,
        g_attn[None],
        g_ffn[None],
        g_query,
        g_key,
        cosine,
        sine,
        docs,
        full_qkv,
        my_out,
        5,
    )

    chips = ring.chips
    entries = tok_rows * TOP
    capacity = min(tok_rows, (9 * entries + 8 * groups - 1) // (8 * groups))
    capacity = -(-capacity // 16) * 16
    named = weight_in > 0
    before = dot32(
        named.astype(BF), jnp.tri(tok_rows, dtype=BF).T
    )
    slot = jnp.where(named, before - 1.0, -1.0).astype(jnp.int32)
    rows_in, grads_in, acts, grad_gates, grad_ups = expert_rows(
        chips, capacity, h2_b, dy_all, slot, weight_in, w_gate[0], w_up[0], w_down[0], 2
    )
    all_rows = rows_in.reshape(-1, D)
    all_grads = grads_in.reshape(-1, D)
    all_acts = acts.reshape(groups * capacity, -1)
    all_gates = grad_gates.reshape(groups * capacity, -1)
    all_ups = grad_ups.reshape(groups * capacity, -1)

    def rep_send(v):
        return v, [from_rep(v, k) for k in range(1, reps)]

    def rep_sum(sent, after):
        (v, came), _ = lax.optimization_barrier((sent, after))
        return v.astype(F32) + sum(c.astype(F32) for c in came)

    slot_t, weight_t = slot.astype(F32).T, weight_in.T
    together = split_out and chips <= 8
    if together:
        out_sum, own_down, came_down, grad_wgate, grad_wup = outputs(
            chips, capacity, all_acts, all_rows, all_grads, all_gates, all_ups,
            slot_t, weight_t, w_down[0], 6,
        )
        grad_wdown = (own_down, [came_down])
    else:
        grad_wdown = rep_send(
            jnp.einsum("rf,rd->fd", all_acts, all_grads, preferred_element_type=F32).astype(BF)
        )
        grad_wgate = jnp.einsum("rd,rf->df", all_rows, all_gates, preferred_element_type=F32).astype(BF)
        grad_wup = jnp.einsum("rd,rf->df", all_rows, all_ups, preferred_element_type=F32).astype(BF)
    grad_wgate = rep_send(grad_wgate)
    grad_wup = rep_send(grad_wup)

    cuts = 1 if chips <= 8 else chips // 8
    (grad_gates, grad_ups), _ = lax.optimization_barrier(
        ((grad_gates, grad_ups), (grad_wdown[0], grad_wgate[0], grad_wup[0]))
    )
    grad_h2 = jnp.concatenate(
        [
            rows_back(chips, capacity, grad_gates, grad_ups, slot_t, wg, wu, 8 + i)
            for i, (wg, wu) in enumerate(
                zip(jnp.split(w_gate[0], cuts), jnp.split(w_up[0], cuts), strict=True)
            )
        ],
        axis=1,
    )


    grad_out = cotangent[0].astype(F32)
    _, hat_two, inv_two = rms_forward(mid_rows, g_ffn)
    grad_mid_norm, ffn_terms = rms_backward(grad_h2, hat_two, inv_two, g_ffn)
    grad_mid = grad_out + grad_mid_norm
    grad_mid_b = grad_mid.astype(BF)
    if not together:
        pick = (slot[:, None, :] == jnp.arange(capacity, dtype=jnp.int32)[None, :, None]).astype(BF)
        row_weight = jnp.sum(pick.astype(F32) * weight_in[:, None, :], axis=-1)
        acts_late, _ = lax.optimization_barrier((all_acts, grad_mid_b))
        eout = dot32(acts_late, w_down[0]).astype(BF).astype(F32)
        eout = (row_weight.reshape(-1, 1) * eout).astype(BF).reshape(groups, capacity, D)
        out_all = jnp.einsum("gct,gcd->gtd", pick, eout, preferred_element_type=F32).astype(BF)
        out_sum = lax.psum_scatter(
            out_all.reshape(groups * tok_rows, D), "grp", scatter_dimension=0, tiled=True
        )
    result = mid_rows + lax.optimization_barrier((out_sum, grad_mid_b))[0].astype(F32)
    grad_wdown = rep_sum(grad_wdown, grad_mid_b)
    grad_wgate = rep_sum(grad_wgate, grad_mid_b)
    grad_branch_b = rep_gather(grad_mid_b)
    (grad_branch_b, result, grad_wdown, grad_wgate), _ = lax.optimization_barrier(
        ((grad_branch_b, result, grad_wdown, grad_wgate), grad_mid_b)
    )
    grad_proj, query_terms, key_terms, grad_h1, rest, attn_terms = attention_back(
        tok_rows, projected, grad_branch_b, my_out, seq_b, g_query, g_key, cosine, sine, docs,
        full_qkv,
    )
    for k in range(1, reps):
        part = rest[(k - 1) * tok_rows : k * tok_rows]
        grad_h1 = grad_h1 + to_rep(part, k).astype(F32)
    _, hat_one, inv_one = rms_forward(own_b.astype(F32), g_attn)
    grad_rows_one, _ = rms_backward(grad_h1, hat_one, inv_one, g_attn)
    grad_tokens = grad_mid + grad_rows_one
    grad_gains = jnp.concatenate(
        [
            attn_terms[0],
            jnp.sum(ffn_terms, axis=0),
            query_terms[0],
            key_terms[0],
        ]
    )

    gain_size = gains.shape[0]
    gain_blocks = jnp.pad(
        grad_gains.reshape(groups, gain_size), ((0, 0), (0, 4096 - gain_size))
    ).reshape(groups, 32, 128)
    shard_qkv, half_out, total = dense_gradients(
        chips,
        split_out,
        h1_b,
        grad_proj,
        attended_b,
        grad_branch_b,
        gain_blocks,
        4,
    )
    total = total.reshape(-1)[:gain_size]
    grad_wup = rep_sum(grad_wup, shard_qkv)

    if split_out:
        shard_out = half_out
    else:
        qkv_all = [shard_qkv] + [from_rep(shard_qkv, k) for k in range(1, reps)]
        columns = jnp.stack(qkv_all, axis=0).reshape(reps, shard, 3, heads, HD)
        columns = columns[(jnp.arange(reps) - rep) % reps]
        shard_qkv = columns.transpose(1, 2, 3, 0, 4).reshape(shard, 3 * D).astype(F32)
        grad_wout = dot_tn(attended_b, grad_branch_b)
        whole = lax.dynamic_update_slice(
            jnp.zeros((heads, reps, HD, D), BF),
            grad_wout.astype(BF).reshape(heads, 1, HD, D),
            (0, rep, 0, 0),
        ).reshape(D, D)
        shard_out = lax.psum(
            lax.psum_scatter(whole, "grp", scatter_dimension=0, tiled=True), "rep"
        ).astype(F32)
        own_gains = total
        for k in range(1, reps):
            total = total + from_rep(own_gains, k)
    return (
        result[None],
        grad_tokens[None],
        shard_qkv,
        shard_out,
        total,
        grad_wgate[None],
        grad_wup[None],
        grad_wdown[None],
    )


def solution(mesh):
    in_specs = (
        P("grp", "rep", None),
        P("grp", None),
        P("grp", None),
        P("grp"),
        P("grp", None, None),
        P("grp", None, None),
        P("grp", None, None),
        P("grp", None),
        P("grp", "rep", None),
        P("grp", "rep", None),
        P("grp", "rep", None),
    )
    out_specs = (
        P("grp", "rep", None),
        P("grp", "rep", None),
        P("grp", None),
        P("grp", None),
        P("grp"),
        P("grp", None, None),
        P("grp", None, None),
        P("grp", None, None),
    )
    return jax.shard_map(
        per_device, mesh=mesh, in_specs=in_specs, out_specs=out_specs, check_vma=False
    )
```

```python
import functools

import jax
import jax.numpy as jnp
import numpy as np
from jax import lax
from jax.experimental import pallas as pl
from jax.experimental.pallas import tpu as pltpu
from jax.sharding import PartitionSpec as P

D = 2048
HEADS = 16
HD = 128
TOP = 8
BF = jnp.bfloat16
F32 = jnp.float32

epsilon = 1e-06
rope_base = 10000.0


def rms_forward(values, gain_vec):
    inverse = lax.rsqrt(jnp.mean(values * values, axis=-1, keepdims=True) + epsilon)
    normed = values * inverse
    return (normed * gain_vec, normed, inverse)


def rms_backward(grad_out, normed, inverse, gain_vec):
    scaled = grad_out * gain_vec
    grad_in = inverse * (scaled - normed * jnp.mean(scaled * normed, axis=-1, keepdims=True))
    return (grad_in, grad_out * normed)


def dot32(a, b):
    return jnp.dot(a, b, preferred_element_type=F32)


class Ring:
    def __init__(self, devices):
        self.devices = devices
        self.chips = devices // 2
        outer = 4 if self.chips % 4 == 0 else 2
        inner = self.chips // outer
        cycle = [(a, 0) for a in range(outer)]
        for step, a in enumerate(reversed(range(outer))):
            columns = range(1, inner)
            cycle += [(a, b) for b in (columns if step % 2 == 0 else reversed(columns))]
        self.cycle = [a * inner + b for a, b in cycle]
        self.place = {chip: i for i, chip in enumerate(self.cycle)}
        self.half = self.chips // 2

    def perm(self, shift):
        pairs = []
        for chip in range(self.chips):
            other = self.cycle[(self.place[chip] + shift) % self.chips]
            pairs += [(2 * chip + core, 2 * other + core) for core in range(2)]
        return pairs

    def table(self):
        out = np.zeros((self.devices, self.chips, 2), np.int32)
        for dev in range(self.devices):
            chip, core = dev // 2, dev % 2
            for d in range(self.chips):
                other = self.cycle[(self.place[chip] + d) % self.chips]
                out[dev, d, 0] = 2 * other + core
                out[dev, d, 1] = 2 * other + (1 - core)
        return out

    def ahead(self, v):
        return lax.ppermute(v, "grp", self.perm(1))

    def back(self, v):
        return lax.ppermute(v, "grp", self.perm(-1))

    def flip(self, v):
        return lax.ppermute(v, "grp", [(i, i ^ 1) for i in range(self.devices)])

    def gather(self, own):
        rows = own.shape[0] // 2
        blocks = {0: (own, self.flip(own))}
        up = down = own
        for step in range(1, self.half):
            up, down = self.ahead(up), self.back(down)
            blocks[-step % self.chips] = (up, self.flip(up))
            blocks[step] = (down, self.flip(down))
        first, last = self.ahead(up[:rows]), self.back(down[rows:])
        far = jnp.concatenate([first, last], axis=0)
        blocks[self.half] = (far, self.flip(far))
        return blocks

    def scatter_sum(self, blocks):
        def joined(d):
            same, other = blocks[d]
            return same.astype(F32) + self.flip(other.astype(BF)).astype(F32)

        far = joined(self.half).astype(BF)
        rows = far.shape[0] // 2
        up, down = self.ahead(far[:rows]), self.back(far[rows:])
        zero = jnp.zeros_like(up)
        up = jnp.concatenate([up, zero], axis=0)
        down = jnp.concatenate([zero, down], axis=0)
        for step in range(self.half - 1, 0, -1):
            up = self.ahead((joined(step) + up.astype(F32)).astype(BF))
            down = self.back((joined(-step % self.chips) + down.astype(F32)).astype(BF))
        return joined(0) + up.astype(F32) + down.astype(F32)


MESH = pl.DeviceIdType.MESH
DMA = pltpu.SemaphoreType.DMA
VMEM_LIMIT = 60 << 20


class Hops:
    def __init__(self, chips):
        self.chips, self.half = chips, chips // 2
        self.outer = 4 if chips % 4 == 0 else 2
        self.inner = chips // self.outer
        self.me = lax.axis_index("grp")
        chip, self.core = self.me // 2, self.me % 2
        a, b = chip // self.inner, chip % self.inner
        row = self.outer - 1 - a
        along = jnp.where(row % 2 == 0, b - 1, self.inner - 1 - b)
        self.place = jnp.where(b == 0, a, self.outer + row * (self.inner - 1) + along)
        self.ahead, self.back = self.device(1), self.device(-1)
        self.flip = self.me + 1 - 2 * self.core
        self.started = []

    def chip(self, d):
        p = (self.place + (d % self.chips)) % self.chips
        q = jnp.maximum(p - self.outer, 0)
        k, m = q // (self.inner - 1), q % (self.inner - 1)
        b = jnp.where(k % 2 == 0, m + 1, self.inner - 1 - m)
        return jnp.where(
            p < self.outer, p * self.inner, (self.outer - 1 - k) * self.inner + b
        )

    def device(self, d):
        return 2 * self.chip(d) + self.core

    def meet(self, reps=1):
        barrier = pltpu.get_barrier_semaphore()
        for dev in (self.ahead, self.back, self.flip):
            pl.semaphore_signal(barrier, inc=1, device_id={"grp": dev}, device_id_type=MESH)
        rep = lax.axis_index("rep")
        for k in range(1, reps):
            pl.semaphore_signal(
                barrier, inc=1, device_id={"rep": (rep + k) % reps}, device_id_type=MESH
            )
        pl.semaphore_wait(barrier, 2 + reps)

    def copy(self, src, dst, send_sem, recv_sem, dev):
        return pltpu.make_async_remote_copy(
            src_ref=src,
            dst_ref=dst,
            send_sem=send_sem,
            recv_sem=recv_sem,
            device_id={"grp": dev},
            device_id_type=MESH,
        )

    def send(self, src, dst, sems, at, dev):
        c = self.copy(src, dst, sems.at[0, at], sems.at[1, at], dev)
        c.start()
        self.started.append(c)

    def wait(self, dst, sems, at):
        self.copy(dst, dst, sems.at[0, at], sems.at[1, at], self.flip).wait_recv()

    def drain(self):
        for c in self.started:
            c.wait_send()

    def gather(self, items, use):
        half = self.half

        def parts(ref):
            cut = ref.shape[0] // 2
            return ref.at[pl.ds(0, cut)], ref.at[pl.ds(cut, ref.shape[0] - cut)]

        for own, slot, up, down, side in items:
            self.send(own, slot(self.me), up, 0, self.ahead)
            self.send(own, slot(self.me), down, 0, self.back)
            self.send(own, slot(self.me), side, 0, self.flip)
        yield

        def ready(d):
            dev = self.device(d)
            for _, slot, _, _, side in items:
                self.wait(slot(dev + 1 - 2 * self.core), side, d % self.chips)
            use(d)

        ready(0)
        for s in range(1, half):
            last = s == half - 1
            for _, slot, up, down, side in items:
                a, b = slot(self.device(-s)), slot(self.device(s))
                self.wait(a, up, s - 1)
                part = parts(a)[0] if last else a
                self.send(part, part, up, s, self.ahead)
                self.send(a, a, side, -s % self.chips, self.flip)
                self.wait(b, down, s - 1)
                part = parts(b)[1] if last else b
                self.send(part, part, down, s, self.back)
                self.send(b, b, side, s, self.flip)
            for d in (-s, s):
                ready(d)
            yield
        for _, slot, up, down, side in items:
            far = slot(self.device(half))
            low, high = parts(far)
            self.wait(low, up, half - 1)
            self.wait(high, down, half - 1)
            self.send(far, far, side, half, self.flip)
        ready(half)

    def scatter(self, rows, produce, mine, out, came, far, up_in, down_in, up, down, side, finish):
        half, chips = self.half, self.chips
        cut = rows // 2
        strip = 16
        made = {}

        def make(d):
            made[d] = len(made) % mine.shape[0]
            produce(d, mine.at[made[d]], out.at[d % chips])
            self.send(out.at[d % chips], came.at[d % chips], side, d % chips, self.flip)

        def joined(d, at):
            return mine[made[d], at, :] + came[d % chips, at, :].astype(F32)

        def strips(first, last, body):
            def step(i, carry):
                body(pl.ds(pl.multiple_of(first + i * strip, strip), strip))
                return carry

            lax.fori_loop(0, (last - first) // strip, step, 0)

        for d in (half, half - 1):
            make(d)
        self.wait(came.at[half], side, half)

        def far_sum(at):
            far[at, :] = joined(half, at).astype(BF)

        strips(0, rows, far_sum)
        low, high = pl.ds(0, cut), pl.ds(cut, rows - cut)
        self.send(far.at[low], up_in.at[0, low], up, 0, self.ahead)
        self.send(far.at[high], down_in.at[0, high], down, 0, self.back)
        make(1 - half)
        yield
        for s in range(half - 1, 0, -1):
            i = half - s
            for d in sorted({s - 1, 1 - s}):
                make(d)
            for d, buf, sems, target in (
                (s, up_in, up, self.ahead),
                (-s, down_in, down, self.back),
            ):
                self.wait(came.at[d % chips], side, d % chips)

                def fresh(at, d=d, buf=buf, i=i):
                    buf[i - 1, at, :] = joined(d, at).astype(BF)

                def onto(at, d=d, buf=buf, i=i):
                    buf[i - 1, at, :] = (joined(d, at) + buf[i - 1, at, :].astype(F32)).astype(BF)

                if i > 1:
                    self.wait(buf.at[i - 1], sems, i - 1)
                    strips(0, rows, onto)
                elif d > 0:
                    self.wait(buf.at[0, low], sems, 0)
                    strips(0, cut, onto)
                    strips(cut, rows, fresh)
                else:
                    self.wait(buf.at[0, high], sems, 0)
                    strips(0, cut, fresh)
                    strips(cut, rows, onto)
                self.send(buf.at[i - 1], buf.at[i], sems, i, target)
            yield
        self.wait(came.at[0], side, 0)
        self.wait(up_in.at[half - 1], up, half - 1)
        self.wait(down_in.at[half - 1], down, half - 1)

        def total(at):
            finish(
                joined(0, at)
                + up_in[half - 1, at, :].astype(F32)
                + down_in[half - 1, at, :].astype(F32),
                at,
            )

        strips(0, rows, total)

    def turn(self, *rings):
        rings = list(rings)
        while rings:
            rings = [r for r in rings if next(r, self) is not self]
        self.drain()


def scatter_scratch(chips, rows, width):
    half = chips // 2
    return [
        pltpu.VMEM((4, rows, width), F32),
        pltpu.VMEM((chips, rows, width), BF),
        pltpu.VMEM((chips, rows, width), BF),
        pltpu.VMEM((rows, width), BF),
        pltpu.VMEM((half, rows, width), BF),
        pltpu.VMEM((half, rows, width), BF),
    ]


def dot_nt(a, b):
    return lax.dot_general(a, b, (((1,), (1,)), ((), ())), preferred_element_type=F32)


def dot_tn(a, b):
    return lax.dot_general(a, b, (((0,), (0,)), ((), ())), preferred_element_type=F32)


def tiles(count, width, body):
    for i in range(count):
        body(pl.ds(i * width, width))


def experts_kernel(
    chips, cap,
    h2_ref, dy_ref, slot_ref, weight_ref, wg_hbm, wu_hbm, wd_hbm,
    xs_ref, de_ref, act_ref, dg_ref, du_ref,
    held, dy, wg, wu, wd, xs_b, de_b, act_b, dg_b, du_b,
    w_sem, dy_sem, own_sem, out_sem, *sems,
):
    hops = Hops(chips)
    half = chips // 2
    tok, width = h2_ref.shape
    ff = wg.shape[1]
    order = [0]
    for s in range(1, half):
        order += [-s, s]
    order += [half]
    number = {d: i for i, d in enumerate(order)}

    loads = [
        pltpu.make_async_copy(a, b, w_sem.at[i])
        for i, (a, b) in enumerate(((wg_hbm, wg), (wu_hbm, wu), (wd_hbm, wd)))
    ]

    def dy_copy(i):
        chip = hops.chip(order[i])
        return pltpu.make_async_copy(dy_ref.at[pl.ds(2 * chip, 2)], dy.at[i % 2], dy_sem.at[i % 2])

    def out_copies(i):
        chip = hops.chip(order[i])
        pairs = ((xs_b, xs_ref), (de_b, de_ref), (act_b, act_ref), (dg_b, dg_ref), (du_b, du_ref))
        return [
            pltpu.make_async_copy(b.at[i % 2], r.at[chip], out_sem.at[i % 2, j])
            for j, (b, r) in enumerate(pairs)
        ]

    hops.meet()
    own = pltpu.make_async_copy(h2_ref, held.at[hops.me], own_sem)
    own.start()

    def use(d):
        i = number[d]
        p = i % 2
        if i == 0:
            own.wait()
            for c in loads:
                c.start()
            dy_copy(0).start()
            for c in loads:
                c.wait()
        dy_copy(i).wait()
        if i + 1 < chips:
            dy_copy(i + 1).start()
        if i >= 2:
            for c in out_copies(i - 2):
                c.wait()
        chip = hops.chip(d)
        for k in range(2):
            dev = 2 * chip + k
            hit = slot_ref[pl.ds(dev, 1), :] == lax.broadcasted_iota(jnp.int32, (cap, tok), 0)
            pick = hit.astype(F32).astype(BF)
            scale = jnp.sum(
                jnp.where(hit, weight_ref[pl.ds(dev, 1), :], 0.0), axis=1, keepdims=True
            )
            rows = pl.ds(k * cap, cap)

            def choose(at, k=k, dev=dev, pick=pick, scale=scale, rows=rows):
                xs_b[p, rows, at] = dot32(pick, held[dev, :, at]).astype(BF)
                de_b[p, rows, at] = (scale * dot32(pick, dy[p, k, :, at])).astype(BF)

            tiles(width // 1024, 1024, choose)

        def hidden(at):
            gpre = dot32(xs_b[p], wg[:, at])
            upre = dot32(xs_b[p], wu[:, at])
            dact = dot_nt(de_b[p], wd[at, :])
            sig = 1.0 / (1.0 + jnp.exp(-gpre))
            act_b[p, :, at] = (gpre * sig * upre).astype(BF)
            dg_b[p, :, at] = (dact * upre * sig * (1.0 + gpre * (1.0 - sig))).astype(BF)
            du_b[p, :, at] = (dact * gpre * sig).astype(BF)

        tiles(ff // 512, 512, hidden)
        for c in out_copies(i):
            c.start()

    hops.turn(hops.gather(in_halves(h2_ref, lambda dev: held.at[dev], sems), use))
    for i in (chips - 2, chips - 1):
        for c in out_copies(i):
            c.wait()


def expert_rows(chips, cap, h2, dy_all, slot, weight, wg, wu, wd, collective_id):
    tok, width = h2.shape
    ff = wg.shape[1]
    anywhere = pl.BlockSpec(memory_space=pl.ANY)
    vmem = pl.BlockSpec(memory_space=pltpu.VMEM)
    wide = jax.ShapeDtypeStruct((chips, 2 * cap, width), BF)
    thin = jax.ShapeDtypeStruct((chips, 2 * cap, ff), BF)
    return pl.pallas_call(
        functools.partial(experts_kernel, chips, cap),
        out_shape=(wide, wide, thin, thin, thin),
        in_specs=[anywhere, anywhere, vmem, vmem, anywhere, anywhere, anywhere],
        out_specs=(anywhere,) * 5,
        scratch_shapes=[
            pltpu.VMEM((2 * chips, tok, width), BF),
            pltpu.VMEM((2, 2, tok, width), BF),
            pltpu.VMEM((width, ff), BF),
            pltpu.VMEM((width, ff), BF),
            pltpu.VMEM((ff, width), BF),
            pltpu.VMEM((2, 2 * cap, width), BF),
            pltpu.VMEM((2, 2 * cap, width), BF),
            pltpu.VMEM((2, 2 * cap, ff), BF),
            pltpu.VMEM((2, 2 * cap, ff), BF),
            pltpu.VMEM((2, 2 * cap, ff), BF),
            DMA((3,)),
            DMA((2,)),
            DMA,
            DMA((2, 5)),
            *ring_sems(chips),
            *ring_sems(chips),
        ],
        compiler_params=pltpu.CompilerParams(
            collective_id=collective_id, has_side_effects=True, vmem_limit_bytes=VMEM_LIMIT
        ),
        cost_estimate=pl.CostEstimate(
            flops=2 * chips * cap * width * ff * 6, transcendentals=0, bytes_accessed=200 << 20
        ),
        name="experts",
    )(h2, dy_all, slot, weight, wg, wu, wd)


def column_of(table, dev):
    lanes = lax.broadcasted_iota(jnp.int32, table.shape, 1)
    return jnp.sum(jnp.where(lanes == dev, table[...], 0.0), axis=1, keepdims=True)


def returned(hops, d, cap, tok, slot_ref, rows_ref, same_ref, other_ref, weight_ref=None):
    chip = hops.chip(d)
    lanes = lax.broadcasted_iota(jnp.int32, (tok, cap), 1).astype(F32)
    for k, ref in ((hops.core, same_ref), (1 - hops.core, other_ref)):
        pick = (column_of(slot_ref, 2 * chip + k) == lanes).astype(F32).astype(BF)
        rows = pl.ds(pl.multiple_of(k * cap, 16), cap)
        weight = None if weight_ref is None else column_of(weight_ref, 2 * chip + k)

        def spread(at, pick=pick, rows=rows, ref=ref, weight=weight):
            value = dot32(pick, rows_ref[rows, at])
            if weight is not None:
                value = weight * value
            ref[:, at] = value.astype(ref.dtype)

        tiles(rows_ref.shape[1] // 1024, 1024, spread)


def scatter_order(half):
    order = [half, half - 1, 1 - half]
    for s in range(half - 2, 0, -1):
        order += [-s, s]
    return order + [0]


def outputs_kernel(
    chips, cap,
    act_ref, xs_ref, de_ref, dg_ref, du_ref, slot_ref, weight_ref, wd_hbm,
    total_ref, down_ref, came_ref, gate_ref, up_ref,
    wd, left, right, made_d, made, act, rows_b, mine, out, came, far, up_in, down_in,
    up, down, side, w_sem, act_sem, left_sem, right_sem, made_sem, down_sem, rep_sem,
):
    hops = Hops(chips)
    replica = lax.axis_index("rep")
    tok, width = total_ref.shape
    order = scatter_order(chips // 2)
    number = {d: i for i, d in enumerate(order)}
    strip = right.shape[2]
    count = width // strip

    def act_copy(i):
        rows = pl.ds(pl.multiple_of(hops.chip(order[i]) * (2 * cap), 2 * cap), 2 * cap)
        return pltpu.make_async_copy(act_ref.at[rows], act.at[i % 2], act_sem.at[i % 2])

    jobs = [
        (thin, wide, result, i)
        for thin, wide, result in (
            (act_ref, de_ref, down_ref),
            (dg_ref, xs_ref, gate_ref),
            (du_ref, xs_ref, up_ref),
        )
        for i in range(count)
    ]
    done, stored, sent = [], {}, []

    def right_copy(n):
        at = pl.ds(jobs[n][3] * strip, strip)
        return pltpu.make_async_copy(jobs[n][1].at[:, at], right.at[n % 2], right_sem.at[n % 2])

    def left_copy(n):
        return pltpu.make_async_copy(jobs[n][0], left, left_sem)

    def job():
        n = len(done)
        if n == len(jobs):
            return
        done.append(n)
        _, _, result, i = jobs[n]
        if i == 0:
            left_copy(n).wait()
        right_copy(n).wait()
        if n + 1 < len(jobs):
            right_copy(n + 1).start()
        at = pl.ds(i * strip, strip)
        if n < count:
            made_d[i] = dot_tn(left[...], right[n % 2]).astype(BF)
            stored[n] = pltpu.make_async_copy(made_d.at[i], result.at[:, at], down_sem.at[i])
            c = pltpu.make_async_remote_copy(
                src_ref=made_d.at[i],
                dst_ref=came_ref.at[:, at],
                send_sem=rep_sem.at[0, i],
                recv_sem=rep_sem.at[1, i],
                device_id={"rep": 1 - replica},
                device_id_type=MESH,
            )
            c.start()
            sent.append(c)
        else:
            if n - 2 >= count:
                stored.pop(n - 2).wait()
            made[n % 2] = dot_tn(right[n % 2], left[...]).astype(BF)
            stored[n] = pltpu.make_async_copy(made.at[n % 2], result.at[at, :], made_sem.at[n % 2])
        stored[n].start()
        if i == count - 1 and n + 1 < len(jobs):
            left_copy(n + 1).start()

    def produce(d, same_ref, other_ref):
        i = number[d]
        act_copy(i).wait()
        if i + 1 < chips:
            act_copy(i + 1).start()

        def last(at):
            rows_b[:, at] = dot32(act[i % 2], wd[:, at]).astype(BF)

        tiles(width // 512, 512, last)
        returned(hops, d, cap, tok, slot_ref, rows_b, same_ref, other_ref, weight_ref)

    def finish(value, at):
        total_ref[at, :] = value

    load = pltpu.make_async_copy(wd_hbm, wd, w_sem)
    left_copy(0).start()
    right_copy(0).start()
    act_copy(0).start()
    load.start()
    hops.meet(2)
    ring = hops.scatter(tok, produce, mine, out, came, far, up_in, down_in, up, down, side, finish)
    job()
    load.wait()
    share = -(-(len(jobs) - 2) // (chips // 2 - 1))
    for step in range(chips // 2):
        next(ring)
        for _ in range(share if step else 1):
            job()
    hops.turn(ring)
    for c in stored.values():
        c.wait()
    for c in sent:
        c.wait()


def outputs(chips, cap, act, xs, de, dg, du, slot_t, weight_t, wd, collective_id):
    ff, width = wd.shape
    tok = slot_t.shape[0]
    strip = 512
    anywhere = pl.BlockSpec(memory_space=pl.ANY)
    vmem = pl.BlockSpec(memory_space=pltpu.VMEM)
    tall, flat = jax.ShapeDtypeStruct((width, ff), BF), jax.ShapeDtypeStruct((ff, width), BF)
    return pl.pallas_call(
        functools.partial(outputs_kernel, chips, cap),
        out_shape=(jax.ShapeDtypeStruct((tok, width), F32), flat, flat, tall, tall),
        in_specs=[anywhere] * 5 + [vmem] * 2 + [anywhere],
        out_specs=(vmem,) + (anywhere,) * 4,
        scratch_shapes=[
            pltpu.VMEM((ff, width), BF),
            pltpu.VMEM((2 * chips * cap, ff), BF),
            pltpu.VMEM((2, 2 * chips * cap, strip), BF),
            pltpu.VMEM((width // strip, ff, strip), BF),
            pltpu.VMEM((2, strip, ff), BF),
            pltpu.VMEM((2, 2 * cap, ff), BF),
            pltpu.VMEM((2 * cap, width), BF),
            *scatter_scratch(chips, tok, width),
            *ring_sems(chips),
            DMA,
            DMA((2,)),
            DMA,
            DMA((2,)),
            DMA((2,)),
            DMA((width // strip,)),
            DMA((2, width // strip)),
        ],
        compiler_params=pltpu.CompilerParams(
            collective_id=collective_id, has_side_effects=True, vmem_limit_bytes=63 << 20
        ),
        cost_estimate=pl.CostEstimate(
            flops=2 * 2 * chips * cap * width * ff * 4, transcendentals=0, bytes_accessed=200 << 20
        ),
        name="outputs",
    )(act, xs, de, dg, du, slot_t, weight_t, wd)


def rows_back_kernel(
    chips, cap,
    dg_ref, du_ref, slot_ref, wg_hbm, wu_hbm, total_ref,
    wg, wu, dg, du, drow, mine, out, came, far, up_in, down_in,
    up, down, side, w_sem, in_sem,
):
    hops = Hops(chips)
    tok, width = total_ref.shape
    order = scatter_order(chips // 2)
    number = {d: i for i, d in enumerate(order)}
    loads = [
        pltpu.make_async_copy(a, b, w_sem.at[i])
        for i, (a, b) in enumerate(((wg_hbm, wg), (wu_hbm, wu)))
    ]

    def in_copies(i):
        chip = hops.chip(order[i])
        return [
            pltpu.make_async_copy(r.at[chip], b.at[i % 2], in_sem.at[i % 2, j])
            for j, (r, b) in enumerate(((dg_ref, dg), (du_ref, du)))
        ]

    for c in loads + in_copies(0):
        c.start()
    hops.meet()
    for c in loads:
        c.wait()

    def produce(d, same_ref, other_ref):
        i = number[d]
        p = i % 2
        for c in in_copies(i):
            c.wait()
        if i + 1 < chips:
            for c in in_copies(i + 1):
                c.start()

        def back(at):
            drow[:, at] = (dot_nt(dg[p], wg[at, :]) + dot_nt(du[p], wu[at, :])).astype(BF)

        tiles(width // 512, 512, back)
        returned(hops, d, cap, tok, slot_ref, drow, same_ref, other_ref)

    def finish(value, at):
        total_ref[at, :] = value

    hops.turn(
        hops.scatter(tok, produce, mine, out, came, far, up_in, down_in, up, down, side, finish)
    )


def rows_back(chips, cap, dg, du, slot, wg, wu, collective_id):
    tok = slot.shape[0]
    width, ff = wg.shape
    anywhere = pl.BlockSpec(memory_space=pl.ANY)
    vmem = pl.BlockSpec(memory_space=pltpu.VMEM)
    return pl.pallas_call(
        functools.partial(rows_back_kernel, chips, cap),
        out_shape=jax.ShapeDtypeStruct((tok, width), F32),
        in_specs=[anywhere, anywhere, vmem, anywhere, anywhere],
        out_specs=vmem,
        scratch_shapes=[
            pltpu.VMEM((width, ff), BF),
            pltpu.VMEM((width, ff), BF),
            pltpu.VMEM((2, 2 * cap, ff), BF),
            pltpu.VMEM((2, 2 * cap, ff), BF),
            pltpu.VMEM((2 * cap, width), BF),
            *scatter_scratch(chips, tok, width),
            *ring_sems(chips),
            DMA((2,)),
            DMA((2, 2)),
        ],
        compiler_params=pltpu.CompilerParams(
            collective_id=collective_id, has_side_effects=True, vmem_limit_bytes=VMEM_LIMIT
        ),
        cost_estimate=pl.CostEstimate(
            flops=2 * chips * cap * width * ff * 6, transcendentals=0, bytes_accessed=200 << 20
        ),
        name="rows_back",
    )(dg, du, slot, wg, wu)


def turned(v, cosine, sine):
    return v * cosine + pltpu.roll(v, HD // 2, 1) * sine


def head_of(proj, at, gain, cosine, sine):
    value = proj[:, at]
    inverse = lax.rsqrt(jnp.mean(value * value, axis=-1, keepdims=True) + epsilon)
    hat = value * inverse
    return hat, inverse, turned(hat * gain, cosine, sine).astype(BF)


def softmax_rows(queries, keys, docs_q, docs_k):
    raw = dot_nt(queries, keys) * HD ** (-0.5)
    raw = jnp.where(docs_q == docs_k, raw, -1e30)
    grown = jnp.exp(raw - jnp.max(raw, axis=-1, keepdims=True))
    return grown * (1.0 / jnp.sum(grown, axis=-1, keepdims=True))


def columns_of(block, head, heads):
    return pl.ds(pl.multiple_of((block * heads + head) * HD, HD), HD)


def attention_kernel(
    chips, reps, heads,
    cot_ref, seq_ref, ga_ref, gf_ref, gq_ref, gk_ref, cos_ref, sin_ref, dc_ref, dr_ref, wq_hbm, wo_hbm,
    dy_ref, h1_out, proj_out, ob_out, mid_ref, h2_ref,
    wq, wo, give, came, h1_ref, proj_ref, ob_ref, rep_sem, own_sem, out_sem, *sems,
):
    hops = Hops(chips)
    rep = lax.axis_index("rep")
    seq_len, width = seq_ref.shape
    tok = mid_ref.shape[0]
    block = min(256, seq_len)
    loads = [
        pltpu.make_async_copy(a, b, own_sem.at[i])
        for i, (a, b) in enumerate(((wq_hbm, wq), (wo_hbm, wo), (cot_ref, dy_ref.at[hops.me])))
    ]
    hops.meet(reps)
    ring = hops.gather(in_halves(cot_ref, lambda dev: dy_ref.at[dev], sems), lambda d: None)
    next(ring)
    for c in loads:
        c.start()

    def normed(i, carry):
        rows = pl.ds(pl.multiple_of(i * 64, 64), 64)
        v = seq_ref[rows, :].astype(F32)
        v = v * lax.rsqrt(jnp.mean(v * v, axis=-1, keepdims=True) + epsilon)
        h1_ref[rows, :] = (v * ga_ref[...]).astype(BF)
        return carry

    lax.fori_loop(0, seq_len // 64, normed, 0)
    loads[0].wait()
    total = 3 * heads * HD
    step = 512 if total % 512 == 0 else HD
    for i in range(total // step):
        at = pl.ds(i * step, step)
        proj_ref[:, at] = dot32(h1_ref[...], wq[:, at])

    stores = [
        pltpu.make_async_copy(a, b, out_sem.at[i])
        for i, (a, b) in enumerate(((h1_ref, h1_out), (proj_ref, proj_out), (ob_ref, ob_out)))
    ]
    stores[0].start()
    stores[1].start()

    def one(head, carry):
        _, _, q_b = head_of(
            proj_ref, columns_of(0, head, heads), gq_ref[...], cos_ref[...], sin_ref[...]
        )
        _, _, k_b = head_of(
            proj_ref, columns_of(1, head, heads), gk_ref[...], cos_ref[...], sin_ref[...]
        )
        v_b = proj_ref[:, columns_of(2, head, heads)].astype(BF)
        for i in range(seq_len // block):
            rows = slice(i * block, (i + 1) * block)
            probs = softmax_rows(q_b[rows], k_b, dc_ref[rows, :], dr_ref[...])
            ob_ref[rows, columns_of(0, head, heads)] = dot32(probs.astype(BF), v_b).astype(BF)
        return carry

    lax.fori_loop(0, heads // 2, one, 0)
    next(ring)
    lax.fori_loop(heads // 2, heads, one, 0)
    stores[2].start()
    loads[1].wait()
    swaps = []
    for k in range(1, reps):
        for i in range(width // 512):
            at = pl.ds(i * 512, 512)
            give[k - 1, :, at] = dot32(ob_ref[pl.ds(k * tok, tok), :], wo[:, at]).astype(BF)
        c = pltpu.make_async_remote_copy(
            src_ref=give.at[k - 1],
            dst_ref=came.at[k - 1],
            send_sem=rep_sem.at[0, k - 1],
            recv_sem=rep_sem.at[1, k - 1],
            device_id={"rep": (rep + k) % reps},
            device_id_type=MESH,
        )
        c.start()
        swaps.append(c)
    for i in range(width // 512):
        at = pl.ds(i * 512, 512)
        mid_ref[:, at] = dot32(ob_ref[pl.ds(0, tok), :], wo[:, at])
    next(ring)
    for c in swaps:
        c.wait()

    def second(i, carry):
        rows = pl.ds(pl.multiple_of(i * 64, 64), 64)
        v = seq_ref[rows, :].astype(F32) + mid_ref[rows, :]
        for k in range(1, reps):
            v = v + came[k - 1, rows, :].astype(F32)
        mid_ref[rows, :] = v
        v = v * lax.rsqrt(jnp.mean(v * v, axis=-1, keepdims=True) + epsilon)
        h2_ref[rows, :] = (v * gf_ref[...]).astype(BF)
        return carry

    lax.fori_loop(0, tok // 64, second, 0)
    loads[2].wait()
    hops.turn(ring)
    for c in stores:
        c.wait()


def attention(chips, reps, cot, seq, ga, gf, gq, gk, cosine, sine, docs, w_qkv, w_out, collective_id):
    seq_len, width = seq.shape
    tok = cot.shape[0]
    heads = w_out.shape[0] // HD
    anywhere = pl.BlockSpec(memory_space=pl.ANY)
    vmem = pl.BlockSpec(memory_space=pltpu.VMEM)
    return pl.pallas_call(
        functools.partial(attention_kernel, chips, reps, heads),
        out_shape=(
            jax.ShapeDtypeStruct((2 * chips, tok, width), BF),
            jax.ShapeDtypeStruct((seq_len, width), BF),
            jax.ShapeDtypeStruct((seq_len, 3 * heads * HD), F32),
            jax.ShapeDtypeStruct((seq_len, heads * HD), BF),
            jax.ShapeDtypeStruct((tok, width), F32),
            jax.ShapeDtypeStruct((tok, width), BF),
        ),
        in_specs=[anywhere] + [vmem] * 9 + [anywhere] * 2,
        out_specs=(anywhere,) * 4 + (vmem,) * 2,
        scratch_shapes=[
            pltpu.VMEM(w_qkv.shape, BF),
            pltpu.VMEM(w_out.shape, BF),
            pltpu.VMEM((reps - 1, tok, width), BF),
            pltpu.VMEM((reps - 1, tok, width), BF),
            pltpu.VMEM((seq_len, width), BF),
            pltpu.VMEM((seq_len, 3 * heads * HD), F32),
            pltpu.VMEM((seq_len, heads * HD), BF),
            DMA((2, reps - 1)),
            DMA((3,)),
            DMA((3,)),
            *ring_sems(chips),
            *ring_sems(chips),
        ],
        compiler_params=pltpu.CompilerParams(
            collective_id=collective_id, has_side_effects=True, vmem_limit_bytes=VMEM_LIMIT
        ),
        cost_estimate=pl.CostEstimate(
            flops=2 * seq_len * w_qkv.size, transcendentals=0, bytes_accessed=100 << 20
        ),
        name="attention",
    )(cot, seq, ga, gf, gq, gk, cosine, sine, docs[:, None], docs[None, :], w_qkv, w_out)


def attention_back_kernel(
    heads,
    proj_ref, mid_ref, wo_ref, seq_ref, gq_ref, gk_ref, cos_ref, sin_ref, dc_ref, dr_ref, wq_hbm,
    grad_ref, qt_ref, kt_ref, own_ref, rest_ref, at_ref,
    dob, dk, dv, wq, scale_b, w_sem,
):
    seq_len = proj_ref.shape[0]
    load = pltpu.make_async_copy(wq_hbm, wq, w_sem)
    load.start()
    block = min(256, seq_len)
    scale = HD ** (-0.5)
    for i in range(heads * HD // 512):
        at = pl.ds(i * 512, 512)
        dob[:, at] = dot_nt(mid_ref[...], wo_ref[at, :]).astype(BF)
    qt_ref[...] = jnp.zeros_like(qt_ref)
    kt_ref[...] = jnp.zeros_like(kt_ref)

    def unturned(grad, hat, inverse, gain, rows):
        grad = turned(grad, cos_ref[rows, :], -sin_ref[rows, :])
        scaled = grad * gain
        pre = inverse * (scaled - hat * jnp.mean(scaled * hat, axis=-1, keepdims=True))
        return pre.astype(BF), jnp.sum(grad * hat, axis=0, keepdims=True)

    def one(head, carry):
        q_at, k_at, v_at = (columns_of(b, head, heads) for b in range(3))
        q_hat, q_inv, q_b = head_of(proj_ref, q_at, gq_ref[...], cos_ref[...], sin_ref[...])
        k_hat, k_inv, k_b = head_of(proj_ref, k_at, gk_ref[...], cos_ref[...], sin_ref[...])
        v_b = proj_ref[:, v_at].astype(BF)
        for i in range(seq_len // block):
            rows = slice(i * block, (i + 1) * block)
            probs = softmax_rows(q_b[rows], k_b, dc_ref[rows, :], dr_ref[...])
            grad_o = dob[rows, columns_of(0, head, heads)]
            grad_p = dot_nt(grad_o, v_b)
            grad_s = (
                probs * (grad_p - jnp.sum(probs * grad_p, axis=-1, keepdims=True))
            ).astype(BF)
            dv_part = dot_tn(probs.astype(BF), grad_o)
            dk_part = dot_tn(grad_s, q_b[rows])
            if i == 0:
                dv[...] = dv_part
                dk[...] = dk_part
            else:
                dv[...] += dv_part
                dk[...] += dk_part
            pre, terms = unturned(
                dot32(grad_s, k_b) * scale, q_hat[rows], q_inv[rows], gq_ref[...], rows
            )
            grad_ref[rows, q_at] = pre
            qt_ref[...] += terms
        pre, terms = unturned(dk[...] * scale, k_hat, k_inv, gk_ref[...], slice(0, seq_len))
        grad_ref[:, k_at] = pre
        kt_ref[...] += terms
        grad_ref[:, v_at] = dv[...].astype(BF)
        return carry

    lax.fori_loop(0, heads, one, 0)

    tok = own_ref.shape[0]

    def inverses(i, carry):
        rows = pl.ds(pl.multiple_of(i * 64, 64), 64)
        v = seq_ref[rows, :].astype(F32)
        scale_b[rows, :] = lax.rsqrt(jnp.mean(v * v, axis=-1, keepdims=True) + epsilon)
        return carry

    lax.fori_loop(0, seq_len // 64, inverses, 0)
    load.wait()
    for i in range(wq.shape[0] // 256):
        at = pl.ds(i * 256, 256)
        part = dot_nt(grad_ref[...], wq[at, :])
        own_ref[:, at] = part[:tok]
        rest_ref[:, at] = part[tok:].astype(BF)
        hat = seq_ref[:, at].astype(F32) * scale_b[...]
        at_ref[:, at] = jnp.sum(part * hat, axis=0, keepdims=True)


def attention_back(tok, proj, mid, w_out, seq, gq, gk, cosine, sine, docs, w_qkv):
    seq_len = proj.shape[0]
    heads = w_out.shape[0] // HD
    vmem = pl.BlockSpec(memory_space=pltpu.VMEM)
    return pl.pallas_call(
        functools.partial(attention_back_kernel, heads),
        out_shape=(
            jax.ShapeDtypeStruct(proj.shape, BF),
            jax.ShapeDtypeStruct((1, HD), F32),
            jax.ShapeDtypeStruct((1, HD), F32),
            jax.ShapeDtypeStruct((tok, D), F32),
            jax.ShapeDtypeStruct((seq_len - tok, D), BF),
            jax.ShapeDtypeStruct((1, D), F32),
        ),
        in_specs=[vmem] * 10 + [pl.BlockSpec(memory_space=pl.ANY)],
        out_specs=(vmem,) * 6,
        scratch_shapes=[
            pltpu.VMEM((seq_len, heads * HD), BF),
            pltpu.VMEM((seq_len, HD), F32),
            pltpu.VMEM((seq_len, HD), F32),
            pltpu.VMEM(w_qkv.shape, BF),
            pltpu.VMEM((seq_len, 1), F32),
            DMA,
        ],
        compiler_params=pltpu.CompilerParams(vmem_limit_bytes=VMEM_LIMIT),
        cost_estimate=pl.CostEstimate(
            flops=20 * heads * seq_len * seq_len * HD, transcendentals=0, bytes_accessed=20 << 20
        ),
        name="attention_back",
    )(proj, mid, w_out, seq, gq, gk, cosine, sine, docs[:, None], docs[None, :], w_qkv)


def in_halves(own, slot, sems):
    cut = own.shape[0] // 2
    return [
        (
            own.at[pl.ds(i * cut, cut)],
            lambda dev, i=i: slot(dev).at[pl.ds(i * cut, cut)],
            *sems[3 * i : 3 * i + 3],
        )
        for i in range(2)
    ]


def ring_sems(chips):
    return [DMA((2, chips // 2)), DMA((2, chips // 2)), DMA((2, chips))]


def dense_gradients_kernel(
    chips, split_out, h1_ref, grad_ref, ob_ref, mid_ref, gains_ref, qkv_ref, out_ref, gain_ref, *scratch
):
    hops = Hops(chips)
    scratches = [scratch[9 * i : 9 * i + 9] for i in range(4)]
    hops.meet(2 if split_out else 1)
    first = hops.core == 0
    if split_out:
        q_sum, q_came, o_sum, o_came, o_give, o_got, g_sum, g_came, rep_sem, flip_sem = scratch[36:]
    else:
        q_sum, o_sum, g_sum = qkv_ref, out_ref, gain_ref

    def product(left_ref, right_ref, rows, width):
        step = 512 if width % 512 == 0 else 256

        def produce(d, same_ref, other_ref):
            columns = pl.ds(pl.multiple_of(2 * rows * hops.chip(d), 2 * rows), 2 * rows)
            left = left_ref[:, columns]

            def block(at):
                value = dot_tn(left, right_ref[:, at])
                low, high = value[:rows], value[rows:]
                same_ref[:, at] = jnp.where(first, low, high)
                other_ref[:, at] = jnp.where(first, high, low).astype(BF)

            tiles(width // step, step, block)

        return produce

    def small(d, same_ref, other_ref):
        dev = hops.device(d)
        same_ref[...] = gains_ref[dev]
        other_ref[...] = gains_ref[dev + 1 - 2 * hops.core].astype(BF)

    def into(ref):
        def finish(value, at):
            ref[at, :] = value.astype(ref.dtype)

        return finish

    def ring(produce, ref, bufs):
        return hops.scatter(ref.shape[0], produce, *bufs, into(ref))

    shard, wide = q_sum.shape
    replica = lax.axis_index("rep")
    halves = [pl.ds(0, wide // 2), pl.ds(wide // 2, wide // 2)]
    if split_out:
        pairs = [(o_sum, o_came), *((q_sum.at[:, h], q_came.at[:, h]) for h in halves), (g_sum, g_came)]
        swaps = [
            pltpu.make_async_remote_copy(
                src_ref=src,
                dst_ref=dst,
                send_sem=rep_sem.at[0, i],
                recv_sem=rep_sem.at[1, i],
                device_id={"rep": 1 - replica},
                device_id_type=MESH,
            )
            for i, (src, dst) in enumerate(pairs)
        ]

    def then_swap(ring_steps, i):
        yield from ring_steps
        if split_out:
            swaps[i].start()

    rings = []
    if split_out:
        steps = ring(product(ob_ref, mid_ref, *o_sum.shape), o_sum, scratches[2])
        rings.append(then_swap(steps, 0))
    for i, h in enumerate(halves):
        part = product(h1_ref, grad_ref.at[:, h], shard, wide // 2)
        rings.append(then_swap(ring(part, q_sum.at[:, h], scratches[i]), 1 + i))
    rings.append(then_swap(ring(small, g_sum, scratches[3]), 3))
    hops.turn(*rings)
    if not split_out:
        return

    mine = hops.core == replica
    swaps[0].wait()
    o_give[...] = jnp.where(mine, o_came[...], o_sum[...])
    give = hops.copy(o_give, o_got, flip_sem.at[0], flip_sem.at[1], hops.flip)
    give.start()
    keep = jnp.where(mine, o_sum[...], o_came[...])
    even = replica == 0
    for i in range(wide // HD):
        if i * HD == 0 or i * HD == wide // 2:
            swaps[1 + (i > 0)].wait()
        own, came = q_sum[:, pl.ds(i * HD, HD)], q_came[:, pl.ds(i * HD, HD)]
        qkv_ref[:, pl.ds(2 * i * HD, HD)] = jnp.where(even, own, came).astype(F32)
        qkv_ref[:, pl.ds((2 * i + 1) * HD, HD)] = jnp.where(even, came, own).astype(F32)
    swaps[3].wait()
    gain_ref[...] = g_sum[...] + g_came[...]
    give.wait()
    half = o_sum.shape[0]
    got = o_got[...]
    out_ref[pl.ds(0, half), :] = jnp.where(first, keep, got).astype(F32)
    out_ref[pl.ds(half, half), :] = jnp.where(first, got, keep).astype(F32)


def dense_gradients(chips, split_out, h1, grad, ob, mid, gain_blocks, collective_id):
    shard = h1.shape[1] // (2 * chips)
    width = grad.shape[1]
    half = ob.shape[1] // (2 * chips) if split_out else 32
    vmem = pl.BlockSpec(memory_space=pltpu.VMEM)
    shapes = ((shard, width), (half, D), gain_blocks.shape[1:])
    scratch = []
    for rows, columns in ((shard, width // 2), (shard, width // 2), *shapes[1:]):
        scratch += [*scatter_scratch(chips, rows, columns), *ring_sems(chips)]
    if split_out:
        scratch += [pltpu.VMEM(shapes[0], BF)] * 2 + [pltpu.VMEM(shapes[1], BF)] * 4
        scratch += [pltpu.VMEM(shapes[2], F32)] * 2 + [DMA((2, 4)), DMA((2,))]
        shapes = ((shard, 2 * width), (2 * half, D), shapes[2])
    kinds = (F32, F32, F32) if split_out else (BF, BF, F32)
    return pl.pallas_call(
        functools.partial(dense_gradients_kernel, chips, split_out),
        out_shape=tuple(
            jax.ShapeDtypeStruct(shape, kind) for shape, kind in zip(shapes, kinds, strict=True)
        ),
        in_specs=[vmem] * 5,
        out_specs=(vmem,) * 3,
        scratch_shapes=scratch,
        compiler_params=pltpu.CompilerParams(
            collective_id=collective_id, has_side_effects=True, vmem_limit_bytes=VMEM_LIMIT
        ),
        cost_estimate=pl.CostEstimate(
            flops=2 * h1.size * width, transcendentals=0, bytes_accessed=200 << 20
        ),
        name="dense_gradients",
    )(h1, grad, ob, mid, gain_blocks)


def start_kernel(
    chips, reps, heads, split_out,
    tok_ref, small_ref, wq_ref, wo_ref,
    seq_ref, smalls_ref, full_ref, out_ref,
    own_q, own_o, *sems,
):
    hops = Hops(chips)
    rep = lax.axis_index("rep")
    sems_q, sems_s, sems_o = sems[:6], sems[6:9], sems[9:12]
    rep_sem, col_sem, own_sem, half_sem = sems[12:]
    pieces = []
    for i in range(3 * heads):
        q, j = i // heads, i % heads
        at = pl.multiple_of(((q * heads + j) * reps + rep) * HD, HD)
        pieces.append(
            pltpu.make_async_copy(
                wq_ref.at[:, pl.ds(at, HD)], own_q.at[:, pl.ds(i * HD, HD)], col_sem.at[i]
            )
        )
        pieces[-1].start()
    hops.meet(reps)
    swaps = []
    for k in range(1, reps):
        c = pltpu.make_async_remote_copy(
            src_ref=tok_ref,
            dst_ref=seq_ref.at[reps - k],
            send_sem=rep_sem.at[0, reps - k],
            recv_sem=rep_sem.at[1, reps - k],
            device_id={"rep": (rep + k) % reps},
            device_id_type=MESH,
        )
        c.start()
        swaps.append(c)
    locals_ = [
        pltpu.make_async_copy(tok_ref, seq_ref.at[0], own_sem.at[0]),
        pltpu.make_async_copy(small_ref, smalls_ref.at[hops.me], own_sem.at[1]),
    ]
    for c in locals_:
        c.start()
    for c in pieces:
        c.wait()
    mine = pltpu.make_async_copy(own_q, full_ref.at[hops.me], own_sem.at[2])
    mine.start()
    items = [
        *in_halves(own_q, lambda dev: full_ref.at[dev], sems_q),
        (small_ref, lambda dev: smalls_ref.at[dev], *sems_s),
    ]
    if split_out:
        rows = own_o.shape[0]
        kept = wo_ref.at[pl.ds(pl.multiple_of(hops.core * rows, rows), rows)]
        given = wo_ref.at[pl.ds(pl.multiple_of((1 - hops.core) * rows, rows), rows)]
        give = hops.copy(given, own_o, half_sem.at[0], half_sem.at[1], hops.flip)

        @pl.when(hops.core == rep)
        def _():
            give.start()
            keep = pltpu.make_async_copy(kept, own_o, half_sem.at[2])
            keep.start()
            keep.wait()
            give.wait_send()

        @pl.when(hops.core != rep)
        def _():
            give.wait_recv()

        def slot(dev):
            return out_ref.at[dev // 2, pl.ds(pl.multiple_of(dev % 2 * rows, rows), rows)]

        mine_o = pltpu.make_async_copy(own_o, slot(hops.me), half_sem.at[3])
        mine_o.start()
        items.append((own_o, slot, *sems_o))
    hops.turn(hops.gather(items, lambda d: None))
    for c in locals_:
        c.wait()
    mine.wait()
    if split_out:
        mine_o.wait()
    for c in swaps:
        c.wait()


def start(chips, reps, heads, split_out, tok, small, w_qkv, w_out, collective_id):
    anywhere = pl.BlockSpec(memory_space=pl.ANY)
    vmem = pl.BlockSpec(memory_space=pltpu.VMEM)
    shard, wide = w_qkv.shape[0], 3 * heads * HD
    half = w_out.shape[0] // 2
    return pl.pallas_call(
        functools.partial(start_kernel, chips, reps, heads, split_out),
        out_shape=(
            jax.ShapeDtypeStruct((reps, *tok.shape), BF),
            jax.ShapeDtypeStruct((2 * chips, *small.shape), F32),
            jax.ShapeDtypeStruct((2 * chips, shard, wide), BF),
            jax.ShapeDtypeStruct((chips, 2 * half, D), BF),
        ),
        in_specs=[vmem, vmem, anywhere, anywhere],
        out_specs=(anywhere,) * 4,
        scratch_shapes=[
            pltpu.VMEM((shard, wide), BF),
            pltpu.VMEM((half, D), BF),
            *ring_sems(chips),
            *ring_sems(chips),
            *ring_sems(chips),
            *ring_sems(chips),
            DMA((2, max(reps, 2))),
            DMA((3 * heads,)),
            DMA((3,)),
            DMA((4,)),
        ],
        compiler_params=pltpu.CompilerParams(collective_id=collective_id, has_side_effects=True),
        cost_estimate=pl.CostEstimate(
            flops=0, transcendentals=0, bytes_accessed=200 << 20
        ),
        name="start",
    )(tok, small, w_qkv, w_out)


def per_device(
    tokens, w_qkv, w_out, gains, w_gate, w_up, w_down, segment_ids, routes, gate_weights, cotangent
):
    groups = lax.axis_size("grp")
    reps = lax.axis_size("rep")
    ring = Ring(groups)
    rep, grp = lax.axis_index("rep"), lax.axis_index("grp")
    rel = jnp.asarray(ring.table())[grp]
    tok_rows = tokens.shape[1]
    seq_len = segment_ids.shape[1]
    heads = HEADS // reps
    wide = heads * HD

    def from_rep(v, k):
        return lax.ppermute(v, "rep", [((s + k) % reps, s) for s in range(reps)])

    def to_rep(v, k):
        return lax.ppermute(v, "rep", [(s, (s + k) % reps) for s in range(reps)])

    def rep_gather(v):
        return jnp.concatenate([v] + [from_rep(v, k) for k in range(1, reps)], axis=0)

    own_b = tokens[0]
    gates_f = gate_weights[0]
    experts = jnp.arange(groups, dtype=jnp.int32)
    weight_of = jnp.sum(
        jnp.where(routes[0][None] == experts[:, None, None], gates_f[None], 0.0), axis=-1
    )
    gain_rows = -(-gains.shape[0] // tok_rows)
    small_rows = -(-(groups + gain_rows) // 16) * 16
    small = jnp.concatenate(
        [
            weight_of,
            jnp.pad(gains.astype(F32), (0, gain_rows * tok_rows - gains.shape[0])).reshape(
                gain_rows, tok_rows
            ),
            jnp.zeros((small_rows - groups - gain_rows, tok_rows), F32),
        ],
        axis=0,
    )
    split_out = reps == 2 and heads == ring.chips
    seq_b, smalls, full_qkv, my_out = start(
        ring.chips, reps, heads, split_out, own_b, small, w_qkv, w_out, 1
    )
    seq_b = seq_b.reshape(seq_len, D)
    shard = full_qkv.shape[1]
    full_qkv = full_qkv.reshape(D, 3 * wide)
    if not split_out:
        my_out = lax.all_gather(w_out, "grp", axis=0, tiled=True)
        my_out = lax.dynamic_index_in_dim(
            my_out.reshape(heads, reps, HD, D), rep, axis=1, keepdims=False
        )
    my_out = my_out.reshape(wide, D)
    gains_f = smalls[:, groups : groups + gain_rows].reshape(groups, -1)
    gains_f = gains_f[:, : gains.shape[0]].reshape(-1)
    weight_in = lax.dynamic_index_in_dim(smalls, grp, 1, False)
    g_attn = gains_f[:D]
    g_ffn = gains_f[D : 2 * D]
    g_query = gains_f[2 * D : 2 * D + HD]
    g_key = gains_f[2 * D + HD :]

    def this_first(table):
        return lax.dynamic_slice_in_dim(
            jnp.concatenate([table, table], axis=0), rep * tok_rows, seq_len, axis=0
        )

    frequency = np.float32(rope_base) ** (-2.0 * np.arange(HD // 2, dtype=np.float32) / HD)
    angles = np.arange(seq_len, dtype=np.float32)[:, None] * frequency.astype(np.float32)[None, :]
    cosine = this_first(jnp.asarray(np.concatenate([np.cos(angles)] * 2, axis=1)))
    sine = this_first(jnp.asarray(np.concatenate([-np.sin(angles), np.sin(angles)], axis=1)))
    docs = this_first(segment_ids[0])
    g_query, g_key = g_query[None], g_key[None]
    dy_all, h1_b, projected, attended_b, mid_rows, h2_b = attention(
        ring.chips,
        reps,
        cotangent[0],
        seq_b,
        g_attn[None],
        g_ffn[None],
        g_query,
        g_key,
        cosine,
        sine,
        docs,
        full_qkv,
        my_out,
        5,
    )

    chips = ring.chips
    entries = tok_rows * TOP
    capacity = min(tok_rows, (9 * entries + 8 * groups - 1) // (8 * groups))
    capacity = -(-capacity // 16) * 16
    named = weight_in > 0
    before = dot32(
        named.astype(BF), jnp.tri(tok_rows, dtype=BF).T
    )
    slot = jnp.where(named, before - 1.0, -1.0).astype(jnp.int32)
    rows_in, grads_in, acts, grad_gates, grad_ups = expert_rows(
        chips, capacity, h2_b, dy_all, slot, weight_in, w_gate[0], w_up[0], w_down[0], 2
    )
    all_rows = rows_in.reshape(-1, D)
    all_grads = grads_in.reshape(-1, D)
    all_acts = acts.reshape(groups * capacity, -1)
    all_gates = grad_gates.reshape(groups * capacity, -1)
    all_ups = grad_ups.reshape(groups * capacity, -1)

    def rep_send(v):
        return v, [from_rep(v, k) for k in range(1, reps)]

    def rep_sum(sent, after):
        (v, came), _ = lax.optimization_barrier((sent, after))
        return v.astype(F32) + sum(c.astype(F32) for c in came)

    slot_t, weight_t = slot.astype(F32).T, weight_in.T
    together = split_out and chips <= 8
    if together:
        out_sum, own_down, came_down, grad_wgate, grad_wup = outputs(
            chips, capacity, all_acts, all_rows, all_grads, all_gates, all_ups,
            slot_t, weight_t, w_down[0], 6,
        )
        grad_wdown = (own_down, [came_down])
    else:
        grad_wdown = rep_send(
            jnp.einsum("rf,rd->fd", all_acts, all_grads, preferred_element_type=F32).astype(BF)
        )
        grad_wgate = jnp.einsum("rd,rf->df", all_rows, all_gates, preferred_element_type=F32).astype(BF)
        grad_wup = jnp.einsum("rd,rf->df", all_rows, all_ups, preferred_element_type=F32).astype(BF)
    grad_wgate = rep_send(grad_wgate)
    grad_wup = rep_send(grad_wup)

    cuts = 1 if chips <= 8 else chips // 8
    (grad_gates, grad_ups), _ = lax.optimization_barrier(
        ((grad_gates, grad_ups), (grad_wdown[0], grad_wgate[0], grad_wup[0]))
    )
    grad_h2 = jnp.concatenate(
        [
            rows_back(chips, capacity, grad_gates, grad_ups, slot_t, wg, wu, 8 + i)
            for i, (wg, wu) in enumerate(
                zip(jnp.split(w_gate[0], cuts), jnp.split(w_up[0], cuts), strict=True)
            )
        ],
        axis=1,
    )


    grad_out = cotangent[0].astype(F32)
    _, hat_two, inv_two = rms_forward(mid_rows, g_ffn)
    grad_mid_norm, ffn_terms = rms_backward(grad_h2, hat_two, inv_two, g_ffn)
    grad_mid = grad_out + grad_mid_norm
    grad_mid_b = grad_mid.astype(BF)
    if not together:
        pick = (slot[:, None, :] == jnp.arange(capacity, dtype=jnp.int32)[None, :, None]).astype(BF)
        row_weight = jnp.sum(pick.astype(F32) * weight_in[:, None, :], axis=-1)
        acts_late, _ = lax.optimization_barrier((all_acts, grad_mid_b))
        eout = dot32(acts_late, w_down[0]).astype(BF).astype(F32)
        eout = (row_weight.reshape(-1, 1) * eout).astype(BF).reshape(groups, capacity, D)
        out_all = jnp.einsum("gct,gcd->gtd", pick, eout, preferred_element_type=F32).astype(BF)
        out_sum = lax.psum_scatter(
            out_all.reshape(groups * tok_rows, D), "grp", scatter_dimension=0, tiled=True
        )
    result = mid_rows + lax.optimization_barrier((out_sum, grad_mid_b))[0].astype(F32)
    grad_wdown = rep_sum(grad_wdown, grad_mid_b)
    grad_wgate = rep_sum(grad_wgate, grad_mid_b)
    grad_branch_b = rep_gather(grad_mid_b)
    (grad_branch_b, result, grad_wdown, grad_wgate), _ = lax.optimization_barrier(
        ((grad_branch_b, result, grad_wdown, grad_wgate), grad_mid_b)
    )
    grad_proj, query_terms, key_terms, grad_h1, rest, attn_terms = attention_back(
        tok_rows, projected, grad_branch_b, my_out, seq_b, g_query, g_key, cosine, sine, docs,
        full_qkv,
    )
    for k in range(1, reps):
        part = rest[(k - 1) * tok_rows : k * tok_rows]
        grad_h1 = grad_h1 + to_rep(part, k).astype(F32)
    _, hat_one, inv_one = rms_forward(own_b.astype(F32), g_attn)
    grad_rows_one, _ = rms_backward(grad_h1, hat_one, inv_one, g_attn)
    grad_tokens = grad_mid + grad_rows_one
    grad_gains = jnp.concatenate(
        [
            attn_terms[0],
            jnp.sum(ffn_terms, axis=0),
            query_terms[0],
            key_terms[0],
        ]
    )

    gain_size = gains.shape[0]
    gain_blocks = jnp.pad(
        grad_gains.reshape(groups, gain_size), ((0, 0), (0, 4096 - gain_size))
    ).reshape(groups, 32, 128)
    shard_qkv, half_out, total = dense_gradients(
        chips,
        split_out,
        h1_b,
        grad_proj,
        attended_b,
        grad_branch_b,
        gain_blocks,
        4,
    )
    total = total.reshape(-1)[:gain_size]
    grad_wup = rep_sum(grad_wup, shard_qkv)

    if split_out:
        shard_out = half_out
    else:
        qkv_all = [shard_qkv] + [from_rep(shard_qkv, k) for k in range(1, reps)]
        columns = jnp.stack(qkv_all, axis=0).reshape(reps, shard, 3, heads, HD)
        columns = columns[(jnp.arange(reps) - rep) % reps]
        shard_qkv = columns.transpose(1, 2, 3, 0, 4).reshape(shard, 3 * D).astype(F32)
        grad_wout = dot_tn(attended_b, grad_branch_b)
        whole = lax.dynamic_update_slice(
            jnp.zeros((heads, reps, HD, D), BF),
            grad_wout.astype(BF).reshape(heads, 1, HD, D),
            (0, rep, 0, 0),
        ).reshape(D, D)
        shard_out = lax.psum(
            lax.psum_scatter(whole, "grp", scatter_dimension=0, tiled=True), "rep"
        ).astype(F32)
        own_gains = total
        for k in range(1, reps):
            total = total + from_rep(own_gains, k)
    return (
        result[None],
        grad_tokens[None],
        shard_qkv,
        shard_out,
        total,
        grad_wgate[None],
        grad_wup[None],
        grad_wdown[None],
    )


def solution(mesh):
    in_specs = (
        P("grp", "rep", None),
        P("grp", None),
        P("grp", None),
        P("grp"),
        P("grp", None, None),
        P("grp", None, None),
        P("grp", None, None),
        P("grp", None),
        P("grp", "rep", None),
        P("grp", "rep", None),
        P("grp", "rep", None),
    )
    out_specs = (
        P("grp", "rep", None),
        P("grp", "rep", None),
        P("grp", None),
        P("grp", None),
        P("grp"),
        P("grp", None, None),
        P("grp", None, None),
        P("grp", None, None),
    )
    return jax.shard_map(
        per_device, mesh=mesh, in_specs=in_specs, out_specs=out_specs, check_vma=False
    )
```
